32 devices in a mesh: pod: 1 (over z), data: 4 (over y), stage: 8 (over x, core).
Axes of the slice: x: 4, y: 4, z: 1, core: 2. Of those that a mesh axis runs over, the one named last changes fastest.
The devices are a block of a 4x4x8 slice.
Arguments:
- x_last: bfloat16 [16384, 768], P(('pod', 'data', 'stage'))
- w_head: bfloat16 [50304, 768], P('stage')
- labels: int32 [16384], P(('pod', 'data'))
- loss_mask: int32 [16384], P(('pod', 'data'))
- w_embed: bfloat16 [50304, 768], P('stage')
- tok_ids: int32 [16384], P(('pod', 'data'))
- act_in: bfloat16 [131072, 768], P(('pod', 'data', 'stage'))
- w_up: bfloat16 [8, 768, 3072], P('stage')
- w_down: bfloat16 [8, 3072, 768], P('stage')
Outputs:
- output 1: float32 [1], P('pod')
- output 2: float32 [16384, 768], P(('pod', 'data', 'stage'))
- output 3: bfloat16 [50304, 768], P(('pod', 'stage'))
- output 4: bfloat16 [16384, 768], P(('pod', 'data', 'stage'))
- output 5: bfloat16 [131072, 768], P(('pod', 'data', 'stage'))
All inputs are finite; a program needn't handle non-finite values.
Results may differ from the reference program's by a relative error of at most 0.001.
Values are sent between devices in bfloat16 or wider.
A program may use at most 768 MiB of HBM per device.

```python
import jax
import jax.numpy as jnp
from jax import lax

D_MODEL = 768
VOCAB_SIZE = 50304
D_FF = 3072
TOKENS = 4096
N_DATA = 4
N_STAGE = 8

SLICE_ROWS = VOCAB_SIZE // N_STAGE


def setup_inputs(seed: int = 0, part: int = 0) -> dict:
    base_key = jax.random.key(seed)
    shared_keys = jax.random.split(base_key, 4)
    part_keys = jax.random.split(jax.random.fold_in(base_key, part), 5)
    all_rows = N_DATA * TOKENS
    x_last = jax.random.normal(part_keys[0], (all_rows, D_MODEL), jnp.float32).astype(jnp.bfloat16)
    w_head = (2.0 * D_MODEL ** -0.5 * jax.random.normal(shared_keys[0], (VOCAB_SIZE, D_MODEL), jnp.float32)).astype(jnp.bfloat16)
    labels = jax.random.randint(part_keys[1], (all_rows,), 0, VOCAB_SIZE, jnp.int32)
    labels = labels.at[0].set(0).at[1].set(VOCAB_SIZE - 1)
    loss_mask = (jax.random.randint(part_keys[2], (all_rows,), 0, 16, jnp.int32) != 0).astype(jnp.int32)
    w_embed = jax.random.normal(shared_keys[1], (VOCAB_SIZE, D_MODEL), jnp.float32).astype(jnp.bfloat16)
    tok_ids = jax.random.randint(part_keys[3], (all_rows,), 0, VOCAB_SIZE, jnp.int32)
    tok_ids = tok_ids.at[0].set(VOCAB_SIZE - 1).at[1].set(0)
    act_in = jax.random.normal(part_keys[4], (N_DATA * N_STAGE * TOKENS, D_MODEL), jnp.float32).astype(jnp.bfloat16)
    w_up = (D_MODEL ** -0.5 * jax.random.normal(shared_keys[2], (N_STAGE, D_MODEL, D_FF), jnp.float32)).astype(jnp.bfloat16)
    w_down = (D_FF ** -0.5 * jax.random.normal(shared_keys[3], (N_STAGE, D_FF, D_MODEL), jnp.float32)).astype(jnp.bfloat16)
    return {'x_last': x_last, 'w_head': w_head, 'labels': labels, 'loss_mask': loss_mask, 'w_embed': w_embed, 'tok_ids': tok_ids, 'act_in': act_in, 'w_up': w_up, 'w_down': w_down}


def head_replica(x_rows, w_head, labels, loss_mask):
    w_slices = w_head.reshape(N_STAGE, SLICE_ROWS, D_MODEL)

    def stats_step(run_state, w_part):
        run_max, run_sum = run_state
        logits = jnp.dot(x_rows, w_part.T, preferred_element_type=jnp.float32)
        new_max = jnp.maximum(run_max, jnp.max(logits, axis=1))
        new_sum = run_sum * jnp.exp(run_max - new_max) + jnp.sum(jnp.exp(logits - new_max[:, None]), axis=1)
        return (new_max, new_sum), None

    start_state = (jnp.full((TOKENS,), -jnp.inf, jnp.float32), jnp.zeros((TOKENS,), jnp.float32))
    (row_max, row_sum), unused_out = lax.scan(stats_step, start_state, w_slices)
    weights = loss_mask.astype(jnp.float32)
    loss_denom = jnp.maximum(jnp.sum(weights), 1.0)
    target = jnp.sum(x_rows.astype(jnp.float32) * jnp.take(w_head, labels, axis=0).astype(jnp.float32), axis=1)
    rep_loss = jnp.sum(weights * (jnp.log(row_sum) + row_max - target)) / loss_denom
    row_scale = weights / loss_denom
    col_base = jnp.arange(N_STAGE, dtype=jnp.int32) * SLICE_ROWS

    def grad_step(dx_acc, step_in):
        w_part, first_col = step_in
        logits = jnp.dot(x_rows, w_part.T, preferred_element_type=jnp.float32)
        soft_probs = jnp.exp(logits - row_max[:, None]) / row_sum[:, None]
        col_ids = first_col + jnp.arange(SLICE_ROWS, dtype=jnp.int32)
        is_label = labels[:, None] == col_ids[None, :]
        grad_logits = (jnp.where(is_label, soft_probs - 1.0, soft_probs) * row_scale[:, None]).astype(jnp.bfloat16)
        dx_acc = dx_acc + jnp.dot(grad_logits, w_part, preferred_element_type=jnp.float32)
        dw_part = jnp.dot(grad_logits.T, x_rows, preferred_element_type=jnp.float32)
        return dx_acc, dw_part

    grad_rows, dw_parts = lax.scan(grad_step, jnp.zeros((TOKENS, D_MODEL), jnp.float32), (w_slices, col_base))
    return rep_loss, grad_rows, dw_parts


def reference(x_last, w_head, labels, loss_mask, w_embed, tok_ids, act_in, w_up, w_down):
    x_reps = x_last.reshape(N_DATA, TOKENS, D_MODEL)
    lab_reps = labels.reshape(N_DATA, TOKENS)
    mask_reps = loss_mask.reshape(N_DATA, TOKENS)

    def replica_step(dw_acc, rep_data):
        x_rows, rep_labels, rep_mask = rep_data
        rep_loss, grad_rows, dw_parts = head_replica(x_rows, w_head, rep_labels, rep_mask)
        return dw_acc + dw_parts, (rep_loss, grad_rows)

    dw_start = jnp.zeros((N_STAGE, SLICE_ROWS, D_MODEL), jnp.float32)
    dw_sum, (rep_losses, grad_reps) = lax.scan(replica_step, dw_start, (x_reps, lab_reps, mask_reps))
    mean_loss = (jnp.sum(rep_losses) / N_DATA).reshape(1)
    grad_x = grad_reps.reshape(N_DATA * TOKENS, D_MODEL)
    grad_head = (dw_sum / N_DATA).astype(jnp.bfloat16).reshape(VOCAB_SIZE, D_MODEL)
    embed_out = jnp.take(w_embed, tok_ids, axis=0)
    up_f32 = w_up.astype(jnp.float32)
    down_f32 = w_down.astype(jnp.float32)

    def mlp_replica(act_rep):
        act_f32 = act_rep.astype(jnp.float32)
        hidden = jax.nn.gelu(jnp.einsum('std,sdf->stf', act_f32, up_f32)).astype(jnp.bfloat16)
        out_f32 = act_f32 + jnp.einsum('stf,sfd->std', hidden.astype(jnp.float32), down_f32)
        return out_f32.astype(jnp.bfloat16)

    mlp_out = lax.map(mlp_replica, act_in.reshape(N_DATA, N_STAGE, TOKENS, D_MODEL))
    mlp_out = mlp_out.reshape(N_DATA * N_STAGE * TOKENS, D_MODEL)
    return mean_loss, grad_x, grad_head, embed_out, mlp_out
```

```python
import functools

import jax
import jax.numpy as jnp
from jax import lax
from jax.experimental import pallas as pl
from jax.experimental.pallas import tpu as pltpu
from jax.sharding import PartitionSpec as P

MESH = pl.DeviceIdType.MESH
F32 = jnp.float32
BF16 = jnp.bfloat16
N_TILE = 6
MLP_EIGHTHS = (2, 3, 3)
LOW = -1e30


def _params(mib=60, **kw):
    return pltpu.CompilerParams(vmem_limit_bytes=mib * 2**20, **kw)


def _cost(flops, nbytes, trans=0):
    return pl.CostEstimate(flops=int(flops), bytes_accessed=int(nbytes), transcendentals=int(trans))


def _mlp_body(a_ref, w1_ref, w2_ref, *rest, chunk):
    o_ref, u_ref = rest[-2:]
    ff = w1_ref.shape[1]
    for c in range(ff // chunk):
        cs = slice(c * chunk, (c + 1) * chunk)
        h = jnp.dot(a_ref[...], w1_ref[:, cs], preferred_element_type=F32)
        u_ref[:, cs] = jax.nn.gelu(h).astype(BF16)
    y = jnp.dot(u_ref[...], w2_ref[...], preferred_element_type=F32)
    o_ref[...] = (a_ref[...].astype(F32) + y).astype(BF16)


def mlp(a, w1, w2, out, first, count, tb=512):
    n, d = a.shape
    ff = w1.shape[1]
    extra = [] if out is None else [out]
    return pl.pallas_call(
        functools.partial(_mlp_body, chunk=512),
        grid=(count,),
        in_specs=[
            pl.BlockSpec((tb, d), lambda i: (first + i, 0)),
            pl.BlockSpec((d, ff), lambda i: (0, 0)),
            pl.BlockSpec((ff, d), lambda i: (0, 0)),
        ] + [pl.BlockSpec(memory_space=pl.ANY)] * len(extra),
        out_specs=pl.BlockSpec((tb, d), lambda i: (first + i, 0)),
        out_shape=jax.ShapeDtypeStruct((n, d), BF16),
        scratch_shapes=[pltpu.VMEM((tb, ff), BF16)],
        input_output_aliases={3: 0} if extra else {},
        compiler_params=_params(),
        cost_estimate=_cost(4 * count * tb * d * ff, 4 * count * tb * d + 4 * d * ff, count * tb * ff),
        name="mlp",
    )(a, w1, w2, *extra)


def _logits_body(lo_ref, lab_ref, x_ref, w_ref, z_ref, st_ref, *, vt):
    tb = x_ref.shape[0]
    lab8 = jnp.broadcast_to(lab_ref[0:1, :], (8, tb))
    sub = lax.broadcasted_iota(jnp.int32, (vt // 8, 8, tb), 0) * 8 + lax.broadcasted_iota(jnp.int32, (vt // 8, 8, tb), 1)
    m8 = s8 = t8 = None
    for v in range(w_ref.shape[0] // vt):
        vs = slice(v * vt, (v + 1) * vt)
        z = lax.dot_general(w_ref[vs, :], x_ref[...], (((1,), (1,)), ((), ())), preferred_element_type=F32)
        if v == 0:
            z = jnp.where(lax.broadcasted_iota(jnp.int32, (vt, tb), 0) >= lo_ref[0], z, LOW)
        z_ref[0, vs, :] = z
        zr = z_ref[0, vs, :].reshape(vt // 8, 8, tb)
        tile_max = jnp.max(zr, axis=0)
        m_new = tile_max if v == 0 else jnp.maximum(m8, tile_max)
        e_sum = jnp.sum(jnp.exp(zr - m_new[None]), axis=0)
        hit = jnp.sum(jnp.where(sub == (lab8 - v * vt)[None], zr, 0.0), axis=0)
        s8 = e_sum if v == 0 else s8 * jnp.exp(m8 - m_new) + e_sum
        t8 = hit if v == 0 else t8 + hit
        m8 = m_new
    m = jnp.max(m8, axis=0, keepdims=True)
    s = jnp.sum(s8 * jnp.exp(m8 - m), axis=0, keepdims=True)
    t = jnp.sum(t8, axis=0, keepdims=True)
    st_ref[...] = jnp.concatenate([m, s, t, jnp.zeros((5, tb), F32)], axis=0)


def logits(lo, lab, x, w, vt, tb=512):
    n, d = x.shape
    win = w.shape[0]
    return pl.pallas_call(
        functools.partial(_logits_body, vt=vt),
        grid=(n // tb,),
        in_specs=[
            pl.BlockSpec(memory_space=pltpu.SMEM),
            pl.BlockSpec((1, tb), lambda i: (0, i)),
            pl.BlockSpec((tb, d), lambda i: (i, 0)),
            pl.BlockSpec((win, d), lambda i: (0, 0)),
        ],
        out_specs=[
            pl.BlockSpec((1, win, tb), lambda i: (0, 0, i)),
            pl.BlockSpec((8, tb), lambda i: (0, i)),
        ],
        out_shape=[jax.ShapeDtypeStruct((1, win, n), F32), jax.ShapeDtypeStruct((8, n), F32)],
        compiler_params=_params(),
        cost_estimate=_cost(2 * n * d * win, 4 * n * win + 2 * d * (n + win), n * win),
        name="logits",
    )(lo, lab, x, w)


def _stats_body(mask_ref, sp_ref, so_ref, out_ref, got, mine, coef, send1, recv1, send2, recv2, *, n_stage):
    y, s = lax.axis_index("data"), lax.axis_index("stage")
    rows = sp_ref.shape[1] // n_stage
    peers = [(f, k) for f in range(2) for k in range(n_stage) if (f, k) != (0, 0)]

    def where_to(f, k):
        y_to = y if f == 0 else y + 1 - 2 * lax.rem(y, 2)
        return {"data": y_to, "stage": lax.rem(s + k, n_stage)}

    def cols(stage):
        return pl.ds(pl.multiple_of(stage * rows, rows), rows)

    barrier = pltpu.get_barrier_semaphore()
    for f, k in peers:
        pl.semaphore_signal(barrier, inc=1, device_id=where_to(f, k), device_id_type=MESH)
    pl.semaphore_wait(barrier, len(peers))

    first = []
    for f, k in peers:
        src = so_ref if f == 0 else sp_ref
        slot = f * n_stage + k
        c = pltpu.make_async_remote_copy(
            src_ref=src.at[:, cols(lax.rem(s + k, n_stage))],
            dst_ref=got.at[slot],
            send_sem=send1.at[slot],
            recv_sem=recv1.at[slot],
            device_id=where_to(f, k),
            device_id_type=MESH,
        )
        c.start()
        first.append(c)
    weight = mask_ref[...].astype(F32)
    denom = jnp.maximum(jnp.sum(weight), 1.0)
    mu = mask_ref[:, cols(s)].astype(F32)
    own = so_ref[:, cols(s)]
    for c in first:
        c.wait_recv()
    parts = [own] + [got[f * n_stage + k] for f, k in peers]
    m = functools.reduce(jnp.maximum, [p[0:1, :] for p in parts])
    z = sum(p[1:2, :] * jnp.exp(p[0:1, :] - m) for p in parts)
    t = sum(p[2:3, :] for p in parts)
    scale = mu / denom
    loss = scale * (jnp.log(z) + m - t)
    res = jnp.concatenate([m, scale / z, scale, loss, jnp.zeros((4, rows), F32)], axis=0)
    mine[...] = res
    second = []
    for f, k in peers:
        slot = f * n_stage + k
        c = pltpu.make_async_remote_copy(
            src_ref=mine,
            dst_ref=coef.at[1 - f, :, cols(s)],
            send_sem=send2.at[slot],
            recv_sem=recv2.at[slot],
            device_id=where_to(f, k),
            device_id_type=MESH,
        )
        c.start()
        second.append(c)
    coef[1, :, cols(s)] = res
    for c in first:
        c.wait_send()
    for c in second:
        c.wait_recv()
    out_ref[...] = coef[...]
    for c in second:
        c.wait_send()


def stats(mask, st_p, st_o, n_stage):
    n = st_p.shape[1]
    rows = n // n_stage
    vm = pl.BlockSpec(memory_space=pltpu.VMEM)
    slots = 2 * n_stage
    dma = pltpu.SemaphoreType.DMA((slots,))
    return pl.pallas_call(
        functools.partial(_stats_body, n_stage=n_stage),
        in_specs=[vm] * 3,
        out_specs=vm,
        out_shape=jax.ShapeDtypeStruct((2, 8, n), F32),
        scratch_shapes=[
            pltpu.VMEM((slots, 8, rows), F32),
            pltpu.VMEM((8, rows), F32),
            pltpu.VMEM((2, 8, n), F32),
            dma, dma, dma, dma,
        ],
        compiler_params=_params(32, collective_id=0, has_side_effects=True),
        cost_estimate=_cost(10**9, 10**7),
        name="stats",
    )(mask, st_p, st_o)


def _gdw_body(tile_ref, coef_ref, lab_ref, zp_ref, zo_ref, xp_ref, xo_ref, gin_ref, g_ref, dw_ref, gs, *, ch):
    del gin_ref
    t = pl.program_id(0)
    vt, tb = dw_ref.shape[0], coef_ref.shape[2]
    row0 = tile_ref[0] * vt
    sub = lax.broadcasted_iota(jnp.int32, (vt // 8, 8, ch), 0) * 8 + lax.broadcasted_iota(jnp.int32, (vt // 8, 8, ch), 1)

    def run(z_ref, x_ref, t_local):
        acc = None
        for c in range(tb // ch):
            cs = slice(c * ch, (c + 1) * ch)
            m8 = jnp.broadcast_to(coef_ref[0, 0:1, cs], (8, ch))
            c8 = jnp.broadcast_to(coef_ref[0, 1:2, cs], (8, ch))
            r8 = jnp.broadcast_to(coef_ref[0, 2:3, cs], (8, ch))
            lab8 = jnp.broadcast_to(lab_ref[0:1, cs], (8, ch)) - row0
            zr = z_ref[0, :, cs].reshape(vt // 8, 8, ch)
            e = jnp.exp(zr - m8[None]) * c8[None]
            g = jnp.where(sub == lab8[None], e - r8[None], e)
            gb = g.reshape(vt, ch).astype(BF16)
            g_ref[0, :, cs] = gb
            xb = x_ref[pl.ds(pl.multiple_of(t_local * tb + c * ch, ch), ch), :]
            d = jnp.dot(gb, xb, preferred_element_type=F32)
            acc = d if acc is None else acc + d
        dw_ref[...] = jnp.where(t == 0, 0.0, dw_ref[...]) + acc

    half = pl.num_programs(0) // 2

    @pl.when(t < half)
    def _():
        run(zp_ref, xp_ref, t)

    @pl.when(t >= half)
    def _():
        run(zo_ref, xo_ref, t - half)


def gdw(tile, coef, lab, z_p, z_o, x_p, x_o, g, vt, tb=2048, ch=512):
    n, d = x_p.shape
    win = z_p.shape[1]
    tb = min(tb, n)
    nt = n // tb
    spec = pltpu.PrefetchScalarGridSpec(
        num_scalar_prefetch=1,
        grid=(2 * nt,),
        in_specs=[
            pl.BlockSpec((1, 8, tb), lambda t, i: (t // nt, 0, t % nt)),
            pl.BlockSpec((1, tb), lambda t, i: (0, t)),
            pl.BlockSpec((1, vt, tb), lambda t, i: (0, i[0], jnp.minimum(t, nt - 1))),
            pl.BlockSpec((1, vt, tb), lambda t, i: (0, i[0], jnp.maximum(t - nt, 0))),
            pl.BlockSpec((n, d), lambda t, i: (0, 0), pipeline_mode=pl.Buffered(1)),
            pl.BlockSpec((n, d), lambda t, i: (0, 0), pipeline_mode=pl.Buffered(1)),
            pl.BlockSpec(memory_space=pl.ANY),
        ],
        out_specs=[
            pl.BlockSpec((1, vt, tb), lambda t, i: (t // nt, i[0], t % nt)),
            pl.BlockSpec((vt, d), lambda t, i: (0, 0)),
        ],
        scratch_shapes=[pltpu.VMEM((vt, ch), BF16)],
    )
    kw = {}
    args = [tile, coef, lab, z_p, z_o, x_p, x_o]
    if g is None:
        g = jnp.zeros((8, 128), BF16)
    else:
        kw["input_output_aliases"] = {7: 0}
    return pl.pallas_call(
        functools.partial(_gdw_body, ch=ch),
        grid_spec=spec,
        out_shape=[jax.ShapeDtypeStruct((2, win, n), BF16), jax.ShapeDtypeStruct((vt, d), F32)],
        compiler_params=_params(62),
        cost_estimate=_cost(4 * n * d * vt, 12 * n * vt + 4 * n * d, 2 * n * vt),
        name="gdw",
        **kw,
    )(*args, g)


def _dx_body(g_ref, w_ref, o_ref):
    o_ref[...] = lax.dot_general(g_ref[0], w_ref[...], (((0,), (0,)), ((), ())), preferred_element_type=F32)


def dx(g, w, role, tb=512):
    n = g.shape[2]
    win, d = w.shape
    return pl.pallas_call(
        _dx_body,
        grid=(n // tb,),
        in_specs=[
            pl.BlockSpec((1, win, tb), lambda i: (role, 0, i)),
            pl.BlockSpec((win, d), lambda i: (0, 0)),
        ],
        out_specs=pl.BlockSpec((tb, d), lambda i: (i, 0)),
        out_shape=jax.ShapeDtypeStruct((n, d), F32),
        compiler_params=_params(),
        cost_estimate=_cost(2 * n * d * win, 2 * n * win + 4 * n * d),
        name="dx",
    )(g, w)


def solution(mesh):
    n_data, n_stage = mesh.shape["data"], mesh.shape["stage"]
    tok_spec = P(("pod", "data", "stage"), None)
    rep_spec = P(("pod", "data"))
    vocab_spec = P("stage", None)
    layer_spec = P("stage", None, None)
    swap_a = [(i, i ^ 1) for i in range(n_data)]
    swap_b = [(i, n_data - 1 - i) for i in range(n_data)]

    def local_step(x_rows, w_head, labels, loss_mask, w_embed, tok_ids, act_in, w_up, w_down):
        y, s = lax.axis_index("data"), lax.axis_index("stage")
        shard, d = w_head.shape
        yh = y >> 1
        h = (y ^ yh) & 1
        vt = -(-shard // (2 * N_TILE * 16)) * 16
        win = N_TILE * vt
        first_row = shard - win
        lo = (2 * win - shard) * h

        def over_a(v):
            return lax.ppermute(v, "data", swap_a)

        def over_b(v):
            return lax.ppermute(v, "data", swap_b)

        w_win = lax.dynamic_slice(w_head, (h * first_row, 0), (win, d))
        lab_a = over_a(labels)
        x_a = over_a(x_rows)
        x_o = lax.all_gather(x_rows, "stage", axis=0, tiled=True)
        x_p = lax.all_gather(x_a, "stage", axis=0, tiled=True)

        def local(lab):
            lab = lab - (s * shard + h * first_row)
            return jnp.where(lab < lo, -1, lab)

        lab = jnp.concatenate([local(lab_a), local(labels)]).reshape(1, -1)
        lo_arr = lo.reshape(1)
        n_tok = labels.shape[0]
        mlp_out, done = None, 0
        for part in MLP_EIGHTHS:
            count = n_tok // 512 * part // 8
            mlp_out = mlp(act_in, w_up[0], w_down[0], mlp_out, done, count)
            done += count

        offset = s * shard
        local_ids = tok_ids - offset
        in_slice = (local_ids >= 0) & (local_ids < shard)
        rows_emb = jnp.take(w_embed, jnp.clip(local_ids, 0, shard - 1), axis=0)
        emb_part = jnp.where(in_slice[:, None], rows_emb, jnp.zeros_like(rows_emb))
        embed_out = lax.psum_scatter(emb_part, "stage", scatter_dimension=0, tiled=True)

        z_o, st_o = logits(lo_arr, lab[:, n_tok:], x_o, w_win, vt)
        z_p, st_p = logits(lo_arr, lab[:, :n_tok], x_p, w_win, vt)
        coef = stats(loss_mask.reshape(1, -1), st_p, st_o, n_stage)

        loss_two = jnp.sum(coef[:, 3, :], axis=1)
        loss_pair = loss_two[0] + loss_two[1]
        loss_far = over_b(loss_pair.reshape(1, 1))[0, 0]
        mean_loss = (loss_pair + loss_far) / n_data

        half = N_TILE // 2
        g = None
        sent, kept = [], []
        for j in range(half):
            tile = ((1 - yh) * half + j).reshape(1)
            g, dw = gdw(tile, coef, lab, z_p, z_o, x_p, x_o, g, vt)
            sent.append(over_b(dw))
        for j in range(half):
            tile = (yh * half + j).reshape(1)
            g, dw = gdw(tile, coef, lab, z_p, z_o, x_p, x_o, g, vt)
            kept.append(dw)

        dx_p = dx(g, w_win, 0)
        rs_p = lax.psum_scatter(dx_p, "stage", scatter_dimension=0, tiled=True)
        dx_o = dx(g, w_win, 1)
        rs_o = lax.psum_scatter(dx_o, "stage", scatter_dimension=0, tiled=True)
        gx_a = over_a(rs_p)
        grad_x = rs_o + gx_a

        grad_head = jnp.zeros((shard, d), BF16)
        for j in range(half):
            fin = lax.optimization_barrier(((kept[j] + sent[j]) / n_data).astype(BF16))
            fin_b = over_b(fin)
            fin_a = over_a(fin)
            fin_ab = over_a(fin_b)
            for v, hh, part in ((fin, h, yh), (fin_a, 1 - h, yh), (fin_b, h, 1 - yh), (fin_ab, 1 - h, 1 - yh)):
                row = hh * first_row + (part * half + j) * vt
                grad_head = lax.dynamic_update_slice(grad_head, v, (row, 0))

        return mean_loss.reshape(1), grad_x, grad_head, embed_out, mlp_out

    return jax.shard_map(
        local_step,
        mesh=mesh,
        in_specs=(tok_spec, vocab_spec, rep_spec, rep_spec, vocab_spec, rep_spec, tok_spec, layer_spec, layer_spec),
        out_specs=(P("pod"), tok_spec, P(("pod", "stage"), None), tok_spec, tok_spec),
        check_vma=False,
    )
```

```python
import functools

import jax
import jax.numpy as jnp
from jax import lax
from jax.experimental import pallas as pl
from jax.experimental.pallas import tpu as pltpu
from jax.sharding import PartitionSpec as P

MESH = pl.DeviceIdType.MESH
F32 = jnp.float32
BF16 = jnp.bfloat16
N_TILE = 6


def VT_LOGITS(win):
    return next(v for v in range(352, 0, -16) if win % v == 0 and v <= 288)


LOW = -1e30


def _params(mib=60, **kw):
    return pltpu.CompilerParams(vmem_limit_bytes=mib * 2**20, **kw)


def _cost(flops, nbytes, trans=0):
    return pl.CostEstimate(flops=int(flops), bytes_accessed=int(nbytes), transcendentals=int(trans))


def _mlp_body(a_ref, w1_ref, w2_ref, *rest, chunk):
    o_ref, u_ref = rest[-2:]
    ff = w1_ref.shape[1]
    for c in range(ff // chunk):
        cs = slice(c * chunk, (c + 1) * chunk)
        h = jnp.dot(a_ref[...], w1_ref[:, cs], preferred_element_type=F32)
        u_ref[:, cs] = jax.nn.gelu(h).astype(BF16)
    y = jnp.dot(u_ref[...], w2_ref[...], preferred_element_type=F32)
    o_ref[...] = (a_ref[...].astype(F32) + y).astype(BF16)


def mlp(a, w1, w2, out, first, count, tb=512):
    n, d = a.shape
    ff = w1.shape[1]
    extra = [] if out is None else [out]
    return pl.pallas_call(
        functools.partial(_mlp_body, chunk=512),
        grid=(count,),
        in_specs=[
            pl.BlockSpec((tb, d), lambda i: (first + i, 0)),
            pl.BlockSpec((d, ff), lambda i: (0, 0)),
            pl.BlockSpec((ff, d), lambda i: (0, 0)),
        ] + [pl.BlockSpec(memory_space=pl.ANY)] * len(extra),
        out_specs=pl.BlockSpec((tb, d), lambda i: (first + i, 0)),
        out_shape=jax.ShapeDtypeStruct((n, d), BF16),
        scratch_shapes=[pltpu.VMEM((tb, ff), BF16)],
        input_output_aliases={3: 0} if extra else {},
        compiler_params=_params(),
        cost_estimate=_cost(4 * count * tb * d * ff, 4 * count * tb * d + 4 * d * ff, count * tb * ff),
        name="mlp",
    )(a, w1, w2, *extra)


def _logits_block(z_ref, x, w_ref, lab, lo, vt):
    tb = x.shape[0]
    lab8 = jnp.broadcast_to(lab, (8, tb))
    sub = lax.broadcasted_iota(jnp.int32, (vt // 8, 8, tb), 0) * 8 + lax.broadcasted_iota(jnp.int32, (vt // 8, 8, tb), 1)
    m8 = s8 = t8 = None
    for v in range(w_ref.shape[0] // vt):
        vs = slice(v * vt, (v + 1) * vt)
        z = lax.dot_general(w_ref[vs, :], x, (((1,), (1,)), ((), ())), preferred_element_type=F32)
        if v == 0:
            z = jnp.where(lax.broadcasted_iota(jnp.int32, (vt, tb), 0) >= lo, z, LOW)
        z_ref[vs, :] = z
        zr = z_ref[vs, :].reshape(vt // 8, 8, tb)
        tile_max = jnp.max(zr, axis=0)
        m_new = tile_max if v == 0 else jnp.maximum(m8, tile_max)
        e_sum = jnp.sum(jnp.exp(zr - m_new[None]), axis=0)
        hit = jnp.sum(jnp.where(sub == (lab8 - v * vt)[None], zr, 0.0), axis=0)
        s8 = e_sum if v == 0 else s8 * jnp.exp(m8 - m_new) + e_sum
        t8 = hit if v == 0 else t8 + hit
        m8 = m_new
    m = jnp.max(m8, axis=0, keepdims=True)
    s = jnp.sum(s8 * jnp.exp(m8 - m), axis=0, keepdims=True)
    t = jnp.sum(t8, axis=0, keepdims=True)
    return jnp.concatenate([m, s, t, jnp.zeros((5, tb), F32)], axis=0)


def _head_body(
    x_ref, wh_ref, lab_ref, mask_ref, z_ref, xo_ref, wo_ref, coef_out,
    xbuf, wbuf, zbuf, st, got, mine, coef,
    own_sem, w_sem, wo_sem, z_sem, xo_sem, xs_sem, xr_sem, send1, recv1, send2, recv2, *, n_stage, first_row, over, vt,
):
    y, s = lax.axis_index("data"), lax.axis_index("stage")
    h = lax.rem(y + y // 2, 2)
    n_x = n_stage // 2
    x, c = s // 2, lax.rem(s, 2)
    rows = xbuf.shape[2]
    win = wbuf.shape[0]
    n_blk = 2 * n_stage
    y_a = y + 1 - 2 * lax.rem(y, 2)
    sib = s + 1 - 2 * c

    def at(off, flip=0):
        return 2 * lax.rem(x + off, n_x) + lax.rem(c + flip, 2)

    left, right, far = at(n_x - 1), at(1), at(2)
    here = {"data": y, "stage": s}
    to_a = {"data": y_a, "stage": s}
    to_sib = {"data": y, "stage": sib}
    to_left = {"data": y, "stage": left}
    to_right = {"data": y, "stage": right}

    def slot(f, stage):
        return f * n_stage + stage

    sends = [
        (slot(0, s), slot(0, s), to_right, None),
        (slot(0, s), slot(0, s), to_left, None),
        (slot(0, s), slot(1, s), to_a, None),
        (slot(0, s), slot(0, s), to_sib, None),
        (slot(0, left), slot(0, left), to_right, 0),
        (slot(0, right), slot(0, right), to_left, 1),
        (slot(1, s), slot(1, s), to_right, None),
        (slot(1, s), slot(1, s), to_left, None),
        (slot(1, s), slot(1, s), to_sib, None),
        (slot(0, left), slot(0, left), to_sib, None),
        (slot(0, right), slot(0, right), to_sib, None),
        (slot(0, far), slot(1, far), to_a, None),
        (slot(0, far), slot(0, far), to_sib, None),
        (slot(1, left), slot(1, left), to_sib, None),
        (slot(1, right), slot(1, right), to_sib, None),
        (slot(1, far), slot(1, far), to_sib, None),
    ]

    def copy(k):
        src, dst, to, part = sends[k]
        return pltpu.make_async_remote_copy(
            src_ref=xbuf.at[src] if part is None else xbuf.at[src, part],
            dst_ref=xbuf.at[dst] if part is None else xbuf.at[dst, part],
            send_sem=xs_sem.at[k],
            recv_sem=xr_sem.at[n_blk if part == 1 else dst],
            device_id=to,
            device_id_type=MESH,
        )

    def arrival(ref, sem):
        return pltpu.make_async_remote_copy(
            src_ref=ref, dst_ref=ref, send_sem=xs_sem.at[0], recv_sem=sem, device_id=here, device_id_type=MESH
        )

    def got_block(f, stage):
        arrival(xbuf.at[slot(f, stage)], xr_sem.at[slot(f, stage)]).wait_recv()

    def got_half(part):
        i = slot(0, far)
        arrival(xbuf.at[i, part], xr_sem.at[n_blk if part == 1 else i]).wait_recv()

    own = pltpu.make_async_copy(x_ref, xbuf.at[slot(0, s)], own_sem)
    own.start()
    w_load = pltpu.make_async_copy(wh_ref.at[pl.ds(pl.multiple_of(h * first_row, 16), win), :], wbuf, w_sem)
    w_load.start()

    peers = [(f, k) for f in range(2) for k in range(n_stage) if (f, k) != (0, 0)]

    def peer(f, k):
        return {"data": y if f == 0 else y_a, "stage": lax.rem(s + k, n_stage)}

    barrier = pltpu.get_barrier_semaphore()
    for f, k in peers:
        pl.semaphore_signal(barrier, inc=1, device_id=peer(f, k), device_id_type=MESH)
    pl.semaphore_wait(barrier, len(peers))

    own.wait()
    for k in range(4):
        copy(k).start()
    w_load.wait()
    w_out = pltpu.make_async_copy(wbuf, wo_ref, wo_sem)
    w_out.start()

    def quarter(stage):
        return pl.ds(pl.multiple_of(stage * rows, rows), rows)

    def z_copy(zs, b, f, stage):
        return pltpu.make_async_copy(
            zbuf.at[zs, :, pl.ds(b * rows, rows)],
            z_ref.at[2 * (1 - f) + b, :, quarter(stage)],
            z_sem.at[zs, b],
        )

    def x_copy(f, stage):
        i = slot(f, stage)
        return pltpu.make_async_copy(xbuf.at[i], xo_ref.at[pl.ds(2 * (1 - f), 2), quarter(stage), :], xo_sem.at[i])

    def step(i, carry):
        @pl.when(i == 1)
        def _():
            got_block(0, sib)

        @pl.when(i == 2)
        def _():
            got_block(1, s)
            got_block(0, left)
            got_block(0, right)
            for k in range(4, 11):
                copy(k).start()

        @pl.when(i == 5)
        def _():
            got_half(0)
            got_half(1)
            copy(11).start()
            copy(12).start()
            got_block(1, sib)

        @pl.when(i == 6)
        def _():
            got_block(0, at(n_x - 1, 1))

        @pl.when(i == 7)
        def _():
            got_block(0, at(1, 1))

        @pl.when(i == 9)
        def _():
            got_block(0, at(2, 1))

        @pl.when(i == 10)
        def _():
            got_block(1, left)
            got_block(1, right)
            copy(13).start()
            copy(14).start()

        @pl.when(i == 12)
        def _():
            got_block(1, far)
            copy(15).start()
            got_block(1, at(n_x - 1, 1))

        @pl.when(i == 13)
        def _():
            got_block(1, at(1, 1))

        @pl.when(i == 15)
        def _():
            got_block(1, at(2, 1))

        def among(*ks):
            return functools.reduce(jnp.logical_or, [i == k for k in ks])

        f = jnp.where(jnp.logical_or(among(2, 5), i >= 10), 1, 0)
        flip = jnp.where(among(1, 5, 6, 7, 9, 12, 13, 15), 1, 0)
        off = jnp.where(among(3, 6, 10, 12), n_x - 1, jnp.where(among(4, 7, 11, 13), 1, jnp.where(among(8, 9, 14, 15), 2, 0)))
        stage = at(off, flip)
        blk = slot(f, stage)
        zs = lax.rem(i, 2)

        @pl.when(i >= 2)
        def _():
            for b in range(2):
                z_copy(zs, b, f, stage).wait()

        x_copy(f, stage).start()
        lab = lab_ref[f, :, pl.ds(pl.multiple_of(stage * 2 * rows, 2 * rows), 2 * rows)]
        res = _logits_block(zbuf.at[zs], xbuf[blk].reshape(2 * rows, -1), wbuf, lab, over * h, vt)
        for b in range(2):
            st[2 * (1 - f) + b, :, quarter(stage)] = res[:, b * rows:(b + 1) * rows]
            z_copy(zs, b, f, stage).start()
        return carry

    lax.fori_loop(0, n_blk, step, 0)

    first = []
    for f, k in peers:
        c1 = pltpu.make_async_remote_copy(
            src_ref=st.at[pl.ds(2 * (1 - f), 2), :, quarter(lax.rem(s + k, n_stage))],
            dst_ref=got.at[slot(f, k)],
            send_sem=send1.at[slot(f, k)],
            recv_sem=recv1.at[slot(f, k)],
            device_id=peer(f, k),
            device_id_type=MESH,
        )
        c1.start()
        first.append(c1)
    weight = mask_ref[...].astype(F32)
    denom = jnp.maximum(jnp.sum(weight), 1.0)
    mu = jnp.stack([mask_ref[:, pl.ds(pl.multiple_of((2 * s + b) * rows, rows), rows)].astype(F32) for b in range(2)])
    scale = mu / denom
    for c1 in first:
        c1.wait_recv()
    parts = [st[2:4, :, quarter(s)]] + [got[slot(f, k)] for f, k in peers]
    m = functools.reduce(jnp.maximum, [p[:, 0:1, :] for p in parts])
    z = sum(p[:, 1:2, :] * jnp.exp(p[:, 0:1, :] - m) for p in parts)
    t = sum(p[:, 2:3, :] for p in parts)
    loss = scale * (jnp.log(z) + m - t)
    res = jnp.concatenate([m, scale / z, scale, loss, jnp.zeros((2, 4, rows), F32)], axis=1)
    mine[...] = res
    second = []
    for f, k in peers:
        c2 = pltpu.make_async_remote_copy(
            src_ref=mine,
            dst_ref=coef.at[pl.ds(2 * (1 - f), 2), :, quarter(s)],
            send_sem=send2.at[slot(f, k)],
            recv_sem=recv2.at[slot(f, k)],
            device_id=peer(f, k),
            device_id_type=MESH,
        )
        c2.start()
        second.append(c2)
    coef[2:4, :, quarter(s)] = res
    for zs in range(2):
        for b in range(2):
            z_copy(zs, b, 0, s).wait()
    for i in range(n_blk):
        x_copy(i // n_stage, i % n_stage).wait()
    w_out.wait()
    for k in range(len(sends)):
        copy(k).wait_send()
    for c1 in first:
        c1.wait_send()
    for c2 in second:
        c2.wait_recv()
    coef_out[...] = coef[...]
    for c2 in second:
        c2.wait_send()


def head(x_rows, w_head, lab, mask, n_stage, win, vt):
    rows, d = x_rows.shape
    hr = rows // 2
    shard = w_head.shape[0]
    n = n_stage * hr
    n_blk = 2 * n_stage
    vm = pl.BlockSpec(memory_space=pltpu.VMEM)
    hbm = pl.BlockSpec(memory_space=pl.ANY)
    dma = pltpu.SemaphoreType.DMA
    x3 = x_rows.reshape(2, hr, d)
    total = n_blk * rows
    return pl.pallas_call(
        functools.partial(_head_body, n_stage=n_stage, first_row=shard - win, over=2 * win - shard, vt=vt),
        in_specs=[hbm, hbm, vm, vm],
        out_specs=[hbm, hbm, hbm, vm],
        out_shape=[
            jax.ShapeDtypeStruct((4, win, n), F32),
            jax.ShapeDtypeStruct((4, n, d), BF16),
            jax.ShapeDtypeStruct((win, d), BF16),
            jax.ShapeDtypeStruct((4, 8, n), F32),
        ],
        scratch_shapes=[
            pltpu.VMEM((n_blk, 2, hr, d), BF16),
            pltpu.VMEM((win, d), BF16),
            pltpu.VMEM((2, win, rows), F32),
            pltpu.VMEM((4, 8, n), F32),
            pltpu.VMEM((n_blk, 2, 8, hr), F32),
            pltpu.VMEM((2, 8, hr), F32),
            pltpu.VMEM((4, 8, n), F32),
            dma, dma, dma, dma((2, 2)), dma((n_blk,)), dma((16,)), dma((n_blk + 1,)),
            dma((n_blk,)), dma((n_blk,)), dma((n_blk,)), dma((n_blk,)),
        ],
        compiler_params=_params(56, collective_id=0, has_side_effects=True),
        cost_estimate=_cost(2 * total * d * win, 4 * total * win, total * win),
        name="head",
    )(x3, w_head, lab, mask)


def _gdw_body(tile_ref, coef_ref, lab_ref, z_ref, x_ref, *rest, ch, nv):
    g_ref, dw_refs, acc_ref = rest[-nv - 2], rest[-nv - 1:-1], rest[-1]
    t, v = pl.program_id(0), pl.program_id(1)
    vt, tb = z_ref.shape[1:]
    row0 = (tile_ref[0] + v) * vt
    sub = lax.broadcasted_iota(jnp.int32, (vt // 8, 8, ch), 0) * 8 + lax.broadcasted_iota(jnp.int32, (vt // 8, 8, ch), 1)
    acc = None
    for c in range(tb // ch):
        cs = slice(c * ch, (c + 1) * ch)
        m8 = jnp.broadcast_to(coef_ref[0, 0:1, cs], (8, ch))
        c8 = jnp.broadcast_to(coef_ref[0, 1:2, cs], (8, ch))
        r8 = jnp.broadcast_to(coef_ref[0, 2:3, cs], (8, ch))
        lab8 = jnp.broadcast_to(lab_ref[0, 0:1, cs], (8, ch)) - row0
        zr = z_ref[0, :, cs].reshape(vt // 8, 8, ch)
        e = jnp.exp(zr - m8[None]) * c8[None]
        g = jnp.where(sub == lab8[None], e - r8[None], e)
        gb = g.reshape(vt, ch).astype(BF16)
        g_ref[0, :, cs] = gb
        d = jnp.dot(gb, x_ref[0, cs, :], preferred_element_type=F32)
        acc = d if acc is None else acc + d
    if nv == 1:
        dw_refs[0][...] = jnp.where(t == 0, 0.0, dw_refs[0][...]) + acc
        return
    acc_ref[...] = acc
    for j in range(nv):
        @pl.when(v == j)
        def _(dw_ref=dw_refs[j]):
            dw_ref[...] = jnp.where(t == 0, 0.0, dw_ref[...]) + acc_ref[...]


def gdw(tile, nv, coef, lab, z, x, g, vt, ch=512):
    nq, n, d = x.shape
    win = z.shape[1]
    extra = [] if g is None else [g]
    ch = min(ch, n)
    spec = pltpu.PrefetchScalarGridSpec(
        num_scalar_prefetch=1,
        grid=(nq, nv),
        in_specs=[
            pl.BlockSpec((1, 8, n), lambda t, v, i: (t, 0, 0)),
            pl.BlockSpec((1, 1, n), lambda t, v, i: (t, 0, 0)),
            pl.BlockSpec((1, vt, n), lambda t, v, i: (t, i[0] + v, 0)),
            pl.BlockSpec((1, n, d), lambda t, v, i: (t, 0, 0)),
        ] + [pl.BlockSpec(memory_space=pl.ANY)] * len(extra),
        out_specs=[
            pl.BlockSpec((1, vt, n), lambda t, v, i: (t, i[0] + v, 0)),
        ] + [pl.BlockSpec((vt, d), lambda t, v, i: (0, 0))] * nv,
        scratch_shapes=[pltpu.VMEM((vt if nv > 1 else 8, d), F32)],
    )
    rows = nv * vt
    return pl.pallas_call(
        functools.partial(_gdw_body, ch=ch, nv=nv),
        grid_spec=spec,
        out_shape=[jax.ShapeDtypeStruct((nq, win, n), BF16)] + [jax.ShapeDtypeStruct((vt, d), F32)] * nv,
        input_output_aliases={5: 0} if extra else {},
        compiler_params=_params(62),
        cost_estimate=_cost(2 * nq * n * d * rows, 6 * nq * n * rows + 2 * nq * n * d, nq * n * rows),
        name="gdw",
    )(tile, coef, lab, z, x, *extra)


def _dx_body(g_ref, w_ref, o_ref):
    o_ref[...] = lax.dot_general(g_ref[0], w_ref[...], (((0,), (0,)), ((), ())), preferred_element_type=F32)


def dx(g, w, q, tb=512):
    n = g.shape[2]
    win, d = w.shape
    tb = min(tb, n)
    return pl.pallas_call(
        _dx_body,
        grid=(n // tb,),
        in_specs=[
            pl.BlockSpec((1, win, tb), lambda i: (q, 0, i)),
            pl.BlockSpec((win, d), lambda i: (0, 0)),
        ],
        out_specs=pl.BlockSpec((tb, d), lambda i: (i, 0)),
        out_shape=jax.ShapeDtypeStruct((n, d), F32),
        compiler_params=_params(),
        cost_estimate=_cost(2 * n * d * win, 2 * n * win + 4 * n * d),
        name="dx",
    )(g, w)


def solution(mesh):
    n_data, n_stage = mesh.shape["data"], mesh.shape["stage"]
    tok_spec = P(("pod", "data", "stage"), None)
    rep_spec = P(("pod", "data"))
    vocab_spec = P("stage", None)
    layer_spec = P("stage", None, None)
    swap_a = [(i, i ^ 1) for i in range(n_data)]
    swap_b = [(i, n_data - 1 - i) for i in range(n_data)]

    def local_step(x_rows, w_head, labels, loss_mask, w_embed, tok_ids, act_in, w_up, w_down):
        y, s = lax.axis_index("data"), lax.axis_index("stage")
        shard, d = w_head.shape
        yh = y >> 1
        h = (y ^ yh) & 1
        vt = -(-shard // (2 * N_TILE * 16)) * 16
        win = N_TILE * vt
        first_row = shard - win
        lo = (2 * win - shard) * h

        def over_a(v):
            return lax.ppermute(v, "data", swap_a)

        def over_b(v):
            return lax.ppermute(v, "data", swap_b)

        lab_a = over_a(labels)

        def local(lab):
            lab = lab - (s * shard + h * first_row)
            return jnp.where(lab < lo, -1, lab)

        n_tok = labels.shape[0]
        lab_two = jnp.stack([local(labels), local(lab_a)])
        z, x_all, w_win, coef = head(x_rows, w_head, lab_two.reshape(2, 1, n_tok), loss_mask.reshape(1, -1), n_stage, win, VT_LOGITS(win))
        half_rows = n_tok // n_stage // 2
        lab = lab_two[::-1].reshape(2, n_stage, 2, half_rows).transpose(0, 2, 1, 3).reshape(4, 1, n_tok // 2)

        loss_q = jnp.sum(coef[:, 3, :], axis=1)
        loss_pair = (loss_q[0] + loss_q[1]) + (loss_q[2] + loss_q[3])
        loss_far = over_b(loss_pair.reshape(1, 1))[0, 0]
        mean_loss = (loss_pair + loss_far) / n_data

        half = N_TILE // 2
        far_tile, own_tile = (1 - yh) * half, yh * half
        sent = []
        g, *sent_parts = gdw(far_tile.reshape(1), 1, coef, lab, z, x_all, None, vt)
        g, *more = gdw((far_tile + 1).reshape(1), half - 1, coef, lab, z, x_all, g, vt)
        for part in sent_parts + more:
            sent.append(over_b(part))
        g, *kept = gdw(own_tile.reshape(1), half, coef, lab, z, x_all, g, vt)

        rs = []
        for q in range(4):
            dx_q = dx(g, w_win, q)
            rs.append(lax.psum_scatter(dx_q, "stage", scatter_dimension=0, tiled=True))
        gx = []
        for q in range(2):
            gx.append(over_a(rs[q]))
        grad_x = jnp.concatenate([rs[2] + gx[0], rs[3] + gx[1]], axis=0)

        offset = s * shard
        local_ids = tok_ids - offset
        in_slice = (local_ids >= 0) & (local_ids < shard)
        rows_emb = jnp.take(w_embed, jnp.clip(local_ids, 0, shard - 1), axis=0)
        emb_part = jnp.where(in_slice[:, None], rows_emb, jnp.zeros_like(rows_emb))
        embed_out = lax.psum_scatter(emb_part, "stage", scatter_dimension=0, tiled=True)

        mlp_out = mlp(act_in, w_up[0], w_down[0], None, 0, act_in.shape[0] // 512)

        grad_head = jnp.zeros((shard, d), BF16)
        for j in range(half):
            fin = lax.optimization_barrier(((kept[j] + sent[j]) / n_data).astype(BF16))
            fin_b = over_b(fin)
            fin_a = over_a(fin)
            fin_ab = over_a(fin_b)
            for v, hh, part in ((fin, h, yh), (fin_a, 1 - h, yh), (fin_b, h, 1 - yh), (fin_ab, 1 - h, 1 - yh)):
                row = hh * first_row + (part * half + j) * vt
                grad_head = lax.dynamic_update_slice(grad_head, v, (row, 0))

        return mean_loss.reshape(1), grad_x, grad_head, embed_out, mlp_out

    return jax.shard_map(
        local_step,
        mesh=mesh,
        in_specs=(tok_spec, vocab_spec, rep_spec, rep_spec, vocab_spec, rep_spec, tok_spec, layer_spec, layer_spec),
        out_specs=(P("pod"), tok_spec, P(("pod", "stage"), None), tok_spec, tok_spec),
        check_vma=False,
    )
```

```python
import functools

import jax
import jax.numpy as jnp
from jax import lax
from jax.experimental import pallas as pl
from jax.experimental.pallas import tpu as pltpu
from jax.sharding import PartitionSpec as P

MESH = pl.DeviceIdType.MESH
F32 = jnp.float32
BF16 = jnp.bfloat16
N_TILE = 6
MLP_EIGHTHS = (3, 3, 2)


def logits_tile(win):
    return next(v for v in range(352, 0, -16) if win % v == 0 and v <= 288)


LOW = -1e30


def _params(mib=60, **kw):
    return pltpu.CompilerParams(vmem_limit_bytes=mib * 2**20, **kw)


def _cost(flops, nbytes, trans=0):
    return pl.CostEstimate(flops=int(flops), bytes_accessed=int(nbytes), transcendentals=int(trans))


def _mlp_body(a_ref, w1_ref, w2_ref, *rest, chunk):
    o_ref, u_ref = rest[-2:]
    ff = w1_ref.shape[1]
    for c in range(ff // chunk):
        cs = slice(c * chunk, (c + 1) * chunk)
        h = jnp.dot(a_ref[...], w1_ref[:, cs], preferred_element_type=F32)
        u_ref[:, cs] = jax.nn.gelu(h).astype(BF16)
    y = jnp.dot(u_ref[...], w2_ref[...], preferred_element_type=F32)
    o_ref[...] = (a_ref[...].astype(F32) + y).astype(BF16)


def mlp(a, w1, w2, out, first, count, tb=512):
    n, d = a.shape
    ff = w1.shape[1]
    extra = [] if out is None else [out]
    return pl.pallas_call(
        functools.partial(_mlp_body, chunk=512),
        grid=(count,),
        in_specs=[
            pl.BlockSpec((tb, d), lambda i: (first + i, 0)),
            pl.BlockSpec((d, ff), lambda i: (0, 0)),
            pl.BlockSpec((ff, d), lambda i: (0, 0)),
        ] + [pl.BlockSpec(memory_space=pl.ANY)] * len(extra),
        out_specs=pl.BlockSpec((tb, d), lambda i: (first + i, 0)),
        out_shape=jax.ShapeDtypeStruct((n, d), BF16),
        scratch_shapes=[pltpu.VMEM((tb, ff), BF16)],
        input_output_aliases={3: 0} if extra else {},
        compiler_params=_params(),
        cost_estimate=_cost(4 * count * tb * d * ff, 4 * count * tb * d + 4 * d * ff, count * tb * ff),
        name="mlp",
    )(a, w1, w2, *extra)


def _logits_block(z_ref, x, w_ref, lab, end, vt):
    tb = x.shape[0]
    lab8 = jnp.broadcast_to(lab, (8, tb))
    sub = lax.broadcasted_iota(jnp.int32, (vt // 8, 8, tb), 0) * 8 + lax.broadcasted_iota(jnp.int32, (vt // 8, 8, tb), 1)
    m8 = s8 = t8 = None
    n_v = w_ref.shape[0] // vt
    for v in range(n_v):
        vs = slice(v * vt, (v + 1) * vt)
        z = lax.dot_general(w_ref[vs, :], x, (((1,), (1,)), ((), ())), preferred_element_type=F32)
        if v == n_v - 1:
            z = jnp.where(lax.broadcasted_iota(jnp.int32, (vt, tb), 0) + v * vt < end, z, LOW)
        z_ref[vs, :] = z
        zr = z_ref[vs, :].reshape(vt // 8, 8, tb)
        tile_max = jnp.max(zr, axis=0)
        m_new = tile_max if v == 0 else jnp.maximum(m8, tile_max)
        e_sum = jnp.sum(jnp.exp(zr - m_new[None]), axis=0)
        hit = jnp.sum(jnp.where(sub == (lab8 - v * vt)[None], zr, 0.0), axis=0)
        s8 = e_sum if v == 0 else s8 * jnp.exp(m8 - m_new) + e_sum
        t8 = hit if v == 0 else t8 + hit
        m8 = m_new
    m = jnp.max(m8, axis=0, keepdims=True)
    s = jnp.sum(s8 * jnp.exp(m8 - m), axis=0, keepdims=True)
    t = jnp.sum(t8, axis=0, keepdims=True)
    return jnp.concatenate([m, s, t, jnp.zeros((5, tb), F32)], axis=0)


def _head_body(
    x_ref, wh_ref, lab_ref, mask_ref, z_ref, xo_ref, wo_ref, coef_out,
    xbuf, wbuf, zbuf, st, got, mine, coef,
    own_sem, w_sem, wo_sem, z_sem, xo_sem, xs_sem, xr_sem, send1, recv1, send2, recv2, *, n_stage, first_row, over, vt,
):
    y, s = lax.axis_index("data"), lax.axis_index("stage")
    h = lax.rem(y + y // 2, 2)
    n_x = n_stage // 2
    x, c = s // 2, lax.rem(s, 2)
    n_q, rows = xbuf.shape[1:3]
    win = wbuf.shape[0]
    n_blk = 2 * n_stage
    y_a = y + 1 - 2 * lax.rem(y, 2)
    sib = s + 1 - 2 * c

    def at(off, flip=0):
        return 2 * lax.rem(x + off, n_x) + lax.rem(c + flip, 2)

    left, right, far = at(n_x - 1), at(1), at(2)
    here = {"data": y, "stage": s}
    to_a = {"data": y_a, "stage": s}
    to_sib = {"data": y, "stage": sib}
    to_left = {"data": y, "stage": left}
    to_right = {"data": y, "stage": right}

    def slot(f, stage):
        return f * n_stage + stage

    sends = [
        (slot(0, s), slot(0, s), to_right, None),
        (slot(0, s), slot(0, s), to_left, None),
        (slot(0, s), slot(1, s), to_a, None),
        (slot(0, s), slot(0, s), to_sib, None),
        (slot(0, left), slot(0, left), to_right, 0),
        (slot(0, right), slot(0, right), to_left, 1),
        (slot(1, s), slot(1, s), to_right, None),
        (slot(1, s), slot(1, s), to_left, None),
        (slot(1, s), slot(1, s), to_sib, None),
        (slot(0, left), slot(0, left), to_sib, None),
        (slot(0, right), slot(0, right), to_sib, None),
        (slot(0, far), slot(1, far), to_a, None),
        (slot(0, far), slot(0, far), to_sib, None),
        (slot(1, left), slot(1, left), to_sib, None),
        (slot(1, right), slot(1, right), to_sib, None),
        (slot(1, far), slot(1, far), to_sib, None),
    ]

    def half(i, part):
        return xbuf.at[i, pl.ds(part * n_q // 2, n_q // 2)]

    def copy(k):
        src, dst, to, part = sends[k]
        return pltpu.make_async_remote_copy(
            src_ref=xbuf.at[src] if part is None else half(src, part),
            dst_ref=xbuf.at[dst] if part is None else half(dst, part),
            send_sem=xs_sem.at[k],
            recv_sem=xr_sem.at[n_blk if part == 1 else dst],
            device_id=to,
            device_id_type=MESH,
        )

    def arrival(ref, sem):
        return pltpu.make_async_remote_copy(
            src_ref=ref, dst_ref=ref, send_sem=xs_sem.at[0], recv_sem=sem, device_id=here, device_id_type=MESH
        )

    def got_block(f, stage):
        arrival(xbuf.at[slot(f, stage)], xr_sem.at[slot(f, stage)]).wait_recv()

    def got_half(part):
        i = slot(0, far)
        arrival(half(i, part), xr_sem.at[n_blk if part == 1 else i]).wait_recv()

    own = pltpu.make_async_copy(x_ref, xbuf.at[slot(0, s)], own_sem)
    own.start()
    w_load = pltpu.make_async_copy(wh_ref.at[pl.ds(pl.multiple_of(h * first_row, 16), win), :], wbuf, w_sem)
    w_load.start()

    peers = [(f, k) for f in range(2) for k in range(n_stage) if (f, k) != (0, 0)]

    def peer(f, k):
        return {"data": y if f == 0 else y_a, "stage": lax.rem(s + k, n_stage)}

    barrier = pltpu.get_barrier_semaphore()
    for f, k in peers:
        pl.semaphore_signal(barrier, inc=1, device_id=peer(f, k), device_id_type=MESH)
    pl.semaphore_wait(barrier, len(peers))

    own.wait()
    for k in range(4):
        copy(k).start()
    w_load.wait()
    w_out = pltpu.make_async_copy(wbuf, wo_ref, wo_sem)
    w_out.start()

    def quarter(stage):
        return pl.ds(pl.multiple_of(stage * rows, rows), rows)

    def z_copy(zs, b, f, stage):
        return pltpu.make_async_copy(
            zbuf.at[zs, :, pl.ds(b * rows, rows)],
            z_ref.at[n_q * (1 - f) + b, stage],
            z_sem.at[zs, b],
        )

    def x_copy(f, stage):
        i = slot(f, stage)
        return pltpu.make_async_copy(xbuf.at[i], xo_ref.at[pl.ds(n_q * (1 - f), n_q), stage], xo_sem.at[i])

    def step(i, carry):
        @pl.when(i == 1)
        def _():
            got_block(0, sib)

        @pl.when(i == 2)
        def _():
            got_block(1, s)
            got_block(0, left)
            got_block(0, right)
            for k in range(4, 11):
                copy(k).start()

        @pl.when(i == 5)
        def _():
            got_half(0)
            got_half(1)
            copy(11).start()
            copy(12).start()
            got_block(1, sib)

        @pl.when(i == 6)
        def _():
            got_block(0, at(n_x - 1, 1))

        @pl.when(i == 7)
        def _():
            got_block(0, at(1, 1))

        @pl.when(i == 9)
        def _():
            got_block(0, at(2, 1))

        @pl.when(i == 10)
        def _():
            got_block(1, left)
            got_block(1, right)
            copy(13).start()
            copy(14).start()

        @pl.when(i == 12)
        def _():
            got_block(1, far)
            copy(15).start()
            got_block(1, at(n_x - 1, 1))

        @pl.when(i == 13)
        def _():
            got_block(1, at(1, 1))

        @pl.when(i == 15)
        def _():
            got_block(1, at(2, 1))

        def among(*ks):
            return functools.reduce(jnp.logical_or, [i == k for k in ks])

        f = jnp.where(jnp.logical_or(among(2, 5), i >= 10), 1, 0)
        flip = jnp.where(among(1, 5, 6, 7, 9, 12, 13, 15), 1, 0)
        off = jnp.where(among(3, 6, 10, 12), n_x - 1, jnp.where(among(4, 7, 11, 13), 1, jnp.where(among(8, 9, 14, 15), 2, 0)))
        stage = at(off, flip)
        blk = slot(f, stage)
        zs = lax.rem(i, 2)

        @pl.when(i >= 2)
        def _():
            for b in range(n_q):
                z_copy(zs, b, f, stage).wait()

        x_copy(f, stage).start()
        lab = lab_ref[f, :, pl.ds(pl.multiple_of(stage * n_q * rows, n_q * rows), n_q * rows)]
        res = _logits_block(zbuf.at[zs], xbuf[blk].reshape(n_q * rows, -1), wbuf, lab, win - over * (1 - h), vt)
        for b in range(n_q):
            st[n_q * (1 - f) + b, :, quarter(stage)] = res[:, b * rows:(b + 1) * rows]
            z_copy(zs, b, f, stage).start()
        return carry

    lax.fori_loop(0, n_blk, step, 0)

    first = []
    for f, k in peers:
        c1 = pltpu.make_async_remote_copy(
            src_ref=st.at[pl.ds(n_q * (1 - f), n_q), :, quarter(lax.rem(s + k, n_stage))],
            dst_ref=got.at[slot(f, k)],
            send_sem=send1.at[slot(f, k)],
            recv_sem=recv1.at[slot(f, k)],
            device_id=peer(f, k),
            device_id_type=MESH,
        )
        c1.start()
        first.append(c1)
    weight = mask_ref[...].astype(F32)
    denom = jnp.maximum(jnp.sum(weight), 1.0)
    mu = jnp.stack([mask_ref[:, pl.ds(pl.multiple_of((n_q * s + b) * rows, rows), rows)].astype(F32) for b in range(n_q)])
    scale = mu / denom
    for c1 in first:
        c1.wait_recv()
    parts = [st[n_q:2 * n_q, :, quarter(s)]] + [got[slot(f, k)] for f, k in peers]
    m = functools.reduce(jnp.maximum, [p[:, 0:1, :] for p in parts])
    z = sum(p[:, 1:2, :] * jnp.exp(p[:, 0:1, :] - m) for p in parts)
    t = sum(p[:, 2:3, :] for p in parts)
    loss = scale * (jnp.log(z) + m - t)
    res = jnp.concatenate([m, scale / z, scale, loss, jnp.zeros((n_q, 4, rows), F32)], axis=1)
    mine[...] = res
    second = []
    for f, k in peers:
        c2 = pltpu.make_async_remote_copy(
            src_ref=mine,
            dst_ref=coef.at[pl.ds(n_q * (1 - f), n_q), :, quarter(s)],
            send_sem=send2.at[slot(f, k)],
            recv_sem=recv2.at[slot(f, k)],
            device_id=peer(f, k),
            device_id_type=MESH,
        )
        c2.start()
        second.append(c2)
    coef[n_q:2 * n_q, :, quarter(s)] = res
    for zs in range(2):
        for b in range(n_q):
            z_copy(zs, b, 0, s).wait()
    for i in range(n_blk):
        x_copy(i // n_stage, i % n_stage).wait()
    w_out.wait()
    for k in range(len(sends)):
        copy(k).wait_send()
    for c1 in first:
        c1.wait_send()
    for c2 in second:
        c2.wait_recv()
    coef_out[...] = coef[...]
    for c2 in second:
        c2.wait_send()


def head(x_rows, w_head, lab, mask, n_stage, win, vt):
    rows, d = x_rows.shape
    n_q = 4
    hr = rows // n_q
    shard = w_head.shape[0]
    n = n_stage * hr
    n_blk = 2 * n_stage
    vm = pl.BlockSpec(memory_space=pltpu.VMEM)
    hbm = pl.BlockSpec(memory_space=pl.ANY)
    dma = pltpu.SemaphoreType.DMA
    x3 = x_rows.reshape(n_q, hr, d)
    total = n_blk * rows
    return pl.pallas_call(
        functools.partial(_head_body, n_stage=n_stage, first_row=shard - win, over=2 * win - shard, vt=vt),
        in_specs=[hbm, hbm, vm, vm],
        out_specs=[hbm, hbm, hbm, vm],
        out_shape=[
            jax.ShapeDtypeStruct((2 * n_q, n_stage, win, hr), F32),
            jax.ShapeDtypeStruct((2 * n_q, n_stage, hr, d), BF16),
            jax.ShapeDtypeStruct((win, d), BF16),
            jax.ShapeDtypeStruct((2 * n_q, 8, n), F32),
        ],
        scratch_shapes=[
            pltpu.VMEM((n_blk, n_q, hr, d), BF16),
            pltpu.VMEM((win, d), BF16),
            pltpu.VMEM((2, win, rows), F32),
            pltpu.VMEM((2 * n_q, 8, n), F32),
            pltpu.VMEM((n_blk, n_q, 8, hr), F32),
            pltpu.VMEM((n_q, 8, hr), F32),
            pltpu.VMEM((2 * n_q, 8, n), F32),
            dma, dma, dma, dma((2, n_q)), dma((n_blk,)), dma((16,)), dma((n_blk + 1,)),
            dma((n_blk,)), dma((n_blk,)), dma((n_blk,)), dma((n_blk,)),
        ],
        compiler_params=_params(56, collective_id=0, has_side_effects=True),
        cost_estimate=_cost(2 * total * d * win, 4 * total * win, total * win),
        name="head",
    )(x3, w_head, lab, mask)


DONE = (12, 17, 27, 31, 38, 41, 44, 47)
N_STEP = 48
AFTER_D, AFTER_1, AFTER_2 = 3, 9, 14
N_SLOT = 4


def _step_of(u):
    phases = (
        (0, 1, 0, 0),
        (8, 5, 1, 0),
        (18, 1, 1, 2),
        (24, 4, 2, 2),
        (32, 1, 2, 4),
        (36, 3, 3, 4),
    )
    tile = group = jnp.int32(0)
    for start, n_tile, tile0, group0 in phases:
        k = jnp.maximum(u - start, 0)
        tile = jnp.where(u >= start, tile0 + k % n_tile, tile)
        group = jnp.where(u >= start, group0 + k // n_tile, group)
    return tile, group


def _grads_body(
    lab_ref, coef_ref, z_ref, x_ref, w_ref, dwo0, dwo1, dwo2, rcv0, rcv1, rcv2, tail_o, tail_r, gx_ref,
    dxb, xb, zb, wb, zt, wt, g, gt, dwb, dwt, rd, r1, r2, ra,
    z_sem, x_sem, w_sem, zt_sem, wt_sem, o_sem, sb_sem, rb_sem, sd_sem, rd_sem, s1_sem, r1_sem, s2_sem, r2_sem, sa_sem, ra_sem,
    *, n_stage,
):
    y, s = lax.axis_index("data"), lax.axis_index("stage")
    n_x = n_stage // 2
    x, c = s // 2, lax.rem(s, 2)
    yh = y // 2
    y_a = y + 1 - 2 * lax.rem(y, 2)
    y_b = lax.axis_size("data") - 1 - y
    x_1, x_3 = x + 1 - 2 * lax.rem(x, 2), n_x - 1 - x
    vt = dwb.shape[1]
    n_own = dwb.shape[0] // 2
    n_t, _, _, rows, d = dxb.shape
    n_tail = dwt.shape[0]
    tail_row = 2 * n_own * vt
    rcv, dwo = (rcv0, rcv1, rcv2), (dwo0, dwo1, dwo2)
    to_sib = {"data": y, "stage": 2 * x + 1 - c}
    to_a = {"data": y_a, "stage": s}
    to_b = {"data": y_b, "stage": s}

    def stage_at(xx):
        return {"data": y, "stage": 2 * xx + c}

    def remote(src, dst, send, recv, to):
        return pltpu.make_async_remote_copy(
            src_ref=src, dst_ref=dst, send_sem=send, recv_sem=recv, device_id=to, device_id_type=MESH
        )

    def row0(tile):
        half = jnp.where(tile < n_own, 1 - yh, yh)
        return pl.multiple_of((half * n_own + tile % n_own) * vt, vt)

    def loads(u):
        tile, t = _step_of(u)
        k = u % 2
        r = pl.ds(row0(tile), vt)
        return (
            pltpu.make_async_copy(z_ref.at[t, :, r, :], zb.at[k], z_sem.at[k]),
            pltpu.make_async_copy(x_ref.at[t], xb.at[k], x_sem.at[k]),
            pltpu.make_async_copy(w_ref.at[r, :], wb.at[k], w_sem.at[k]),
        )

    def tail_load(t):
        return pltpu.make_async_copy(z_ref.at[t, :, pl.ds(tail_row, n_tail), :], zt, zt_sem)

    for cp in loads(jnp.int32(0)):
        cp.start()
    w_tail = pltpu.make_async_copy(w_ref.at[pl.ds(tail_row, n_tail), :], wt, wt_sem)
    w_tail.start()

    peers = (to_sib, to_a, to_b, stage_at(x_1), stage_at(x_3))
    barrier = pltpu.get_barrier_semaphore()
    for p in peers:
        pl.semaphore_signal(barrier, inc=1, device_id=p, device_id_type=MESH)
    pl.semaphore_wait(barrier, len(peers))
    w_tail.wait()

    def send_d(t):
        return remote(dxb.at[t, :, 1 - c], rd.at[t % 2], sd_sem.at[t], rd_sem.at[t], to_sib)

    def order(t):
        even = t % 2 == 0
        return jnp.where(even, x_1, x_3), jnp.where(even, x_3, x_1)

    def send_1(t, k):
        p1, _ = order(t)
        mine = p1 if k == 0 else n_x - 1 - x_1
        return remote(dxb.at[t, mine, c], r1.at[t % N_SLOT, k], s1_sem.at[t, k], r1_sem.at[t, k], stage_at(p1))

    def send_2(t):
        _, p2 = order(t)
        return remote(dxb.at[t, p2, c], r2.at[t % N_SLOT], s2_sem.at[t], r2_sem.at[t], stage_at(p2))

    def send_a(t):
        return remote(dxb.at[t, x, c], ra.at[t], sa_sem.at[t], ra_sem.at[t], to_a)

    def scheduled(u, after):
        t = sum(jnp.where(u == done + after, i, 0) for i, done in enumerate(DONE))
        return functools.reduce(jnp.logical_or, [u == done + after for done in DONE]), t

    def exchanges(u):
        now2, t2 = scheduled(u, AFTER_2)

        @pl.when(now2)
        def _():
            send_2(t2).wait_recv()
            dxb[t2, x, c] = dxb[t2, x, c] + r2[t2 % N_SLOT]

            @pl.when(t2 < n_t // 2)
            def _():
                send_a(t2).start()

        now1, t1 = scheduled(u, AFTER_1)

        @pl.when(now1)
        def _():
            _, p2 = order(t1)
            send_1(t1, 0).wait_recv()
            send_1(t1, 1).wait_recv()
            dxb[t1, p2, c] = dxb[t1, p2, c] + r1[t1 % N_SLOT, 1]
            send_2(t1).start()
            dxb[t1, x, c] = dxb[t1, x, c] + r1[t1 % N_SLOT, 0]

        now, t = scheduled(u, AFTER_D)

        @pl.when(now)
        def _():
            send_d(t).wait_recv()
            for xx in range(n_x):
                dxb[t, xx, c] = dxb[t, xx, c] + rd[t % 2, xx]
            send_1(t, 0).start()
            send_1(t, 1).start()

    def g_tile(z, g_out, t, base):
        n_row = z.shape[1]
        sub = lax.broadcasted_iota(jnp.int32, (n_row // 8, 8, rows), 0) * 8 + lax.broadcasted_iota(jnp.int32, (n_row // 8, 8, rows), 1)
        for i in range(n_stage):
            cs = slice(i * rows, (i + 1) * rows)
            m8 = jnp.broadcast_to(coef_ref[t, 0:1, cs], (8, rows))
            c8 = jnp.broadcast_to(coef_ref[t, 1:2, cs], (8, rows))
            q8 = jnp.broadcast_to(coef_ref[t, 2:3, cs], (8, rows))
            lab8 = jnp.broadcast_to(lab_ref[t, :, cs], (8, rows)) - base
            zr = z[i].reshape(n_row // 8, 8, rows)
            e = jnp.exp(zr - m8[None]) * c8[None]
            gi = jnp.where(sub == lab8[None], e - q8[None], e)
            g_out[:, cs] = gi.reshape(n_row, rows).astype(BF16)

    def step(u, carry):
        tile, t = _step_of(u)
        k = u % 2

        @pl.when(u < N_STEP)
        def _():
            for cp in loads(u):
                cp.wait()

        @pl.when(u < N_STEP - 1)
        def _():
            for cp in loads(u + 1):
                cp.start()

        last = jnp.logical_and(tile == 2 * n_own - 1, u < N_STEP)

        @pl.when(last)
        def _():
            tail_load(t).start()

        exchanges(u)

        @pl.when(u < N_STEP)
        def _():
            g_tile(zb.at[k], g, t, row0(tile))
            xk = xb[k].reshape(n_stage * rows, d)
            dxp = lax.dot_general(g[...], wb[k], (((0,), (0,)), ((), ())), preferred_element_type=F32)
            dxb[t] = jnp.where(tile == 0, 0.0, dxb[t]) + dxp.reshape(n_x, 2, rows, d)
            dwb[tile] = jnp.where(t == 0, 0.0, dwb[tile]) + jnp.dot(g[...], xk, preferred_element_type=F32)

        @pl.when(last)
        def _():
            tail_load(t).wait()
            g_tile(zt, gt, t, tail_row)
            xk = xb[k].reshape(n_stage * rows, d)
            dxp = lax.dot_general(gt[...], wt[...], (((0,), (0,)), ((), ())), preferred_element_type=F32)
            dxb[t] = dxb[t] + dxp.reshape(n_x, 2, rows, d)
            dwt[...] = jnp.where(t == 0, 0.0, dwt[...]) + jnp.dot(gt[...], xk, preferred_element_type=F32)
            send_d(t).start()

        for j, end in enumerate((7, 23, 35)):
            @pl.when(u == end)
            def _(j=j):
                send_b(j).start()

        return carry

    def send_b(j):
        return remote(dwb.at[j], rcv[j], sb_sem.at[j], rb_sem.at[j], to_b)

    lax.fori_loop(0, N_STEP, step, 0)

    outs = [pltpu.make_async_copy(dwb.at[n_own + j], dwo[j], o_sem.at[j]) for j in range(n_own)]
    outs.append(pltpu.make_async_copy(dwt, tail_o, o_sem.at[n_own]))
    for cp in outs:
        cp.start()
    tail = remote(dwt, tail_r, sb_sem.at[n_own], rb_sem.at[n_own], to_b)
    tail.start()

    def drain(u, carry):
        exchanges(u)
        return carry

    lax.fori_loop(N_STEP, DONE[-1] + AFTER_2 + 1, drain, 0)

    for q in range(n_t // 2):
        send_a(q).wait_recv()
        gx_ref[q] = dxb[n_t // 2 + q, x, c] + ra[q]
    for cp in outs:
        cp.wait()
    for j in range(n_own):
        send_b(j).wait()
    tail.wait()
    for t in range(n_t):
        send_d(t).wait_send()
        send_1(t, 0).wait_send()
        send_1(t, 1).wait_send()
        send_2(t).wait_send()
        if t < n_t // 2:
            send_a(t).wait_send()


def grads(lab, coef, z, x, w, vt):
    n_t, n_stage, rows, d = x.shape
    win = w.shape[0]
    n_tail = win - N_TILE * vt
    n = n_stage * rows
    vm = pl.BlockSpec(memory_space=pltpu.VMEM)
    hbm = pl.BlockSpec(memory_space=pl.ANY)
    dma = pltpu.SemaphoreType.DMA
    n_x = n_stage // 2
    tile = jax.ShapeDtypeStruct((vt, d), F32)
    tail = jax.ShapeDtypeStruct((n_tail, d), F32)
    return pl.pallas_call(
        functools.partial(_grads_body, n_stage=n_stage),
        in_specs=[vm, vm, hbm, hbm, hbm],
        out_specs=[hbm] * 8 + [vm],
        out_shape=[tile] * N_TILE + [tail] * 2 + [jax.ShapeDtypeStruct((n_t // 2, rows, d), F32)],
        scratch_shapes=[
            pltpu.VMEM((n_t, n_x, 2, rows, d), F32),
            pltpu.VMEM((2, n_stage, rows, d), BF16),
            pltpu.VMEM((2, n_stage, vt, rows), F32),
            pltpu.VMEM((2, vt, d), BF16),
            pltpu.VMEM((n_stage, n_tail, rows), F32),
            pltpu.VMEM((n_tail, d), BF16),
            pltpu.VMEM((vt, n), BF16),
            pltpu.VMEM((n_tail, n), BF16),
            pltpu.VMEM((N_TILE, vt, d), F32),
            pltpu.VMEM((n_tail, d), F32),
            pltpu.VMEM((2, n_x, rows, d), F32),
            pltpu.VMEM((N_SLOT, 2, rows, d), F32),
            pltpu.VMEM((N_SLOT, rows, d), F32),
            pltpu.VMEM((n_t // 2, rows, d), F32),
            dma((2,)), dma((2,)), dma((2,)), dma, dma, dma((4,)), dma((4,)), dma((4,)),
            dma((n_t,)), dma((n_t,)), dma((n_t, 2)), dma((n_t, 2)), dma((n_t,)), dma((n_t,)), dma((n_t // 2,)), dma((n_t // 2,)),
        ],
        compiler_params=pltpu.CompilerParams(vmem_limit_bytes=67043328, collective_id=1, has_side_effects=True),
        cost_estimate=_cost(4 * n_t * n * d * win, 4 * n_t * n * win, n_t * n * win),
        name="grads",
    )(lab, coef, z, x, w)


def solution(mesh):
    n_data, n_stage = mesh.shape["data"], mesh.shape["stage"]
    tok_spec = P(("pod", "data", "stage"), None)
    rep_spec = P(("pod", "data"))
    vocab_spec = P("stage", None)
    layer_spec = P("stage", None, None)
    swap_a = [(i, i ^ 1) for i in range(n_data)]
    swap_b = [(i, n_data - 1 - i) for i in range(n_data)]

    def local_step(x_rows, w_head, labels, loss_mask, w_embed, tok_ids, act_in, w_up, w_down):
        y, s = lax.axis_index("data"), lax.axis_index("stage")
        shard, d = w_head.shape
        yh = y >> 1
        h = (y ^ yh) & 1
        step_rows = 16 * N_TILE
        win = -(-shard // (2 * step_rows)) * step_rows
        vt = (win // N_TILE - 1) // 16 * 16
        first_row = shard - win
        over = 2 * win - shard

        def over_a(v):
            return lax.ppermute(v, "data", swap_a)

        def over_b(v):
            return lax.ppermute(v, "data", swap_b)

        lab_a = over_a(labels)

        def local(lab):
            lab = lab - (s * shard + h * first_row)
            return jnp.where(lab < win - over * (1 - h), lab, -1)

        n_tok = labels.shape[0]
        lab_two = jnp.stack([local(labels), local(lab_a)])
        z, x_all, w_win, coef = head(x_rows, w_head, lab_two.reshape(2, 1, n_tok), loss_mask.reshape(1, -1), n_stage, win, logits_tile(win))
        n_t, _, rows, _ = x_all.shape
        lab = lab_two[::-1].reshape(2, n_stage, n_t // 2, rows).transpose(0, 2, 1, 3).reshape(n_t, 1, n_stage * rows)
        *parts, tail, tail_far, gx = grads(lab, coef, z, x_all, w_win, vt)
        grad_x = gx.reshape(x_rows.shape)

        loss_t = jnp.sum(coef[:, 3, :], axis=1).reshape(2, n_t // 2).sum(axis=1)
        loss_pair = loss_t[0] + loss_t[1]
        loss_far = over_b(loss_pair.reshape(1, 1))[0, 0]
        mean_loss = (loss_pair + loss_far) / n_data

        offset = s * shard
        local_ids = tok_ids - offset
        in_slice = (local_ids >= 0) & (local_ids < shard)
        rows_emb = jnp.take(w_embed, jnp.clip(local_ids, 0, shard - 1), axis=0)
        emb_part = jnp.where(in_slice[:, None], rows_emb, jnp.zeros_like(rows_emb))
        emb_part, _ = lax.optimization_barrier((emb_part, coef))
        embed_out = lax.psum_scatter(emb_part, "stage", scatter_dimension=0, tiled=True)

        half = N_TILE // 2
        kept, got = parts[:half], parts[half:]
        fins, fas, fbs = [], [], []
        for j in range(half):
            fins.append(lax.optimization_barrier(((kept[j] + got[j]) / n_data).astype(BF16)))
            fbs.append(over_b(fins[j]))
            fas.append(over_a(fins[j]))
        fin_t = lax.optimization_barrier(((tail + tail_far) / n_data).astype(BF16))
        fin_ta = over_a(fin_t)

        mlp_out, done = None, 0
        blocks = n_tok // 512
        for part in MLP_EIGHTHS:
            mlp_out = mlp(act_in, w_up[0], w_down[0], mlp_out, done, blocks * part // 8)
            done += blocks * part // 8

        grad_head = jnp.zeros((shard, d), BF16)
        for j in range(half):
            fin_ab = over_a(fbs[j])
            for v, hh, part in ((fins[j], h, yh), (fas[j], 1 - h, yh), (fbs[j], h, 1 - yh), (fin_ab, 1 - h, 1 - yh)):
                row = hh * first_row + (part * half + j) * vt
                grad_head = lax.dynamic_update_slice(grad_head, v, (row, 0))
        lower = jnp.where(h == 0, fin_t, fin_ta)
        upper = jnp.where(h == 0, fin_ta, fin_t)
        grad_head = lax.dynamic_update_slice(grad_head, lower[: fin_t.shape[0] - over], (N_TILE * vt, 0))
        grad_head = lax.dynamic_update_slice(grad_head, upper, (first_row + N_TILE * vt, 0))

        return mean_loss.reshape(1), grad_x, grad_head, embed_out, mlp_out

    return jax.shard_map(
        local_step,
        mesh=mesh,
        in_specs=(tok_spec, vocab_spec, rep_spec, rep_spec, vocab_spec, rep_spec, tok_spec, layer_spec, layer_spec),
        out_specs=(P("pod"), tok_spec, P(("pod", "stage"), None), tok_spec, tok_spec),
        check_vma=False,
    )
```

```python
import functools

import jax
import jax.numpy as jnp
from jax import lax
from jax.experimental import pallas as pl
from jax.experimental.pallas import tpu as pltpu
from jax.sharding import PartitionSpec as P

MESH = pl.DeviceIdType.MESH
F32 = jnp.float32
BF16 = jnp.bfloat16
N_TILE = 6


def logits_tile(win):
    return next(v for v in range(352, 0, -16) if win % v == 0 and v <= 288)


LOW = -1e30


def _params(mib=60, **kw):
    return pltpu.CompilerParams(vmem_limit_bytes=mib * 2**20, **kw)


def _cost(flops, nbytes, trans=0):
    return pl.CostEstimate(flops=int(flops), bytes_accessed=int(nbytes), transcendentals=int(trans))


def _mlp_body(a_ref, w1_ref, w2_ref, *rest, chunk):
    o_ref, u_ref = rest[-2:]
    ff = w1_ref.shape[1]
    for c in range(ff // chunk):
        cs = slice(c * chunk, (c + 1) * chunk)
        h = jnp.dot(a_ref[...], w1_ref[:, cs], preferred_element_type=F32)
        u_ref[:, cs] = jax.nn.gelu(h).astype(BF16)
    y = jnp.dot(u_ref[...], w2_ref[...], preferred_element_type=F32)
    o_ref[...] = (a_ref[...].astype(F32) + y).astype(BF16)


def mlp(a, w1, w2, out, first, count, tb=512):
    n, d = a.shape
    ff = w1.shape[1]
    extra = [] if out is None else [out]
    return pl.pallas_call(
        functools.partial(_mlp_body, chunk=512),
        grid=(count,),
        in_specs=[
            pl.BlockSpec((tb, d), lambda i: (first + i, 0)),
            pl.BlockSpec((d, ff), lambda i: (0, 0)),
            pl.BlockSpec((ff, d), lambda i: (0, 0)),
        ] + [pl.BlockSpec(memory_space=pl.ANY)] * len(extra),
        out_specs=pl.BlockSpec((tb, d), lambda i: (first + i, 0)),
        out_shape=jax.ShapeDtypeStruct((n, d), BF16),
        scratch_shapes=[pltpu.VMEM((tb, ff), BF16)],
        input_output_aliases={3: 0} if extra else {},
        compiler_params=_params(),
        cost_estimate=_cost(4 * count * tb * d * ff, 4 * count * tb * d + 4 * d * ff, count * tb * ff),
        name="mlp",
    )(a, w1, w2, *extra)


def _logits_block(z_ref, x, w_ref, lab, end, vt):
    tb = x.shape[0]
    lab8 = jnp.broadcast_to(lab, (8, tb))
    sub = lax.broadcasted_iota(jnp.int32, (vt // 8, 8, tb), 0) * 8 + lax.broadcasted_iota(jnp.int32, (vt // 8, 8, tb), 1)
    m8 = s8 = t8 = None
    n_v = w_ref.shape[0] // vt
    for v in range(n_v):
        vs = slice(v * vt, (v + 1) * vt)
        z = lax.dot_general(w_ref[vs, :], x, (((1,), (1,)), ((), ())), preferred_element_type=F32)
        if v == n_v - 1:
            z = jnp.where(lax.broadcasted_iota(jnp.int32, (vt, tb), 0) + v * vt < end, z, LOW)
        z_ref[vs, :] = z
        zr = z_ref[vs, :].reshape(vt // 8, 8, tb)
        tile_max = jnp.max(zr, axis=0)
        m_new = tile_max if v == 0 else jnp.maximum(m8, tile_max)
        e_sum = jnp.sum(jnp.exp(zr - m_new[None]), axis=0)
        hit = jnp.sum(jnp.where(sub + v * vt == lab8[None], zr, 0.0), axis=0)
        s8 = e_sum if v == 0 else s8 * jnp.exp(m8 - m_new) + e_sum
        t8 = hit if v == 0 else t8 + hit
        m8 = m_new
    m = jnp.max(m8, axis=0, keepdims=True)
    s = jnp.sum(s8 * jnp.exp(m8 - m), axis=0, keepdims=True)
    t = jnp.sum(t8, axis=0, keepdims=True)
    return jnp.concatenate([m, s, t, jnp.zeros((5, tb), F32)], axis=0)


def _head_body(
    x_ref, wh_ref, lab_ref, mask_ref, z_ref, xo_ref, wo_ref, coef_out,
    xbuf, wbuf, zbuf, st, got, mine, coef,
    own_sem, w_sem, wo_sem, z_sem, xo_sem, xs_sem, xr_sem, send1, recv1, send2, recv2, *, n_stage, first_row, over, vt,
):
    y, s = lax.axis_index("data"), lax.axis_index("stage")
    h = lax.rem(y + y // 2, 2)
    n_x = n_stage // 2
    x, c = s // 2, lax.rem(s, 2)
    n_q, rows = xbuf.shape[1:3]
    win = wbuf.shape[0]
    n_blk = 2 * n_stage
    y_a = y + 1 - 2 * lax.rem(y, 2)
    sib = s + 1 - 2 * c

    def at(off, flip=0):
        return 2 * lax.rem(x + off, n_x) + lax.rem(c + flip, 2)

    left, right, far = at(n_x - 1), at(1), at(2)
    here = {"data": y, "stage": s}
    to_a = {"data": y_a, "stage": s}
    to_sib = {"data": y, "stage": sib}
    to_left = {"data": y, "stage": left}
    to_right = {"data": y, "stage": right}

    def slot(f, stage):
        return f * n_stage + stage

    sends = [
        (slot(0, s), slot(0, s), to_right, None),
        (slot(0, s), slot(0, s), to_left, None),
        (slot(0, s), slot(1, s), to_a, None),
        (slot(0, s), slot(0, s), to_sib, None),
        (slot(0, left), slot(0, left), to_right, 0),
        (slot(0, right), slot(0, right), to_left, 1),
        (slot(1, s), slot(1, s), to_right, None),
        (slot(1, s), slot(1, s), to_left, None),
        (slot(1, s), slot(1, s), to_sib, None),
        (slot(0, left), slot(0, left), to_sib, None),
        (slot(0, right), slot(0, right), to_sib, None),
        (slot(0, far), slot(1, far), to_a, None),
        (slot(0, far), slot(0, far), to_sib, None),
        (slot(1, left), slot(1, left), to_sib, None),
        (slot(1, right), slot(1, right), to_sib, None),
        (slot(1, far), slot(1, far), to_sib, None),
    ]

    def half(i, part):
        return xbuf.at[i, pl.ds(part * n_q // 2, n_q // 2)]

    def copy(k):
        src, dst, to, part = sends[k]
        return pltpu.make_async_remote_copy(
            src_ref=xbuf.at[src] if part is None else half(src, part),
            dst_ref=xbuf.at[dst] if part is None else half(dst, part),
            send_sem=xs_sem.at[k],
            recv_sem=xr_sem.at[n_blk if part == 1 else dst],
            device_id=to,
            device_id_type=MESH,
        )

    def arrival(ref, sem):
        return pltpu.make_async_remote_copy(
            src_ref=ref, dst_ref=ref, send_sem=xs_sem.at[0], recv_sem=sem, device_id=here, device_id_type=MESH
        )

    def got_block(f, stage):
        arrival(xbuf.at[slot(f, stage)], xr_sem.at[slot(f, stage)]).wait_recv()

    def got_half(part):
        i = slot(0, far)
        arrival(half(i, part), xr_sem.at[n_blk if part == 1 else i]).wait_recv()

    own = pltpu.make_async_copy(x_ref, xbuf.at[slot(0, s)], own_sem)
    own.start()
    w_load = pltpu.make_async_copy(wh_ref.at[pl.ds(pl.multiple_of(h * first_row, 16), win), :], wbuf, w_sem)
    w_load.start()

    peers = [(f, k) for f in range(2) for k in range(n_stage) if (f, k) != (0, 0)]

    def peer(f, k):
        return {"data": y if f == 0 else y_a, "stage": lax.rem(s + k, n_stage)}

    barrier = pltpu.get_barrier_semaphore()
    for f, k in peers:
        pl.semaphore_signal(barrier, inc=1, device_id=peer(f, k), device_id_type=MESH)
    pl.semaphore_wait(barrier, len(peers))

    own.wait()
    for k in range(4):
        copy(k).start()
    w_load.wait()
    w_out = pltpu.make_async_copy(wbuf, wo_ref, wo_sem)
    w_out.start()

    def quarter(stage):
        return pl.ds(pl.multiple_of(stage * rows, rows), rows)

    def z_copy(zs, b, f, stage):
        return pltpu.make_async_copy(
            zbuf.at[zs, :, pl.ds(b * rows, rows)],
            z_ref.at[n_q * (1 - f) + b, stage],
            z_sem.at[zs, b],
        )

    def x_copy(f, stage):
        i = slot(f, stage)
        return pltpu.make_async_copy(xbuf.at[i], xo_ref.at[pl.ds(n_q * (1 - f), n_q), stage], xo_sem.at[i])

    def step(i, carry):
        @pl.when(i == 1)
        def _():
            got_block(0, sib)

        @pl.when(i == 2)
        def _():
            got_block(1, s)
            got_block(0, left)
            got_block(0, right)
            for k in range(4, 11):
                copy(k).start()

        @pl.when(i == 5)
        def _():
            got_half(0)
            got_half(1)
            copy(11).start()
            copy(12).start()
            got_block(1, sib)

        @pl.when(i == 6)
        def _():
            got_block(0, at(n_x - 1, 1))

        @pl.when(i == 7)
        def _():
            got_block(0, at(1, 1))

        @pl.when(i == 9)
        def _():
            got_block(0, at(2, 1))

        @pl.when(i == 10)
        def _():
            got_block(1, left)
            got_block(1, right)
            copy(13).start()
            copy(14).start()

        @pl.when(i == 12)
        def _():
            got_block(1, far)
            copy(15).start()
            got_block(1, at(n_x - 1, 1))

        @pl.when(i == 13)
        def _():
            got_block(1, at(1, 1))

        @pl.when(i == 15)
        def _():
            got_block(1, at(2, 1))

        def among(*ks):
            return functools.reduce(jnp.logical_or, [i == k for k in ks])

        f = jnp.where(jnp.logical_or(among(2, 5), i >= 10), 1, 0)
        flip = jnp.where(among(1, 5, 6, 7, 9, 12, 13, 15), 1, 0)
        off = jnp.where(among(3, 6, 10, 12), n_x - 1, jnp.where(among(4, 7, 11, 13), 1, jnp.where(among(8, 9, 14, 15), 2, 0)))
        stage = at(off, flip)
        blk = slot(f, stage)
        zs = lax.rem(i, 2)

        @pl.when(i >= 2)
        def _():
            for b in range(n_q):
                z_copy(zs, b, f, stage).wait()

        x_copy(f, stage).start()
        lab = lab_ref[f, :, pl.ds(pl.multiple_of(stage * n_q * rows, n_q * rows), n_q * rows)]
        res = _logits_block(zbuf.at[zs], xbuf[blk].reshape(n_q * rows, -1), wbuf, lab, win - over * (1 - h), vt)
        for b in range(n_q):
            st[n_q * (1 - f) + b, :, quarter(stage)] = res[:, b * rows:(b + 1) * rows]
            z_copy(zs, b, f, stage).start()
        return carry

    lax.fori_loop(0, n_blk, step, 0)

    first = []
    for f, k in peers:
        c1 = pltpu.make_async_remote_copy(
            src_ref=st.at[pl.ds(n_q * (1 - f), n_q), :, quarter(lax.rem(s + k, n_stage))],
            dst_ref=got.at[slot(f, k)],
            send_sem=send1.at[slot(f, k)],
            recv_sem=recv1.at[slot(f, k)],
            device_id=peer(f, k),
            device_id_type=MESH,
        )
        c1.start()
        first.append(c1)
    weight = mask_ref[...].astype(F32)
    denom = jnp.maximum(jnp.sum(weight), 1.0)
    mu = jnp.stack([mask_ref[:, pl.ds(pl.multiple_of((n_q * s + b) * rows, rows), rows)].astype(F32) for b in range(n_q)])
    scale = mu / denom
    for c1 in first:
        c1.wait_recv()
    parts = [st[n_q:2 * n_q, :, quarter(s)]] + [got[slot(f, k)] for f, k in peers]
    m = functools.reduce(jnp.maximum, [p[:, 0:1, :] for p in parts])
    z = sum(p[:, 1:2, :] * jnp.exp(p[:, 0:1, :] - m) for p in parts)
    t = sum(p[:, 2:3, :] for p in parts)
    loss = scale * (jnp.log(z) + m - t)
    res = jnp.concatenate([m, scale / z, scale, loss, jnp.zeros((n_q, 4, rows), F32)], axis=1)
    mine[...] = res
    second = []
    for f, k in peers:
        c2 = pltpu.make_async_remote_copy(
            src_ref=mine,
            dst_ref=coef.at[pl.ds(n_q * (1 - f), n_q), :, quarter(s)],
            send_sem=send2.at[slot(f, k)],
            recv_sem=recv2.at[slot(f, k)],
            device_id=peer(f, k),
            device_id_type=MESH,
        )
        c2.start()
        second.append(c2)
    coef[n_q:2 * n_q, :, quarter(s)] = res
    for zs in range(2):
        for b in range(n_q):
            z_copy(zs, b, 0, s).wait()
    for i in range(n_blk):
        x_copy(i // n_stage, i % n_stage).wait()
    w_out.wait()
    for k in range(len(sends)):
        copy(k).wait_send()
    for c1 in first:
        c1.wait_send()
    for c2 in second:
        c2.wait_recv()
    coef_out[...] = coef[...]
    for c2 in second:
        c2.wait_send()


def head(x_rows, w_head, lab, mask, n_stage, win, vt):
    rows, d = x_rows.shape
    n_q = 4
    hr = rows // n_q
    shard = w_head.shape[0]
    n = n_stage * hr
    n_blk = 2 * n_stage
    vm = pl.BlockSpec(memory_space=pltpu.VMEM)
    hbm = pl.BlockSpec(memory_space=pl.ANY)
    dma = pltpu.SemaphoreType.DMA
    x3 = x_rows.reshape(n_q, hr, d)
    total = n_blk * rows
    return pl.pallas_call(
        functools.partial(_head_body, n_stage=n_stage, first_row=shard - win, over=2 * win - shard, vt=vt),
        in_specs=[hbm, hbm, vm, vm],
        out_specs=[hbm, hbm, hbm, vm],
        out_shape=[
            jax.ShapeDtypeStruct((2 * n_q, n_stage, win, hr), F32),
            jax.ShapeDtypeStruct((2 * n_q, n_stage, hr, d), BF16),
            jax.ShapeDtypeStruct((win, d), BF16),
            jax.ShapeDtypeStruct((2 * n_q, 8, n), F32),
        ],
        scratch_shapes=[
            pltpu.VMEM((n_blk, n_q, hr, d), BF16),
            pltpu.VMEM((win, d), BF16),
            pltpu.VMEM((2, win, rows), F32),
            pltpu.VMEM((2 * n_q, 8, n), F32),
            pltpu.VMEM((n_blk, n_q, 8, hr), F32),
            pltpu.VMEM((n_q, 8, hr), F32),
            pltpu.VMEM((2 * n_q, 8, n), F32),
            dma, dma, dma, dma((2, n_q)), dma((n_blk,)), dma((16,)), dma((n_blk + 1,)),
            dma((n_blk,)), dma((n_blk,)), dma((n_blk,)), dma((n_blk,)),
        ],
        compiler_params=_params(56, collective_id=0, has_side_effects=True),
        cost_estimate=_cost(2 * total * d * win, 4 * total * win, total * win),
        name="head",
    )(x3, w_head, lab, mask)


DONE = (12, 17, 27, 31, 35, 41, 44, 47)
SENT = (7, 23, 38)
N_STEP = 48
AFTER_D, AFTER_1, AFTER_2 = 3, 12, 18
SLOTS_1, SLOTS_2 = 6, 4


EVENTS = (
    (48, ("fin", 0)), (49, ("fin", 1)), (51, ("tail", 0)), (54, ("fin", 2)),
    (62, ("pass", 0)), (66, ("pass", 1)), (67, ("pass", 2)),
)
LAST_EVENT = 67


def _step_of(u):
    phases = (
        (0, 1, 0, 0),
        (8, 5, 1, 0),
        (18, 1, 1, 2),
        (24, 4, 2, 2),
        (36, 1, 2, 5),
        (39, 3, 3, 5),
    )
    tile = group = jnp.int32(0)
    for start, n_tile, tile0, group0 in phases:
        k = jnp.maximum(u - start, 0)
        tile = jnp.where(u >= start, tile0 + k % n_tile, tile)
        group = jnp.where(u >= start, group0 + k // n_tile, group)
    return tile, group


def _grads_body(
    lab_ref, coef_ref, z_ref, x_ref, w_ref, gh_ref, rcv0, rcv1, rcv2, gx_ref, loss_ref,
    dxb, dwb, dwt, tr, rd, r1, r2, ra, ls, lr,
    z_sem, x_sem, w_sem, zt_sem, wt_sem, o_sem, sb_sem, rb_sem, sd_sem, rd_sem, s1_sem, r1_sem, s2_sem, r2_sem, sa_sem, ra_sem,
    sf_sem, rf_sem, st_sem, l_sem,
    *, n_stage, first_row, over,
):
    y, s = lax.axis_index("data"), lax.axis_index("stage")
    n_x = n_stage // 2
    x, c = s // 2, lax.rem(s, 2)
    yh = y // 2
    y_a = y + 1 - 2 * lax.rem(y, 2)
    n_data = lax.axis_size("data")
    y_b = n_data - 1 - y
    h = lax.rem(y + yh, 2)
    x_1, x_3 = x + 1 - 2 * lax.rem(x, 2), n_x - 1 - x
    vt = dwb.shape[1]
    n_own = dwb.shape[0] // 2
    n_t, _, _, rows, d = dxb.shape
    n_tail = dwt.shape[0]
    piece = min(rows, vt)
    tail_row = 2 * n_own * vt
    rcv = (rcv0, rcv1, rcv2)
    to_sib = {"data": y, "stage": 2 * x + 1 - c}
    to_a = {"data": y_a, "stage": s}
    to_b = {"data": y_b, "stage": s}

    def stage_at(xx):
        return {"data": y, "stage": 2 * xx + c}

    def remote(src, dst, send, recv, to):
        return pltpu.make_async_remote_copy(
            src_ref=src, dst_ref=dst, send_sem=send, recv_sem=recv, device_id=to, device_id_type=MESH
        )

    def row0(tile):
        half = jnp.where(tile < n_own, 1 - yh, yh)
        return pl.multiple_of((half * n_own + tile % n_own) * vt, vt)

    peers = (to_sib, to_a, to_b, stage_at(x_1), stage_at(x_3))
    barrier = pltpu.get_barrier_semaphore()
    for p in peers:
        pl.semaphore_signal(barrier, inc=1, device_id=p, device_id_type=MESH)
    pl.semaphore_wait(barrier, len(peers))

    loss_part = [jnp.sum(coef_ref[i * n_t // 2:(i + 1) * n_t // 2, 3:4, :]) for i in range(2)]
    loss_pair = loss_part[0] + loss_part[1]
    ls[...] = jnp.full(ls.shape, loss_pair, F32)

    def send_loss():
        return remote(ls, lr, l_sem.at[0], l_sem.at[1], to_b)

    send_loss().start()

    def send_d(t):
        return remote(dxb.at[t, :, 1 - c], rd.at[t % 2], sd_sem.at[t], rd_sem.at[t], to_sib)

    def order(t):
        even = t % 2 == 0
        return jnp.where(even, x_1, x_3), jnp.where(even, x_3, x_1)

    def send_1(t, k):
        p1, _ = order(t)
        mine = p1 if k == 0 else n_x - 1 - x_1
        return remote(dxb.at[t, mine, c], r1.at[t % SLOTS_1, k], s1_sem.at[t, k], r1_sem.at[t, k], stage_at(p1))

    def send_2(t):
        _, p2 = order(t)
        return remote(dxb.at[t, p2, c], r2.at[t % SLOTS_2], s2_sem.at[t], r2_sem.at[t], stage_at(p2))

    def send_a(t):
        return remote(dxb.at[t, x, c], ra.at[t], sa_sem.at[t], ra_sem.at[t], to_a)

    def scheduled(u, after):
        t = sum(jnp.where(u == done + after, i, 0) for i, done in enumerate(DONE))
        return functools.reduce(jnp.logical_or, [u == done + after for done in DONE]), t

    def exchanges(u):
        now2, t2 = scheduled(u, AFTER_2)

        @pl.when(now2)
        def _():
            send_2(t2).wait_recv()
            dxb[t2, x, c] = dxb[t2, x, c] + r2[t2 % SLOTS_2]

            @pl.when(t2 < n_t // 2)
            def _():
                send_a(t2).start()

        now1, t1 = scheduled(u, AFTER_1)

        @pl.when(now1)
        def _():
            _, p2 = order(t1)
            send_1(t1, 0).wait_recv()
            send_1(t1, 1).wait_recv()
            dxb[t1, p2, c] = dxb[t1, p2, c] + r1[t1 % SLOTS_1, 1]
            send_2(t1).start()
            dxb[t1, x, c] = dxb[t1, x, c] + r1[t1 % SLOTS_1, 0]

        now, t = scheduled(u, AFTER_D)

        @pl.when(now)
        def _():
            send_d(t).wait_recv()

            def add(xx, carry):
                dxb[t, xx, c] = dxb[t, xx, c] + rd[t % 2, xx]
                return carry

            lax.fori_loop(0, n_x, add, 0)
            send_1(t, 0).start()
            send_1(t, 1).start()

    def g_tile(z, g_out, t, base):
        n_row = z.shape[1]
        sub = lax.broadcasted_iota(jnp.int32, (n_row // 8, 8, rows), 0) * 8 + lax.broadcasted_iota(jnp.int32, (n_row // 8, 8, rows), 1)
        for i in range(n_stage):
            cs = slice(i * rows, (i + 1) * rows)
            m8 = jnp.broadcast_to(coef_ref[t, 0:1, cs], (8, rows))
            c8 = jnp.broadcast_to(coef_ref[t, 1:2, cs], (8, rows))
            q8 = jnp.broadcast_to(coef_ref[t, 2:3, cs], (8, rows))
            lab8 = jnp.broadcast_to(lab_ref[t, :, cs], (8, rows)) - base
            zr = z[i].reshape(n_row // 8, 8, rows)
            e = jnp.exp(zr - m8[None]) * c8[None]
            gi = jnp.where(sub == lab8[None], e - q8[None], e)
            g_out[:, cs] = gi.reshape(n_row, rows).astype(BF16)

    def send_b(j):
        return remote(dwb.at[j], rcv[j], sb_sem.at[j], rb_sem.at[j], to_b)

    def products(zb, xb, wb, zt, wt, g, gt):
        def loads(u):
            tile, t = _step_of(u)
            k = u % 2
            r = pl.ds(row0(tile), vt)
            return (
                pltpu.make_async_copy(z_ref.at[t, :, r, :], zb.at[k], z_sem.at[k]),
                pltpu.make_async_copy(x_ref.at[t], xb.at[k], x_sem.at[k]),
                pltpu.make_async_copy(w_ref.at[r, :], wb.at[k], w_sem.at[k]),
            )

        def tail_load(t):
            return pltpu.make_async_copy(z_ref.at[t, :, pl.ds(tail_row, n_tail), :], zt, zt_sem)

        for cp in loads(jnp.int32(0)):
            cp.start()
        w_tail = pltpu.make_async_copy(w_ref.at[pl.ds(tail_row, n_tail), :], wt, wt_sem)
        w_tail.start()
        w_tail.wait()

        def step(u, carry):
            tile, t = _step_of(u)
            k = u % 2

            @pl.when(u < N_STEP)
            def _():
                for cp in loads(u):
                    cp.wait()

            @pl.when(u < N_STEP - 1)
            def _():
                for cp in loads(u + 1):
                    cp.start()

            last = jnp.logical_and(tile == 2 * n_own - 1, u < N_STEP)

            @pl.when(last)
            def _():
                tail_load(t).start()

            exchanges(u)

            @pl.when(u < N_STEP)
            def _():
                g_tile(zb.at[k], g, t, row0(tile))
                xk = xb[k].reshape(n_stage * rows, d)
                for xx in range(n_x):
                    gx = g[:, 2 * xx * rows:2 * (xx + 1) * rows]
                    dxp = lax.dot_general(gx, wb[k], (((0,), (0,)), ((), ())), preferred_element_type=F32)
                    dxb[t, xx] = jnp.where(tile == 0, 0.0, dxb[t, xx]) + dxp.reshape(2, rows, d)
                dwb[tile] = jnp.where(t == 0, 0.0, dwb[tile]) + jnp.dot(g[...], xk, preferred_element_type=F32)

            @pl.when(last)
            def _():
                tail_load(t).wait()
                g_tile(zt, gt, t, tail_row)
                xk = xb[k].reshape(n_stage * rows, d)
                dxp = lax.dot_general(gt[...], wt[...], (((0,), (0,)), ((), ())), preferred_element_type=F32)
                dxb[t] = dxb[t] + dxp.reshape(n_x, 2, rows, d)
                dwt[...] = jnp.where(t == 0, 0.0, dwt[...]) + jnp.dot(gt[...], xk, preferred_element_type=F32)
                send_d(t).start()

            for j, end in enumerate(SENT):
                @pl.when(u == end)
                def _(j=j):
                    send_b(j).start()

            return carry

        lax.fori_loop(0, N_STEP, step, 0)

    n_lane = n_stage * rows
    pl.run_scoped(
        products,
        pltpu.VMEM((2, n_stage, vt, rows), F32),
        pltpu.VMEM((2, n_stage, rows, d), BF16),
        pltpu.VMEM((2, vt, d), BF16),
        pltpu.VMEM((n_stage, n_tail, rows), F32),
        pltpu.VMEM((n_tail, d), BF16),
        pltpu.VMEM((vt, n_lane), BF16),
        pltpu.VMEM((n_tail, n_lane), BF16),
    )

    def rows_of(hh, half, j, n=None):
        n = vt if n is None else n
        return gh_ref.at[pl.ds(pl.multiple_of(hh * first_row + (half * n_own + j) * vt, 16), n), :]

    def finish(stage, fin, fint):
        send_tail = remote(dwt, tr, sb_sem.at[n_own], rb_sem.at[n_own], to_b)
        send_tail.start()

        def fin_copy(j, way):
            src, dst = fin.at[j], rows_of(h, yh, j)
            if way == 0:
                return remote(src, dst, sf_sem.at[j, 0], rf_sem.at[j, 0], to_a)
            return remote(src, dst, sf_sem.at[j, 1], rf_sem.at[j, 1], to_b)

        def fin_local(j):
            return pltpu.make_async_copy(fin.at[j], rows_of(h, yh, j), o_sem.at[j])

        def forward(j):
            ref = rows_of(h, 1 - yh, j)
            return remote(ref, ref, sf_sem.at[j, 2], rf_sem.at[j, 2], to_a)

        def arrived(j, way):
            ref = rows_of(1 - h, yh, j) if way == 0 else rows_of(h, 1 - yh, j) if way == 1 else rows_of(1 - h, 1 - yh, j)
            return remote(ref, ref, sf_sem.at[j, way], rf_sem.at[j, way], to_a)

        def finish_tile(j):
            send_b(j).wait_recv()
            cp = pltpu.make_async_copy(rcv[j], stage, st_sem)
            cp.start()
            cp.wait()

            def add(i, carry):
                r = pl.ds(pl.multiple_of(i * piece, piece), piece)
                fin[j, r, :] = ((dwb[n_own + j, r, :] + stage[r, :]) * (1.0 / n_data)).astype(BF16)
                return carry

            lax.fori_loop(0, vt // piece, add, 0)
            fin_copy(j, 0).start()
            fin_copy(j, 1).start()
            fin_local(j).start()

        def tail_copy(hh, remote_copy):
            n = n_tail - over * (1 - hh)
            src, dst = fint.at[pl.ds(0, n), :], gh_ref.at[pl.ds(hh * first_row + tail_row, n), :]
            if remote_copy:
                return remote(src, dst, sf_sem.at[n_own, 0], rf_sem.at[n_own, 0], to_a)
            return pltpu.make_async_copy(src, dst, o_sem.at[n_own])

        def events(u, carry):
            exchanges(u)
            for at, what in EVENTS:
                @pl.when(u == at)
                def _(what=what):
                    kind, j = what
                    if kind == "fin":
                        finish_tile(j)
                    elif kind == "tail":
                        send_tail.wait_recv()
                        fint[...] = ((dwt[...] + tr[...]) * (1.0 / n_data)).astype(BF16)
                        for hh in range(2):
                            @pl.when(h == hh)
                            def _(hh=hh):
                                tail_copy(hh, True).start()
                                tail_copy(hh, False).start()
                    else:
                        arrived(j, 1).wait_recv()
                        forward(j).start()
            return carry

        lax.fori_loop(N_STEP, LAST_EVENT + 1, events, 0)

        for q in range(n_t // 2):
            send_a(q).wait_recv()
            gx_ref[q] = dxb[n_t // 2 + q, x, c] + ra[q]
        send_loss().wait()
        loss_ref[...] = (ls[...] + lr[...]) * (1.0 / n_data)
        for j in range(n_own):
            send_b(j).wait_send()
        send_tail.wait_send()
        for t in range(n_t):
            send_d(t).wait_send()
            send_1(t, 0).wait_send()
            send_1(t, 1).wait_send()
            send_2(t).wait_send()
            if t < n_t // 2:
                send_a(t).wait_send()
        for hh in range(2):
            @pl.when(h == hh)
            def _(hh=hh):
                tail_copy(hh, True).wait_send()
                tail_copy(hh, False).wait()
                tail_copy(1 - hh, True).wait_recv()
        for j in range(n_own):
            fin_local(j).wait()
            fin_copy(j, 0).wait_send()
            fin_copy(j, 1).wait_send()
            forward(j).wait_send()
            arrived(j, 0).wait_recv()
            arrived(j, 2).wait_recv()

    pl.run_scoped(
        finish,
        pltpu.VMEM((vt, d), F32),
        pltpu.VMEM((n_own, vt, d), BF16),
        pltpu.VMEM((n_tail, d), BF16),
    )


def grads(lab, coef, z, x, w, vt, shard):
    n_t, n_stage, rows, d = x.shape
    win = w.shape[0]
    n_tail = win - N_TILE * vt
    n = n_stage * rows
    vm = pl.BlockSpec(memory_space=pltpu.VMEM)
    hbm = pl.BlockSpec(memory_space=pl.ANY)
    dma = pltpu.SemaphoreType.DMA
    n_x = n_stage // 2
    n_own = N_TILE // 2
    return pl.pallas_call(
        functools.partial(_grads_body, n_stage=n_stage, first_row=shard - win, over=2 * win - shard),
        in_specs=[vm, vm, hbm, hbm, hbm],
        out_specs=[hbm] * 4 + [vm] * 2,
        out_shape=[jax.ShapeDtypeStruct((shard, d), BF16)] + [jax.ShapeDtypeStruct((vt, d), F32)] * n_own + [
            jax.ShapeDtypeStruct((n_t // 2, rows, d), F32),
            jax.ShapeDtypeStruct((8, 128), F32),
        ],
        scratch_shapes=[
            pltpu.VMEM((n_t, n_x, 2, rows, d), F32),
            pltpu.VMEM((N_TILE, vt, d), F32),
            pltpu.VMEM((n_tail, d), F32),
            pltpu.VMEM((n_tail, d), F32),
            pltpu.VMEM((2, n_x, rows, d), F32),
            pltpu.VMEM((SLOTS_1, 2, rows, d), F32),
            pltpu.VMEM((SLOTS_2, rows, d), F32),
            pltpu.VMEM((n_t // 2, rows, d), F32),
            pltpu.VMEM((8, 128), F32),
            pltpu.VMEM((8, 128), F32),
            dma((2,)), dma((2,)), dma((2,)), dma, dma, dma((4,)), dma((4,)), dma((4,)),
            dma((n_t,)), dma((n_t,)), dma((n_t, 2)), dma((n_t, 2)), dma((n_t,)), dma((n_t,)), dma((n_t // 2,)), dma((n_t // 2,)),
            dma((4, 3)), dma((4, 3)), dma, dma((2,)),
        ],
        compiler_params=pltpu.CompilerParams(vmem_limit_bytes=67043328, collective_id=1, has_side_effects=True),
        cost_estimate=_cost(4 * n_t * n * d * win, 4 * n_t * n * win, n_t * n * win),
        name="grads",
    )(lab, coef, z, x, w)


def solution(mesh):
    n_data, n_stage = mesh.shape["data"], mesh.shape["stage"]
    tok_spec = P(("pod", "data", "stage"), None)
    rep_spec = P(("pod", "data"))
    vocab_spec = P("stage", None)
    layer_spec = P("stage", None, None)
    swap_a = [(i, i ^ 1) for i in range(n_data)]

    def local_step(x_rows, w_head, labels, loss_mask, w_embed, tok_ids, act_in, w_up, w_down):
        y, s = lax.axis_index("data"), lax.axis_index("stage")
        shard, _ = w_head.shape
        yh = y >> 1
        h = (y ^ yh) & 1
        step_rows = 16 * N_TILE
        win = -(-shard // (2 * step_rows)) * step_rows
        vt = (win // N_TILE - 1) // 16 * 16
        first_row = shard - win
        over = 2 * win - shard

        def over_a(v):
            return lax.ppermute(v, "data", swap_a)

        lab_a = over_a(labels)

        def local(lab):
            lab = lab - (s * shard + h * first_row)
            return jnp.where(lab < win - over * (1 - h), lab, -1)

        n_tok = labels.shape[0]
        lab_two = jnp.stack([local(labels), local(lab_a)])
        z, x_all, w_win, coef = head(x_rows, w_head, lab_two.reshape(2, 1, n_tok), loss_mask.reshape(1, -1), n_stage, win, logits_tile(win))
        n_t, _, rows, _ = x_all.shape
        lab = lab_two[::-1].reshape(2, n_stage, n_t // 2, rows).transpose(0, 2, 1, 3).reshape(n_t, 1, n_stage * rows)
        grad_head, _, _, _, gx, loss = grads(lab, coef, z, x_all, w_win, vt, shard)
        grad_x = gx.reshape(x_rows.shape)
        mean_loss = loss[0, 0]

        offset = s * shard
        local_ids = tok_ids - offset
        in_slice = (local_ids >= 0) & (local_ids < shard)
        rows_emb = jnp.take(w_embed, jnp.clip(local_ids, 0, shard - 1), axis=0)
        emb_part = jnp.where(in_slice[:, None], rows_emb, jnp.zeros_like(rows_emb))
        emb_part, _ = lax.optimization_barrier((emb_part, coef))
        embed_out = lax.psum_scatter(emb_part, "stage", scatter_dimension=0, tiled=True)

        mlp_out = mlp(act_in, w_up[0], w_down[0], None, 0, n_tok // 512)

        return mean_loss.reshape(1), grad_x, grad_head, embed_out, mlp_out

    return jax.shard_map(
        local_step,
        mesh=mesh,
        in_specs=(tok_spec, vocab_spec, rep_spec, rep_spec, vocab_spec, rep_spec, tok_spec, layer_spec, layer_spec),
        out_specs=(P("pod"), tok_spec, P(("pod", "stage"), None), tok_spec, tok_spec),
        check_vma=False,
    )
```

```python
import functools

import jax
import jax.numpy as jnp
from jax import lax
from jax.experimental import pallas as pl
from jax.experimental.pallas import tpu as pltpu
from jax.sharding import PartitionSpec as P

MESH = pl.DeviceIdType.MESH
F32 = jnp.float32
BF16 = jnp.bfloat16
N_TILE = 6


def logits_tile(win):
    return next(v for v in range(352, 0, -16) if win % v == 0 and v <= 288)


LOW = -1e30


def _params(mib=60, **kw):
    return pltpu.CompilerParams(vmem_limit_bytes=mib * 2**20, **kw)


def _cost(flops, nbytes, trans=0):
    return pl.CostEstimate(flops=int(flops), bytes_accessed=int(nbytes), transcendentals=int(trans))


def _logits_block(z_ref, x, w_ref, lab, end, vt):
    tb = x.shape[0]
    lab8 = jnp.broadcast_to(lab, (8, tb))
    sub = lax.broadcasted_iota(jnp.int32, (vt // 8, 8, tb), 0) * 8 + lax.broadcasted_iota(jnp.int32, (vt // 8, 8, tb), 1)
    m8 = s8 = t8 = None
    n_v = w_ref.shape[0] // vt
    for v in range(n_v):
        vs = slice(v * vt, (v + 1) * vt)
        z = lax.dot_general(w_ref[vs, :], x, (((1,), (1,)), ((), ())), preferred_element_type=F32)
        if v == n_v - 1:
            z = jnp.where(lax.broadcasted_iota(jnp.int32, (vt, tb), 0) + v * vt < end, z, LOW)
        z_ref[vs, :] = z
        zr = z_ref[vs, :].reshape(vt // 8, 8, tb)
        tile_max = jnp.max(zr, axis=0)
        m_new = tile_max if v == 0 else jnp.maximum(m8, tile_max)
        e_sum = jnp.sum(jnp.exp(zr - m_new[None]), axis=0)
        hit = jnp.sum(jnp.where(sub + v * vt == lab8[None], zr, 0.0), axis=0)
        s8 = e_sum if v == 0 else s8 * jnp.exp(m8 - m_new) + e_sum
        t8 = hit if v == 0 else t8 + hit
        m8 = m_new
    m = jnp.max(m8, axis=0, keepdims=True)
    s = jnp.sum(s8 * jnp.exp(m8 - m), axis=0, keepdims=True)
    t = jnp.sum(t8, axis=0, keepdims=True)
    return jnp.concatenate([m, s, t, jnp.zeros((5, tb), F32)], axis=0)


def _head_body(
    x_ref, wh_ref, lab_ref, mask_ref, z_ref, xo_ref, wo_ref, coef_out,
    xbuf, wbuf, zbuf, st, got, mine, coef,
    own_sem, w_sem, wo_sem, z_sem, xo_sem, xs_sem, xr_sem, send1, recv1, send2, recv2, *, n_stage, first_row, over, vt,
):
    y, s = lax.axis_index("data"), lax.axis_index("stage")
    h = lax.rem(y + y // 2, 2)
    n_x = n_stage // 2
    x, c = s // 2, lax.rem(s, 2)
    n_q, rows = xbuf.shape[1:3]
    win = wbuf.shape[0]
    n_blk = 2 * n_stage
    y_a = y + 1 - 2 * lax.rem(y, 2)
    sib = s + 1 - 2 * c

    def at(off, flip=0):
        return 2 * lax.rem(x + off, n_x) + lax.rem(c + flip, 2)

    left, right, far = at(n_x - 1), at(1), at(2)
    here = {"data": y, "stage": s}
    to_a = {"data": y_a, "stage": s}
    to_sib = {"data": y, "stage": sib}
    to_left = {"data": y, "stage": left}
    to_right = {"data": y, "stage": right}

    def slot(f, stage):
        return f * n_stage + stage

    sends = [
        (slot(0, s), slot(0, s), to_right, None),
        (slot(0, s), slot(0, s), to_left, None),
        (slot(0, s), slot(1, s), to_a, None),
        (slot(0, s), slot(0, s), to_sib, None),
        (slot(0, left), slot(0, left), to_right, 0),
        (slot(0, right), slot(0, right), to_left, 1),
        (slot(1, s), slot(1, s), to_right, None),
        (slot(1, s), slot(1, s), to_left, None),
        (slot(1, s), slot(1, s), to_sib, None),
        (slot(0, left), slot(0, left), to_sib, None),
        (slot(0, right), slot(0, right), to_sib, None),
        (slot(0, far), slot(1, far), to_a, None),
        (slot(0, far), slot(0, far), to_sib, None),
        (slot(1, left), slot(1, left), to_sib, None),
        (slot(1, right), slot(1, right), to_sib, None),
        (slot(1, far), slot(1, far), to_sib, None),
    ]

    def half(i, part):
        return xbuf.at[i, pl.ds(part * n_q // 2, n_q // 2)]

    def copy(k):
        src, dst, to, part = sends[k]
        return pltpu.make_async_remote_copy(
            src_ref=xbuf.at[src] if part is None else half(src, part),
            dst_ref=xbuf.at[dst] if part is None else half(dst, part),
            send_sem=xs_sem.at[k],
            recv_sem=xr_sem.at[n_blk if part == 1 else dst],
            device_id=to,
            device_id_type=MESH,
        )

    def arrival(ref, sem):
        return pltpu.make_async_remote_copy(
            src_ref=ref, dst_ref=ref, send_sem=xs_sem.at[0], recv_sem=sem, device_id=here, device_id_type=MESH
        )

    def got_block(f, stage):
        arrival(xbuf.at[slot(f, stage)], xr_sem.at[slot(f, stage)]).wait_recv()

    def got_half(part):
        i = slot(0, far)
        arrival(half(i, part), xr_sem.at[n_blk if part == 1 else i]).wait_recv()

    own = pltpu.make_async_copy(x_ref, xbuf.at[slot(0, s)], own_sem)
    own.start()
    w_load = pltpu.make_async_copy(wh_ref.at[pl.ds(pl.multiple_of(h * first_row, 16), win), :], wbuf, w_sem)
    w_load.start()

    peers = [(f, k) for f in range(2) for k in range(n_stage) if (f, k) != (0, 0)]

    def peer(f, k):
        return {"data": y if f == 0 else y_a, "stage": lax.rem(s + k, n_stage)}

    barrier = pltpu.get_barrier_semaphore()
    for f, k in peers:
        pl.semaphore_signal(barrier, inc=1, device_id=peer(f, k), device_id_type=MESH)
    pl.semaphore_wait(barrier, len(peers))

    own.wait()
    for k in range(4):
        copy(k).start()
    w_load.wait()
    w_out = pltpu.make_async_copy(wbuf, wo_ref, wo_sem)
    w_out.start()

    def quarter(stage):
        return pl.ds(pl.multiple_of(stage * rows, rows), rows)

    def z_copy(zs, b, f, stage):
        return pltpu.make_async_copy(
            zbuf.at[zs, :, pl.ds(b * rows, rows)],
            z_ref.at[n_q * (1 - f) + b, stage],
            z_sem.at[zs, b],
        )

    def x_copy(f, stage):
        i = slot(f, stage)
        return pltpu.make_async_copy(xbuf.at[i], xo_ref.at[pl.ds(n_q * (1 - f), n_q), stage], xo_sem.at[i])

    def step(i, carry):
        @pl.when(i == 1)
        def _():
            got_block(0, sib)

        @pl.when(i == 2)
        def _():
            got_block(1, s)
            got_block(0, left)
            got_block(0, right)
            for k in range(4, 11):
                copy(k).start()

        @pl.when(i == 5)
        def _():
            got_half(0)
            got_half(1)
            copy(11).start()
            copy(12).start()
            got_block(1, sib)

        @pl.when(i == 6)
        def _():
            got_block(0, at(n_x - 1, 1))

        @pl.when(i == 7)
        def _():
            got_block(0, at(1, 1))

        @pl.when(i == 9)
        def _():
            got_block(0, at(2, 1))

        @pl.when(i == 10)
        def _():
            got_block(1, left)
            got_block(1, right)
            copy(13).start()
            copy(14).start()

        @pl.when(i == 12)
        def _():
            got_block(1, far)
            copy(15).start()
            got_block(1, at(n_x - 1, 1))

        @pl.when(i == 13)
        def _():
            got_block(1, at(1, 1))

        @pl.when(i == 15)
        def _():
            got_block(1, at(2, 1))

        def among(*ks):
            return functools.reduce(jnp.logical_or, [i == k for k in ks])

        f = jnp.where(jnp.logical_or(among(2, 5), i >= 10), 1, 0)
        flip = jnp.where(among(1, 5, 6, 7, 9, 12, 13, 15), 1, 0)
        off = jnp.where(among(3, 6, 10, 12), n_x - 1, jnp.where(among(4, 7, 11, 13), 1, jnp.where(among(8, 9, 14, 15), 2, 0)))
        stage = at(off, flip)
        blk = slot(f, stage)
        zs = lax.rem(i, 2)

        @pl.when(i >= 2)
        def _():
            for b in range(n_q):
                z_copy(zs, b, f, stage).wait()

        x_copy(f, stage).start()
        lab = lab_ref[f, :, pl.ds(pl.multiple_of(stage * n_q * rows, n_q * rows), n_q * rows)]
        res = _logits_block(zbuf.at[zs], xbuf[blk].reshape(n_q * rows, -1), wbuf, lab, win - over * (1 - h), vt)
        for b in range(n_q):
            st[n_q * (1 - f) + b, :, quarter(stage)] = res[:, b * rows:(b + 1) * rows]
            z_copy(zs, b, f, stage).start()
        return carry

    lax.fori_loop(0, n_blk, step, 0)

    first = []
    for f, k in peers:
        c1 = pltpu.make_async_remote_copy(
            src_ref=st.at[pl.ds(n_q * (1 - f), n_q), :, quarter(lax.rem(s + k, n_stage))],
            dst_ref=got.at[slot(f, k)],
            send_sem=send1.at[slot(f, k)],
            recv_sem=recv1.at[slot(f, k)],
            device_id=peer(f, k),
            device_id_type=MESH,
        )
        c1.start()
        first.append(c1)
    weight = mask_ref[...].astype(F32)
    denom = jnp.maximum(jnp.sum(weight), 1.0)
    mu = jnp.stack([mask_ref[:, pl.ds(pl.multiple_of((n_q * s + b) * rows, rows), rows)].astype(F32) for b in range(n_q)])
    scale = mu / denom
    for c1 in first:
        c1.wait_recv()
    parts = [st[n_q:2 * n_q, :, quarter(s)]] + [got[slot(f, k)] for f, k in peers]
    m = functools.reduce(jnp.maximum, [p[:, 0:1, :] for p in parts])
    z = sum(p[:, 1:2, :] * jnp.exp(p[:, 0:1, :] - m) for p in parts)
    t = sum(p[:, 2:3, :] for p in parts)
    loss = scale * (jnp.log(z) + m - t)
    res = jnp.concatenate([m, scale / z, scale, loss, jnp.zeros((n_q, 4, rows), F32)], axis=1)
    mine[...] = res
    second = []
    for f, k in peers:
        c2 = pltpu.make_async_remote_copy(
            src_ref=mine,
            dst_ref=coef.at[pl.ds(n_q * (1 - f), n_q), :, quarter(s)],
            send_sem=send2.at[slot(f, k)],
            recv_sem=recv2.at[slot(f, k)],
            device_id=peer(f, k),
            device_id_type=MESH,
        )
        c2.start()
        second.append(c2)
    coef[n_q:2 * n_q, :, quarter(s)] = res
    for zs in range(2):
        for b in range(n_q):
            z_copy(zs, b, 0, s).wait()
    for i in range(n_blk):
        x_copy(i // n_stage, i % n_stage).wait()
    w_out.wait()
    for k in range(len(sends)):
        copy(k).wait_send()
    for c1 in first:
        c1.wait_send()
    for c2 in second:
        c2.wait_recv()
    coef_out[...] = coef[...]
    for c2 in second:
        c2.wait_send()


def head(x_rows, w_head, lab, mask, n_stage, win, vt):
    rows, d = x_rows.shape
    n_q = 4
    hr = rows // n_q
    shard = w_head.shape[0]
    n = n_stage * hr
    n_blk = 2 * n_stage
    vm = pl.BlockSpec(memory_space=pltpu.VMEM)
    hbm = pl.BlockSpec(memory_space=pl.ANY)
    dma = pltpu.SemaphoreType.DMA
    x3 = x_rows.reshape(n_q, hr, d)
    total = n_blk * rows
    return pl.pallas_call(
        functools.partial(_head_body, n_stage=n_stage, first_row=shard - win, over=2 * win - shard, vt=vt),
        in_specs=[hbm, hbm, vm, vm],
        out_specs=[hbm, hbm, hbm, vm],
        out_shape=[
            jax.ShapeDtypeStruct((2 * n_q, n_stage, win, hr), F32),
            jax.ShapeDtypeStruct((2 * n_q, n_stage, hr, d), BF16),
            jax.ShapeDtypeStruct((win, d), BF16),
            jax.ShapeDtypeStruct((2 * n_q, 8, n), F32),
        ],
        scratch_shapes=[
            pltpu.VMEM((n_blk, n_q, hr, d), BF16),
            pltpu.VMEM((win, d), BF16),
            pltpu.VMEM((2, win, rows), F32),
            pltpu.VMEM((2 * n_q, 8, n), F32),
            pltpu.VMEM((n_blk, n_q, 8, hr), F32),
            pltpu.VMEM((n_q, 8, hr), F32),
            pltpu.VMEM((2 * n_q, 8, n), F32),
            dma, dma, dma, dma((2, n_q)), dma((n_blk,)), dma((16,)), dma((n_blk + 1,)),
            dma((n_blk,)), dma((n_blk,)), dma((n_blk,)), dma((n_blk,)),
        ],
        compiler_params=_params(56, collective_id=0, has_side_effects=True),
        cost_estimate=_cost(2 * total * d * win, 4 * total * win, total * win),
        name="head",
    )(x3, w_head, lab, mask)


DONE = (12, 17, 27, 31, 35, 41, 44, 47)
SENT = (7, 23, 38)
N_STEP = 48
AFTER_D, AFTER_1, AFTER_2 = 3, 12, 18
SLOTS_1, SLOTS_2 = 6, 4


PHASES = ((0, 1, 0, 0), (8, 5, 1, 0), (18, 1, 1, 2), (24, 4, 2, 2), (36, 1, 2, 5), (39, 3, 3, 5))
EVENTS = (
    (48, "2", 3), (48, "fin", 0), (49, "fin", 1), (53, "d", 7), (54, "tail", 0), (59, "2", 4), (60, "1", 5), (65, "fin", 2), (67, "1", 6), (70, "pass", 0),
    (73, "2", 5), (75, "1", 7), (80, "2", 6), (83, "pass", 1), (87, "2", 7), (98, "pass", 2),
)
MLP_FROM = 50
MLP_CHUNK = 512


def _step_of(u):
    tile = group = xi = wi = jnp.int32(0)
    new_x = new_w = False
    x_base = w_base = 0
    ends = [p[0] for p in PHASES[1:]] + [N_STEP]
    for (start, n_tile, tile0, group0), end in zip(PHASES, ends):
        k = jnp.maximum(u - start, 0)
        on = u >= start
        tile = jnp.where(on, tile0 + k % n_tile, tile)
        group = jnp.where(on, group0 + k // n_tile, group)
        xi = jnp.where(on, x_base + k // n_tile, xi)
        wi = jnp.where(on, w_base + (k if n_tile > 1 else 0), wi)
        new_x = jnp.where(on, k % n_tile == 0, new_x)
        new_w = jnp.where(on, True if n_tile > 1 else k == 0, new_w)
        x_base += (end - start) // n_tile
        w_base += end - start if n_tile > 1 else 1
    return tile, group, xi % 2, wi % 2, new_x, new_w


def _grads_body(
    lab_ref, coef_ref, z_ref, x_ref, w_ref, a_ref, w1_ref, w2_ref, gh_ref, mo_ref, rcv0, rcv1, rcv2, gx_ref, loss_ref,
    dxb, dwb, dwt, tr, rd, r1, r2, ra, ls, lr,
    z_sem, x_sem, w_sem, zt_sem, wt_sem, o_sem, sb_sem, rb_sem, sd_sem, rd_sem, s1_sem, r1_sem, s2_sem, r2_sem, sa_sem, ra_sem,
    sf_sem, rf_sem, st_sem, l_sem, ai_sem, ao_sem, mw_sem,
    *, n_stage, first_row, over,
):
    y, s = lax.axis_index("data"), lax.axis_index("stage")
    n_x = n_stage // 2
    x, c = s // 2, lax.rem(s, 2)
    yh = y // 2
    y_a = y + 1 - 2 * lax.rem(y, 2)
    n_data = lax.axis_size("data")
    y_b = n_data - 1 - y
    h = lax.rem(y + yh, 2)
    x_1, x_3 = x + 1 - 2 * lax.rem(x, 2), n_x - 1 - x
    vt = dwb.shape[1]
    n_own = dwb.shape[0] // 2
    n_t, _, _, rows, d = dxb.shape
    n_tail = dwt.shape[0]
    piece = min(rows, vt)
    tail_row = 2 * n_own * vt
    rcv = (rcv0, rcv1, rcv2)
    to_sib = {"data": y, "stage": 2 * x + 1 - c}
    to_a = {"data": y_a, "stage": s}
    to_b = {"data": y_b, "stage": s}

    def stage_at(xx):
        return {"data": y, "stage": 2 * xx + c}

    def remote(src, dst, send, recv, to):
        return pltpu.make_async_remote_copy(
            src_ref=src, dst_ref=dst, send_sem=send, recv_sem=recv, device_id=to, device_id_type=MESH
        )

    def row0(tile):
        half = jnp.where(tile < n_own, 1 - yh, yh)
        return pl.multiple_of((half * n_own + tile % n_own) * vt, vt)

    peers = (to_sib, to_a, to_b, stage_at(x_1), stage_at(x_3))
    barrier = pltpu.get_barrier_semaphore()
    for p in peers:
        pl.semaphore_signal(barrier, inc=1, device_id=p, device_id_type=MESH)
    pl.semaphore_wait(barrier, len(peers))

    loss_part = [jnp.sum(coef_ref[i * n_t // 2:(i + 1) * n_t // 2, 3:4, :]) for i in range(2)]
    loss_pair = loss_part[0] + loss_part[1]
    ls[...] = jnp.full(ls.shape, loss_pair, F32)

    def send_loss():
        return remote(ls, lr, l_sem.at[0], l_sem.at[1], to_b)

    send_loss().start()

    def send_d(t):
        return remote(dxb.at[t, :, 1 - c], rd.at[t % 2], sd_sem.at[t], rd_sem.at[t], to_sib)

    def order(t):
        even = t % 2 == 0
        return jnp.where(even, x_1, x_3), jnp.where(even, x_3, x_1)

    def send_1(t, k):
        p1, _ = order(t)
        mine = p1 if k == 0 else n_x - 1 - x_1
        return remote(dxb.at[t, mine, c], r1.at[t % SLOTS_1, k], s1_sem.at[t, k], r1_sem.at[t, k], stage_at(p1))

    def send_2(t):
        _, p2 = order(t)
        return remote(dxb.at[t, p2, c], r2.at[t % SLOTS_2], s2_sem.at[t], r2_sem.at[t], stage_at(p2))

    def send_a(t):
        return remote(dxb.at[t, x, c], ra.at[t], sa_sem.at[t], ra_sem.at[t], to_a)

    def exchange_d(t):
        send_d(t).wait_recv()

        def add(xx, carry):
            dxb[t, xx, c] = dxb[t, xx, c] + rd[t % 2, xx]
            return carry

        lax.fori_loop(0, n_x, add, 0)
        send_1(t, 0).start()
        send_1(t, 1).start()

    def exchange_1(t):
        _, p2 = order(t)
        send_1(t, 0).wait_recv()
        send_1(t, 1).wait_recv()
        dxb[t, p2, c] = dxb[t, p2, c] + r1[t % SLOTS_1, 1]
        send_2(t).start()
        dxb[t, x, c] = dxb[t, x, c] + r1[t % SLOTS_1, 0]

    def exchange_2(t):
        send_2(t).wait_recv()
        dxb[t, x, c] = dxb[t, x, c] + r2[t % SLOTS_2]

        @pl.when(t < n_t // 2)
        def _():
            send_a(t).start()

    def exchanges(u):
        for after, run in ((AFTER_2, exchange_2), (AFTER_1, exchange_1), (AFTER_D, exchange_d)):
            done = [d for d in DONE if d + after < N_STEP]
            t = sum(jnp.where(u == d + after, i, 0) for i, d in enumerate(done))

            @pl.when(functools.reduce(jnp.logical_or, [u == d + after for d in done]))
            def _(run=run, t=t):
                run(t)

    def g_tile(z, g_out, t, base):
        n_row = z.shape[1]
        sub = lax.broadcasted_iota(jnp.int32, (n_row // 8, 8, rows), 0) * 8 + lax.broadcasted_iota(jnp.int32, (n_row // 8, 8, rows), 1)
        for i in range(n_stage):
            cs = slice(i * rows, (i + 1) * rows)
            m8 = jnp.broadcast_to(coef_ref[t, 0:1, cs], (8, rows))
            c8 = jnp.broadcast_to(coef_ref[t, 1:2, cs], (8, rows))
            q8 = jnp.broadcast_to(coef_ref[t, 2:3, cs], (8, rows))
            lab8 = jnp.broadcast_to(lab_ref[t, :, cs], (8, rows)) - base
            zr = z[i].reshape(n_row // 8, 8, rows)
            e = jnp.exp(zr - m8[None]) * c8[None]
            gi = jnp.where(sub == lab8[None], e - q8[None], e)
            g_out[:, cs] = gi.reshape(n_row, rows).astype(BF16)

    def send_b(j):
        return remote(dwb.at[j], rcv[j], sb_sem.at[j], rb_sem.at[j], to_b)

    def products(zb, xb, wb, zt, wt, g, gt):
        def whole(u):
            tile, t, xk, wk, new_x, new_w = _step_of(u)
            return (
                pltpu.make_async_copy(z_ref.at[t, :, pl.ds(row0(tile), vt), :], zb.at[u % 2], z_sem.at[u % 2]),
                pltpu.make_async_copy(x_ref.at[t], xb.at[xk], x_sem.at[xk]),
                pltpu.make_async_copy(w_ref.at[pl.ds(row0(tile), vt), :], wb.at[wk], w_sem.at[wk]),
                new_x, new_w,
            )

        def load(u):
            tile, t, xk, wk, new_x, new_w = _step_of(u)
            r0 = row0(tile)
            for i in range(n_stage):
                pltpu.make_async_copy(z_ref.at[t, i, pl.ds(r0, vt), :], zb.at[u % 2, i], z_sem.at[u % 2]).start()

            @pl.when(new_x)
            def _():
                for i in range(0, n_stage, 2):
                    part = pl.ds(i, 2)
                    pltpu.make_async_copy(x_ref.at[t, part], xb.at[xk, part], x_sem.at[xk]).start()

            @pl.when(new_w)
            def _():
                for i in range(2):
                    src, dst = pl.ds(r0 + i * vt // 2, vt // 2), pl.ds(i * vt // 2, vt // 2)
                    pltpu.make_async_copy(w_ref.at[src, :], wb.at[wk, dst, :], w_sem.at[wk]).start()

        def arrive(u):
            z_in, x_in, w_in, new_x, new_w = whole(u)
            z_in.wait()

            @pl.when(new_x)
            def _():
                x_in.wait()

            @pl.when(new_w)
            def _():
                w_in.wait()

        def tail_load(t):
            return pltpu.make_async_copy(z_ref.at[t, :, pl.ds(tail_row, n_tail), :], zt, zt_sem)

        load(jnp.int32(0))
        w_tail = pltpu.make_async_copy(w_ref.at[pl.ds(tail_row, n_tail), :], wt, wt_sem)
        w_tail.start()
        w_tail.wait()

        def step(u, carry):
            tile, t, xk, wk, _, _ = _step_of(u)
            arrive(u)

            @pl.when(u < N_STEP - 1)
            def _():
                load(u + 1)

            last = tile == 2 * n_own - 1

            @pl.when(last)
            def _():
                tail_load(t).start()

            exchanges(u)
            g_tile(zb.at[u % 2], g, t, row0(tile))
            x_t = xb[xk].reshape(n_stage * rows, d)
            for xx in range(n_x):
                gx = g[:, 2 * xx * rows:2 * (xx + 1) * rows]
                dxp = lax.dot_general(gx, wb[wk], (((0,), (0,)), ((), ())), preferred_element_type=F32)
                dxb[t, xx] = jnp.where(tile == 0, 0.0, dxb[t, xx]) + dxp.reshape(2, rows, d)
            dwb[tile] = jnp.where(t == 0, 0.0, dwb[tile]) + jnp.dot(g[...], x_t, preferred_element_type=F32)

            @pl.when(last)
            def _():
                tail_load(t).wait()
                g_tile(zt, gt, t, tail_row)
                x_t = xb[xk].reshape(n_stage * rows, d)
                dxp = lax.dot_general(gt[...], wt[...], (((0,), (0,)), ((), ())), preferred_element_type=F32)
                dxb[t] = dxb[t] + dxp.reshape(n_x, 2, rows, d)
                dwt[...] = jnp.where(t == 0, 0.0, dwt[...]) + jnp.dot(gt[...], x_t, preferred_element_type=F32)
                send_d(t).start()

            for j, end in enumerate(SENT):
                @pl.when(u == end)
                def _(j=j):
                    send_b(j).start()

            return carry

        lax.fori_loop(0, N_STEP, step, 0)

    n_lane = n_stage * rows
    pl.run_scoped(
        products,
        pltpu.VMEM((2, n_stage, vt, rows), F32),
        pltpu.VMEM((2, n_stage, rows, d), BF16),
        pltpu.VMEM((2, vt, d), BF16),
        pltpu.VMEM((n_stage, n_tail, rows), F32),
        pltpu.VMEM((n_tail, d), BF16),
        pltpu.VMEM((vt, n_lane), BF16),
        pltpu.VMEM((n_tail, n_lane), BF16),
    )

    def rows_of(hh, half, j, n=None):
        n = vt if n is None else n
        return gh_ref.at[pl.ds(pl.multiple_of(hh * first_row + (half * n_own + j) * vt, 16), n), :]

    def finish(stage, fin, fint, w1, w2, act, ub):
        send_tail = remote(dwt, tr, sb_sem.at[n_own], rb_sem.at[n_own], to_b)
        send_tail.start()

        def fin_copy(j, way):
            src, dst = fin.at[j], rows_of(h, yh, j)
            if way == 0:
                return remote(src, dst, sf_sem.at[j, 0], rf_sem.at[j, 0], to_a)
            return remote(src, dst, sf_sem.at[j, 1], rf_sem.at[j, 1], to_b)

        def fin_local(j):
            return pltpu.make_async_copy(fin.at[j], rows_of(h, yh, j), o_sem.at[j])

        def forward(j):
            ref = rows_of(1 - h, yh, j) if j == 0 else rows_of(h, 1 - yh, j)
            return remote(ref, ref, sf_sem.at[j, 2], rf_sem.at[j, 2], to_b if j == 0 else to_a)

        def arrived(j, way):
            ref = rows_of(1 - h, yh, j) if way == 0 else rows_of(h, 1 - yh, j) if way == 1 else rows_of(1 - h, 1 - yh, j)
            return remote(ref, ref, sf_sem.at[j, way], rf_sem.at[j, way], to_a)

        n_rows, ff = act.shape[1], w1_ref.shape[1]
        n_block, n_chunk = a_ref.shape[0] // n_rows, ff // MLP_CHUNK
        n_mlp = n_block * n_chunk
        per_group = n_x * 2 * rows // n_rows

        def act_in(m):
            r = pl.ds(pl.multiple_of((m % n_block) * n_rows, n_rows), n_rows)
            return pltpu.make_async_copy(a_ref.at[r, :], act.at[m % 2], ai_sem.at[m % 2])

        def act_out(m):
            r = pl.ds(pl.multiple_of((m % n_block) * n_rows, n_rows), n_rows)
            return pltpu.make_async_copy(act.at[m % 2], mo_ref.at[r, :], ao_sem.at[m % 2])

        def weights(chunk):
            part = pl.ds(pl.multiple_of(chunk * MLP_CHUNK, MLP_CHUNK), MLP_CHUNK)
            k = chunk % 2
            return (
                pltpu.make_async_copy(w1_ref.at[:, part], w1.at[k], mw_sem.at[k, 0]),
                pltpu.make_async_copy(w2_ref.at[part, :], w2.at[k], mw_sem.at[k, 1]),
            )

        def mlp_step(m):
            chunk, block = m // n_block, m % n_block
            k = m % 2

            @pl.when(block == 0)
            def _():
                for cp in weights(chunk):
                    cp.wait()

                @pl.when(chunk + 1 < n_chunk)
                def _():
                    for cp in weights(chunk + 1):
                        cp.start()

            act_in(m).wait()

            @pl.when(m + 1 < n_mlp)
            def _():
                @pl.when(m - 1 >= n_mlp - n_block)
                def _():
                    act_out(m - 1).wait()

                act_in(m + 1).start()

            hid = jnp.dot(act[k], w1[chunk % 2], preferred_element_type=F32)
            ub[...] = jax.nn.gelu(hid).astype(BF16)
            out = jnp.dot(ub[...], w2[chunk % 2], preferred_element_type=F32)
            group, part = block // per_group, block % per_group
            per = n_rows // (2 * rows)
            xs = pl.ds(part * per, per)
            total = jnp.where(chunk == 0, 0.0, dxb[group, xs]) + out.reshape(per, 2, rows, d)

            @pl.when(chunk < n_chunk - 1)
            def _():
                dxb[group, xs] = total

            @pl.when(chunk == n_chunk - 1)
            def _():
                act[k] = (act[k].astype(F32) + total.reshape(n_rows, d)).astype(BF16)
                act_out(m).start()

        for cp in weights(jnp.int32(0)):
            cp.start()
        act_in(jnp.int32(0)).start()

        def finish_tile(j):
            send_b(j).wait_recv()
            cp = pltpu.make_async_copy(rcv[j], stage, st_sem)
            cp.start()
            cp.wait()

            def add(i, carry):
                r = pl.ds(pl.multiple_of(i * piece, piece), piece)
                fin[j, r, :] = ((dwb[n_own + j, r, :] + stage[r, :]) * (1.0 / n_data)).astype(BF16)
                return carry

            lax.fori_loop(0, vt // piece, add, 0)
            fin_copy(j, 0).start()
            fin_copy(j, 1).start()
            fin_local(j).start()

        def tail_copy(hh, remote_copy):
            n = n_tail - over * (1 - hh)
            src, dst = fint.at[pl.ds(0, n), :], gh_ref.at[pl.ds(hh * first_row + tail_row, n), :]
            if remote_copy:
                return remote(src, dst, sf_sem.at[n_own, 0], rf_sem.at[n_own, 0], to_a)
            return pltpu.make_async_copy(src, dst, o_sem.at[n_own])

        def event(what, j):
            if what == "fin":
                finish_tile(j)
            elif what == "d":
                exchange_d(j)
            elif what == "1":
                exchange_1(j)
            elif what == "2":
                exchange_2(j)
            elif what == "tail":
                send_tail.wait_recv()
                fint[...] = ((dwt[...] + tr[...]) * (1.0 / n_data)).astype(BF16)
                for hh in range(2):
                    @pl.when(h == hh)
                    def _(hh=hh):
                        tail_copy(hh, True).start()
                        tail_copy(hh, False).start()
            else:
                arrived(j, 0 if j == 0 else 1).wait_recv()
                forward(j).start()

        def after(u, carry):
            for at, what, j in EVENTS:
                @pl.when(u == at)
                def _(what=what, j=j):
                    event(what, j)

            for t in range(n_t // 2):
                @pl.when(u == MLP_FROM + t * per_group)
                def _(t=t):
                    send_d(t).wait_send()
                    send_1(t, 0).wait_send()
                    send_1(t, 1).wait_send()
                    send_2(t).wait_send()
                    send_a(t).wait_send()

            @pl.when(jnp.logical_and(u >= MLP_FROM, u < MLP_FROM + n_mlp))
            def _():
                mlp_step(u - MLP_FROM)

            return carry

        lax.fori_loop(N_STEP, max(MLP_FROM + n_mlp, EVENTS[-1][0] + 1), after, 0)
        act_out(jnp.int32(n_mlp - 2)).wait()
        act_out(jnp.int32(n_mlp - 1)).wait()

        for q in range(n_t // 2):
            send_a(q).wait_recv()
            gx_ref[q] = dxb[n_t // 2 + q, x, c] + ra[q]
        send_loss().wait()
        loss_ref[...] = (ls[...] + lr[...]) * (1.0 / n_data)
        for j in range(n_own):
            send_b(j).wait_send()
        send_tail.wait_send()
        for t in range(n_t // 2, n_t):
            send_d(t).wait_send()
            send_1(t, 0).wait_send()
            send_1(t, 1).wait_send()
            send_2(t).wait_send()
        for hh in range(2):
            @pl.when(h == hh)
            def _(hh=hh):
                tail_copy(hh, True).wait_send()
                tail_copy(hh, False).wait()
                tail_copy(1 - hh, True).wait_recv()
        for j in range(n_own):
            fin_local(j).wait()
            fin_copy(j, 0).wait_send()
            fin_copy(j, 1).wait_send()
            forward(j).wait_send()
            arrived(j, 1 if j == 0 else 0).wait_recv()
            arrived(j, 2).wait_recv()

    pl.run_scoped(
        finish,
        pltpu.VMEM((vt, d), F32),
        pltpu.VMEM((n_own, vt, d), BF16),
        pltpu.VMEM((n_tail, d), BF16),
        pltpu.VMEM((2, d, MLP_CHUNK), BF16),
        pltpu.VMEM((2, MLP_CHUNK, d), BF16),
        pltpu.VMEM((2, min(512, n_lane), d), BF16),
        pltpu.VMEM((min(512, n_lane), MLP_CHUNK), BF16),
    )


def grads(lab, coef, z, x, w, vt, shard, act, w1, w2):
    n_t, n_stage, rows, d = x.shape
    win = w.shape[0]
    n_tail = win - N_TILE * vt
    n = n_stage * rows
    vm = pl.BlockSpec(memory_space=pltpu.VMEM)
    hbm = pl.BlockSpec(memory_space=pl.ANY)
    dma = pltpu.SemaphoreType.DMA
    n_x = n_stage // 2
    n_own = N_TILE // 2
    return pl.pallas_call(
        functools.partial(_grads_body, n_stage=n_stage, first_row=shard - win, over=2 * win - shard),
        in_specs=[vm, vm] + [hbm] * 6,
        out_specs=[hbm] * 5 + [vm] * 2,
        out_shape=[jax.ShapeDtypeStruct((shard, d), BF16), jax.ShapeDtypeStruct(act.shape, BF16)] + [jax.ShapeDtypeStruct((vt, d), F32)] * n_own + [
            jax.ShapeDtypeStruct((n_t // 2, rows, d), F32),
            jax.ShapeDtypeStruct((8, 128), F32),
        ],
        scratch_shapes=[
            pltpu.VMEM((n_t, n_x, 2, rows, d), F32),
            pltpu.VMEM((N_TILE, vt, d), F32),
            pltpu.VMEM((n_tail, d), F32),
            pltpu.VMEM((n_tail, d), F32),
            pltpu.VMEM((2, n_x, rows, d), F32),
            pltpu.VMEM((SLOTS_1, 2, rows, d), F32),
            pltpu.VMEM((SLOTS_2, rows, d), F32),
            pltpu.VMEM((n_t // 2, rows, d), F32),
            pltpu.VMEM((8, 128), F32),
            pltpu.VMEM((8, 128), F32),
            dma((2,)), dma((2,)), dma((2,)), dma, dma, dma((4,)), dma((4,)), dma((4,)),
            dma((n_t,)), dma((n_t,)), dma((n_t, 2)), dma((n_t, 2)), dma((n_t,)), dma((n_t,)), dma((n_t // 2,)), dma((n_t // 2,)),
            dma((4, 3)), dma((4, 3)), dma, dma((2,)), dma((2,)), dma((2,)), dma((2, 2)),
        ],
        compiler_params=pltpu.CompilerParams(vmem_limit_bytes=67043328, collective_id=1, has_side_effects=True),
        cost_estimate=_cost(4 * n_t * n * d * win, 4 * n_t * n * win, n_t * n * win),
        name="grads",
    )(lab, coef, z, x, w, act, w1, w2)


def solution(mesh):
    n_data, n_stage = mesh.shape["data"], mesh.shape["stage"]
    tok_spec = P(("pod", "data", "stage"), None)
    rep_spec = P(("pod", "data"))
    vocab_spec = P("stage", None)
    layer_spec = P("stage", None, None)
    swap_a = [(i, i ^ 1) for i in range(n_data)]

    def local_step(x_rows, w_head, labels, loss_mask, w_embed, tok_ids, act_in, w_up, w_down):
        y, s = lax.axis_index("data"), lax.axis_index("stage")
        shard, _ = w_head.shape
        yh = y >> 1
        h = (y ^ yh) & 1
        step_rows = 16 * N_TILE
        win = -(-shard // (2 * step_rows)) * step_rows
        vt = (win // N_TILE - 1) // 16 * 16
        first_row = shard - win
        over = 2 * win - shard

        def over_a(v):
            return lax.ppermute(v, "data", swap_a)

        lab_a = over_a(labels)

        def local(lab):
            lab = lab - (s * shard + h * first_row)
            return jnp.where(lab < win - over * (1 - h), lab, -1)

        n_tok = labels.shape[0]
        lab_two = jnp.stack([local(labels), local(lab_a)])
        z, x_all, w_win, coef = head(x_rows, w_head, lab_two.reshape(2, 1, n_tok), loss_mask.reshape(1, -1), n_stage, win, logits_tile(win))
        n_t, _, rows, _ = x_all.shape
        lab = lab_two[::-1].reshape(2, n_stage, n_t // 2, rows).transpose(0, 2, 1, 3).reshape(n_t, 1, n_stage * rows)
        grad_head, mlp_out, _, _, _, gx, loss = grads(lab, coef, z, x_all, w_win, vt, shard, act_in, w_up[0], w_down[0])
        grad_x = gx.reshape(x_rows.shape)
        mean_loss = loss[0, 0]

        offset = s * shard
        local_ids = tok_ids - offset
        in_slice = (local_ids >= 0) & (local_ids < shard)
        rows_emb = jnp.take(w_embed, jnp.clip(local_ids, 0, shard - 1), axis=0)
        emb_part = jnp.where(in_slice[:, None], rows_emb, jnp.zeros_like(rows_emb))
        emb_part, _ = lax.optimization_barrier((emb_part, coef))
        embed_out = lax.psum_scatter(emb_part, "stage", scatter_dimension=0, tiled=True)

        return mean_loss.reshape(1), grad_x, grad_head, embed_out, mlp_out

    return jax.shard_map(
        local_step,
        mesh=mesh,
        in_specs=(tok_spec, vocab_spec, rep_spec, rep_spec, vocab_spec, rep_spec, tok_spec, layer_spec, layer_spec),
        out_specs=(P("pod"), tok_spec, P(("pod", "stage"), None), tok_spec, tok_spec),
        check_vma=False,
    )
```

```python
import functools

import jax
import jax.numpy as jnp
from jax import lax
from jax.experimental import pallas as pl
from jax.experimental.pallas import tpu as pltpu
from jax.sharding import PartitionSpec as P

MESH = pl.DeviceIdType.MESH
F32 = jnp.float32
BF16 = jnp.bfloat16
N_TILE = 6


def logits_tile(win):
    return next(v for v in range(352, 0, -16) if win % v == 0 and v <= 288)


LOW = -1e30


def _params(mib=60, **kw):
    return pltpu.CompilerParams(vmem_limit_bytes=mib * 2**20, **kw)


def _cost(flops, nbytes, trans=0):
    return pl.CostEstimate(flops=int(flops), bytes_accessed=int(nbytes), transcendentals=int(trans))


def _logits_block(z_ref, x, w_ref, lab, end, vt):
    tb = x.shape[0]
    lab8 = jnp.broadcast_to(lab, (8, tb))
    sub = lax.broadcasted_iota(jnp.int32, (vt // 8, 8, tb), 0) * 8 + lax.broadcasted_iota(jnp.int32, (vt // 8, 8, tb), 1)
    m8 = s8 = t8 = None
    n_v = w_ref.shape[0] // vt
    for v in range(n_v):
        vs = slice(v * vt, (v + 1) * vt)
        z = lax.dot_general(w_ref[vs, :], x, (((1,), (1,)), ((), ())), preferred_element_type=F32)
        if v == n_v - 1:
            z = jnp.where(lax.broadcasted_iota(jnp.int32, (vt, tb), 0) + v * vt < end, z, LOW)
        z_ref[vs, :] = z
        zr = z_ref[vs, :].reshape(vt // 8, 8, tb)
        tile_max = jnp.max(zr, axis=0)
        m_new = tile_max if v == 0 else jnp.maximum(m8, tile_max)
        e_sum = jnp.sum(jnp.exp(zr - m_new[None]), axis=0)
        hit = jnp.sum(jnp.where(sub + v * vt == lab8[None], zr, 0.0), axis=0)
        s8 = e_sum if v == 0 else s8 * jnp.exp(m8 - m_new) + e_sum
        t8 = hit if v == 0 else t8 + hit
        m8 = m_new
    m = jnp.max(m8, axis=0, keepdims=True)
    s = jnp.sum(s8 * jnp.exp(m8 - m), axis=0, keepdims=True)
    t = jnp.sum(t8, axis=0, keepdims=True)
    return jnp.concatenate([m, s, t, jnp.zeros((5, tb), F32)], axis=0)


def _head_body(
    x_ref, wh_ref, lab_ref, mask_ref, emb_ref, hit_ref, z_ref, xo_ref, wo_ref, eo_ref, coef_out,
    xbuf, wbuf, zbuf, st, got, mine, coef, ebuf,
    ei_sem, eo_sem, own_sem, w_sem, wo_sem, z_sem, xo_sem, xs_sem, xr_sem, send1, recv1, send2, recv2, *, n_stage, first_row, over, vt,
):
    y, s = lax.axis_index("data"), lax.axis_index("stage")
    h = lax.rem(y + y // 2, 2)
    n_x = n_stage // 2
    x, c = s // 2, lax.rem(s, 2)
    n_q, rows = xbuf.shape[1:3]
    win = wbuf.shape[0]
    n_blk = 2 * n_stage
    y_a = y + 1 - 2 * lax.rem(y, 2)
    sib = s + 1 - 2 * c

    def at(off, flip=0):
        return 2 * lax.rem(x + off, n_x) + lax.rem(c + flip, 2)

    left, right, far = at(n_x - 1), at(1), at(2)
    here = {"data": y, "stage": s}
    to_a = {"data": y_a, "stage": s}
    to_sib = {"data": y, "stage": sib}
    to_left = {"data": y, "stage": left}
    to_right = {"data": y, "stage": right}

    def slot(f, stage):
        return f * n_stage + stage

    sends = [
        (slot(0, s), slot(0, s), to_right, None),
        (slot(0, s), slot(0, s), to_left, None),
        (slot(0, s), slot(1, s), to_a, None),
        (slot(0, s), slot(0, s), to_sib, None),
        (slot(0, left), slot(0, left), to_right, 0),
        (slot(0, right), slot(0, right), to_left, 1),
        (slot(1, s), slot(1, s), to_right, None),
        (slot(1, s), slot(1, s), to_left, None),
        (slot(1, s), slot(1, s), to_sib, None),
        (slot(0, left), slot(0, left), to_sib, None),
        (slot(0, right), slot(0, right), to_sib, None),
        (slot(0, far), slot(1, far), to_a, None),
        (slot(0, far), slot(0, far), to_sib, None),
        (slot(1, left), slot(1, left), to_sib, None),
        (slot(1, right), slot(1, right), to_sib, None),
        (slot(1, far), slot(1, far), to_sib, None),
    ]

    def half(i, part):
        return xbuf.at[i, pl.ds(part * n_q // 2, n_q // 2)]

    def copy(k):
        src, dst, to, part = sends[k]
        return pltpu.make_async_remote_copy(
            src_ref=xbuf.at[src] if part is None else half(src, part),
            dst_ref=xbuf.at[dst] if part is None else half(dst, part),
            send_sem=xs_sem.at[k],
            recv_sem=xr_sem.at[n_blk if part == 1 else dst],
            device_id=to,
            device_id_type=MESH,
        )

    def arrival(ref, sem):
        return pltpu.make_async_remote_copy(
            src_ref=ref, dst_ref=ref, send_sem=xs_sem.at[0], recv_sem=sem, device_id=here, device_id_type=MESH
        )

    def got_block(f, stage):
        arrival(xbuf.at[slot(f, stage)], xr_sem.at[slot(f, stage)]).wait_recv()

    def got_half(part):
        i = slot(0, far)
        arrival(half(i, part), xr_sem.at[n_blk if part == 1 else i]).wait_recv()

    own = pltpu.make_async_copy(x_ref, xbuf.at[slot(0, s)], own_sem)
    own.start()
    w_load = pltpu.make_async_copy(wh_ref.at[pl.ds(pl.multiple_of(h * first_row, 16), win), :], wbuf, w_sem)
    w_load.start()

    def emb_in(e):
        return pltpu.make_async_copy(emb_ref.at[e], ebuf.at[e % 2], ei_sem.at[e % 2])

    def emb_out(e):
        return pltpu.make_async_copy(ebuf.at[e % 2], eo_ref.at[e], eo_sem.at[e % 2])

    def select(e, carry):
        emb_in(e).wait()
        hit = jnp.concatenate([hit_ref[e]] * (ebuf.shape[2] // hit_ref.shape[2]), axis=1)
        v = ebuf[e % 2]
        ebuf[e % 2] = jnp.where(hit != 0, v, jnp.zeros_like(v))
        emb_out(e).start()

        @pl.when(jnp.logical_and(e >= 1, e + 1 < n_stage))
        def _():
            emb_out(e - 1).wait()
            emb_in(e + 1).start()

        return carry

    emb_in(0).start()
    emb_in(1).start()

    peers = [(f, k) for f in range(2) for k in range(n_stage) if (f, k) != (0, 0)]

    def peer(f, k):
        return {"data": y if f == 0 else y_a, "stage": lax.rem(s + k, n_stage)}

    barrier = pltpu.get_barrier_semaphore()
    for f, k in peers:
        pl.semaphore_signal(barrier, inc=1, device_id=peer(f, k), device_id_type=MESH)
    pl.semaphore_wait(barrier, len(peers))

    own.wait()
    for k in range(4):
        copy(k).start()
    w_load.wait()
    w_out = pltpu.make_async_copy(wbuf, wo_ref, wo_sem)
    w_out.start()

    def quarter(stage):
        return pl.ds(pl.multiple_of(stage * rows, rows), rows)

    def z_copy(zs, b, f, stage):
        return pltpu.make_async_copy(
            zbuf.at[zs, :, pl.ds(b * rows, rows)],
            z_ref.at[n_q * (1 - f) + b, stage],
            z_sem.at[zs, b],
        )

    def x_copy(f, stage):
        i = slot(f, stage)
        return pltpu.make_async_copy(xbuf.at[i], xo_ref.at[pl.ds(n_q * (1 - f), n_q), stage], xo_sem.at[i])

    def step(i, carry):
        @pl.when(i == 1)
        def _():
            got_block(0, sib)

        @pl.when(i == 2)
        def _():
            lax.fori_loop(0, n_stage, select, 0)
            got_block(1, s)
            got_block(0, left)
            got_block(0, right)
            for k in range(4, 11):
                copy(k).start()

        @pl.when(i == 5)
        def _():
            got_half(0)
            got_half(1)
            copy(11).start()
            copy(12).start()
            got_block(1, sib)

        @pl.when(i == 6)
        def _():
            got_block(0, at(n_x - 1, 1))

        @pl.when(i == 7)
        def _():
            got_block(0, at(1, 1))

        @pl.when(i == 9)
        def _():
            got_block(0, at(2, 1))

        @pl.when(i == 10)
        def _():
            got_block(1, left)
            got_block(1, right)
            copy(13).start()
            copy(14).start()

        @pl.when(i == 12)
        def _():
            got_block(1, far)
            copy(15).start()
            got_block(1, at(n_x - 1, 1))

        @pl.when(i == 13)
        def _():
            got_block(1, at(1, 1))

        @pl.when(i == 15)
        def _():
            got_block(1, at(2, 1))

        def among(*ks):
            return functools.reduce(jnp.logical_or, [i == k for k in ks])

        f = jnp.where(jnp.logical_or(among(2, 5), i >= 10), 1, 0)
        flip = jnp.where(among(1, 5, 6, 7, 9, 12, 13, 15), 1, 0)
        off = jnp.where(among(3, 6, 10, 12), n_x - 1, jnp.where(among(4, 7, 11, 13), 1, jnp.where(among(8, 9, 14, 15), 2, 0)))
        stage = at(off, flip)
        blk = slot(f, stage)
        zs = lax.rem(i, 2)

        @pl.when(i >= 2)
        def _():
            for b in range(n_q):
                z_copy(zs, b, f, stage).wait()

        x_copy(f, stage).start()
        lab = lab_ref[f, :, pl.ds(pl.multiple_of(stage * n_q * rows, n_q * rows), n_q * rows)]
        res = _logits_block(zbuf.at[zs], xbuf[blk].reshape(n_q * rows, -1), wbuf, lab, win - over * (1 - h), vt)
        for b in range(n_q):
            st[n_q * (1 - f) + b, :, quarter(stage)] = res[:, b * rows:(b + 1) * rows]
            z_copy(zs, b, f, stage).start()
        return carry

    lax.fori_loop(0, n_blk, step, 0)

    first = []
    for f, k in peers:
        c1 = pltpu.make_async_remote_copy(
            src_ref=st.at[pl.ds(n_q * (1 - f), n_q), :, quarter(lax.rem(s + k, n_stage))],
            dst_ref=got.at[slot(f, k)],
            send_sem=send1.at[slot(f, k)],
            recv_sem=recv1.at[slot(f, k)],
            device_id=peer(f, k),
            device_id_type=MESH,
        )
        c1.start()
        first.append(c1)
    weight = mask_ref[...].astype(F32)
    denom = jnp.maximum(jnp.sum(weight), 1.0)
    mu = jnp.stack([mask_ref[:, pl.ds(pl.multiple_of((n_q * s + b) * rows, rows), rows)].astype(F32) for b in range(n_q)])
    scale = mu / denom
    for c1 in first:
        c1.wait_recv()
    parts = [st[n_q:2 * n_q, :, quarter(s)]] + [got[slot(f, k)] for f, k in peers]
    m = functools.reduce(jnp.maximum, [p[:, 0:1, :] for p in parts])
    z = sum(p[:, 1:2, :] * jnp.exp(p[:, 0:1, :] - m) for p in parts)
    t = sum(p[:, 2:3, :] for p in parts)
    loss = scale * (jnp.log(z) + m - t)
    res = jnp.concatenate([m, scale / z, scale, loss, jnp.zeros((n_q, 4, rows), F32)], axis=1)
    mine[...] = res
    second = []
    for f, k in peers:
        c2 = pltpu.make_async_remote_copy(
            src_ref=mine,
            dst_ref=coef.at[pl.ds(n_q * (1 - f), n_q), :, quarter(s)],
            send_sem=send2.at[slot(f, k)],
            recv_sem=recv2.at[slot(f, k)],
            device_id=peer(f, k),
            device_id_type=MESH,
        )
        c2.start()
        second.append(c2)
    coef[n_q:2 * n_q, :, quarter(s)] = res
    for zs in range(2):
        for b in range(n_q):
            z_copy(zs, b, 0, s).wait()
    for i in range(n_blk):
        x_copy(i // n_stage, i % n_stage).wait()
    w_out.wait()
    emb_out(n_stage - 2).wait()
    emb_out(n_stage - 1).wait()
    for k in range(len(sends)):
        copy(k).wait_send()
    for c1 in first:
        c1.wait_send()
    for c2 in second:
        c2.wait_recv()
    coef_out[...] = coef[...]
    for c2 in second:
        c2.wait_send()


def head(x_rows, w_head, lab, mask, emb, hit, n_stage, win, vt):
    rows, d = x_rows.shape
    n_q = 4
    hr = rows // n_q
    shard = w_head.shape[0]
    n = n_stage * hr
    n_blk = 2 * n_stage
    vm = pl.BlockSpec(memory_space=pltpu.VMEM)
    hbm = pl.BlockSpec(memory_space=pl.ANY)
    dma = pltpu.SemaphoreType.DMA
    x3 = x_rows.reshape(n_q, hr, d)
    total = n_blk * rows
    return pl.pallas_call(
        functools.partial(_head_body, n_stage=n_stage, first_row=shard - win, over=2 * win - shard, vt=vt),
        in_specs=[hbm, hbm, vm, vm, hbm, vm],
        out_specs=[hbm, hbm, hbm, hbm, vm],
        out_shape=[
            jax.ShapeDtypeStruct((2 * n_q, n_stage, win, hr), F32),
            jax.ShapeDtypeStruct((2 * n_q, n_stage, hr, d), BF16),
            jax.ShapeDtypeStruct((win, d), BF16),
            jax.ShapeDtypeStruct(emb.shape, BF16),
            jax.ShapeDtypeStruct((2 * n_q, 8, n), F32),
        ],
        scratch_shapes=[
            pltpu.VMEM((n_blk, n_q, hr, d), BF16),
            pltpu.VMEM((win, d), BF16),
            pltpu.VMEM((2, win, rows), F32),
            pltpu.VMEM((2 * n_q, 8, n), F32),
            pltpu.VMEM((n_blk, n_q, 8, hr), F32),
            pltpu.VMEM((n_q, 8, hr), F32),
            pltpu.VMEM((2 * n_q, 8, n), F32),
            pltpu.VMEM((2, *emb.shape[1:]), BF16),
            dma((2,)), dma((2,)), dma, dma, dma, dma((2, n_q)), dma((n_blk,)), dma((16,)), dma((n_blk + 1,)),
            dma((n_blk,)), dma((n_blk,)), dma((n_blk,)), dma((n_blk,)),
        ],
        compiler_params=_params(56, collective_id=0, has_side_effects=True),
        cost_estimate=_cost(2 * total * d * win, 4 * total * win, total * win),
        name="head",
    )(x3, w_head, lab, mask, emb, hit)


DONE = (12, 17, 27, 31, 35, 41, 44, 47)
SENT = (7, 23, 38)
N_STEP = 48
AFTER_D, AFTER_1, AFTER_2 = 3, 12, 18
SLOTS_1, SLOTS_2 = 6, 4


PHASES = ((0, 1, 0, 0), (8, 5, 1, 0), (18, 1, 1, 2), (24, 4, 2, 2), (36, 1, 2, 5), (39, 3, 3, 5))
EVENTS = (
    (48, "2", 3), (48, "fin", 0), (49, "d", 7), (49, "fin", 1), (53, "1", 5), (53, "fin", 2), (53, "fb", 0), (54, "2", 4), (56, "tail", 0),
    (60, "1", 6), (61, "2", 5), (62, "pass", 0), (65, "1", 7), (68, "2", 6), (70, "pass", 1), (72, "2", 7), (83, "pass", 2),
)
MLP_FROM = 50
MLP_CHUNK = 512


def _step_of(u):
    tile = group = xi = wi = jnp.int32(0)
    new_x = new_w = False
    x_base = w_base = 0
    ends = [p[0] for p in PHASES[1:]] + [N_STEP]
    for (start, n_tile, tile0, group0), end in zip(PHASES, ends):
        k = u - start
        on = u >= start
        turn = k if n_tile == 1 else sum(jnp.where(k >= i, 1, 0) for i in range(n_tile, end - start, n_tile))
        place = k - n_tile * turn
        tile = jnp.where(on, tile0 + place, tile)
        group = jnp.where(on, group0 + turn, group)
        xi = jnp.where(on, x_base + turn, xi)
        wi = jnp.where(on, w_base + (k if n_tile > 1 else 0), wi)
        new_x = jnp.where(on, place == 0, new_x)
        new_w = jnp.where(on, True if n_tile > 1 else k == 0, new_w)
        x_base += (end - start) // n_tile
        w_base += end - start if n_tile > 1 else 1
    return tile, group, xi % 2, wi % 2, new_x, new_w


def _grads_body(
    lab_ref, coef_ref, z_ref, x_ref, w_ref, a_ref, w1_ref, w2_ref, gh_ref, mo_ref, rcv0, rcv1, rcv2, gx_ref, loss_ref,
    dxb, dwb, dwt, tr, rd, r1, r2, ra, ls, lr,
    z_sem, x_sem, w_sem, zt_sem, wt_sem, o_sem, sb_sem, rb_sem, sd_sem, rd_sem, s1_sem, r1_sem, s2_sem, r2_sem, sa_sem, ra_sem,
    sf_sem, rf_sem, st_sem, l_sem, ai_sem, ao_sem, mw_sem,
    *, n_stage, first_row, over,
):
    y, s = lax.axis_index("data"), lax.axis_index("stage")
    n_x = n_stage // 2
    x, c = s // 2, lax.rem(s, 2)
    yh = y // 2
    y_a = y + 1 - 2 * lax.rem(y, 2)
    n_data = lax.axis_size("data")
    y_b = n_data - 1 - y
    h = lax.rem(y + yh, 2)
    x_1, x_3 = x + 1 - 2 * lax.rem(x, 2), n_x - 1 - x
    vt = dwb.shape[1]
    n_own = dwb.shape[0] // 2
    n_t, _, _, rows, d = dxb.shape
    n_tail = dwt.shape[0]
    piece = min(rows, vt)
    tail_row = 2 * n_own * vt
    rcv = (rcv0, rcv1, rcv2)
    to_sib = {"data": y, "stage": 2 * x + 1 - c}
    to_a = {"data": y_a, "stage": s}
    to_b = {"data": y_b, "stage": s}

    def stage_at(xx):
        return {"data": y, "stage": 2 * xx + c}

    def remote(src, dst, send, recv, to):
        return pltpu.make_async_remote_copy(
            src_ref=src, dst_ref=dst, send_sem=send, recv_sem=recv, device_id=to, device_id_type=MESH
        )

    def row0(tile):
        far = tile < n_own
        half = jnp.where(far, 1 - yh, yh)
        return pl.multiple_of((half * n_own + tile - jnp.where(far, 0, n_own)) * vt, vt)

    peers = (to_sib, to_a, to_b, stage_at(x_1), stage_at(x_3))
    barrier = pltpu.get_barrier_semaphore()
    for p in peers:
        pl.semaphore_signal(barrier, inc=1, device_id=p, device_id_type=MESH)
    pl.semaphore_wait(barrier, len(peers))

    loss_part = [jnp.sum(coef_ref[i * n_t // 2:(i + 1) * n_t // 2, 3:4, :]) for i in range(2)]
    loss_pair = loss_part[0] + loss_part[1]
    ls[...] = jnp.full(ls.shape, loss_pair, F32)

    def send_loss():
        return remote(ls, lr, l_sem.at[0], l_sem.at[1], to_b)

    send_loss().start()

    def send_d(t):
        return remote(dxb.at[t, :, 1 - c], rd.at[t % 2], sd_sem.at[t], rd_sem.at[t], to_sib)

    def order(t):
        even = t % 2 == 0
        return jnp.where(even, x_1, x_3), jnp.where(even, x_3, x_1)

    def send_1(t, k):
        p1, _ = order(t)
        mine = p1 if k == 0 else n_x - 1 - x_1
        return remote(dxb.at[t, mine, c], r1.at[t % SLOTS_1, k], s1_sem.at[t, k], r1_sem.at[t, k], stage_at(p1))

    def send_2(t):
        _, p2 = order(t)
        return remote(dxb.at[t, p2, c], r2.at[t % SLOTS_2], s2_sem.at[t], r2_sem.at[t], stage_at(p2))

    def send_a(t):
        return remote(dxb.at[t, x, c], ra.at[t], sa_sem.at[t], ra_sem.at[t], to_a)

    def exchange_d(t):
        send_d(t).wait_recv()

        def add(xx, carry):
            dxb[t, xx, c] = dxb[t, xx, c] + rd[t % 2, xx]
            return carry

        lax.fori_loop(0, n_x, add, 0)
        send_1(t, 0).start()
        send_1(t, 1).start()

    def exchange_1(t):
        _, p2 = order(t)
        send_1(t, 0).wait_recv()
        send_1(t, 1).wait_recv()
        dxb[t, p2, c] = dxb[t, p2, c] + r1[t % SLOTS_1, 1]
        send_2(t).start()
        dxb[t, x, c] = dxb[t, x, c] + r1[t % SLOTS_1, 0]

    def exchange_2(t):
        send_2(t).wait_recv()
        dxb[t, x, c] = dxb[t, x, c] + r2[t % SLOTS_2]

        @pl.when(t < n_t // 2)
        def _():
            send_a(t).start()

    def exchanges(u):
        for after, run in ((AFTER_2, exchange_2), (AFTER_1, exchange_1), (AFTER_D, exchange_d)):
            done = [d for d in DONE if d + after < N_STEP]
            t = sum(jnp.where(u == d + after, i, 0) for i, d in enumerate(done))

            @pl.when(functools.reduce(jnp.logical_or, [u == d + after for d in done]))
            def _(run=run, t=t):
                run(t)

    def g_tile(z, g_out, t, base):
        n_row = z.shape[1]
        sub = lax.broadcasted_iota(jnp.int32, (n_row // 8, 8, rows), 0) * 8 + lax.broadcasted_iota(jnp.int32, (n_row // 8, 8, rows), 1)
        for i in range(n_stage):
            cs = slice(i * rows, (i + 1) * rows)
            m8 = jnp.broadcast_to(coef_ref[t, 0:1, cs], (8, rows))
            c8 = jnp.broadcast_to(coef_ref[t, 1:2, cs], (8, rows))
            q8 = jnp.broadcast_to(coef_ref[t, 2:3, cs], (8, rows))
            lab8 = jnp.broadcast_to(lab_ref[t, :, cs], (8, rows)) - base
            zr = z[i].reshape(n_row // 8, 8, rows)
            e = jnp.exp(zr - m8[None]) * c8[None]
            gi = jnp.where(sub == lab8[None], e - q8[None], e)
            g_out[:, cs] = gi.reshape(n_row, rows).astype(BF16)

    def send_b(j):
        return remote(dwb.at[j], rcv[j], sb_sem.at[j], rb_sem.at[j], to_b)

    def products(zb, xb, wb, zt, wt, g, gt):
        def whole(u):
            tile, t, xk, wk, new_x, new_w = _step_of(u)
            return (
                pltpu.make_async_copy(z_ref.at[t, :, pl.ds(row0(tile), vt), :], zb.at[u % 2], z_sem.at[u % 2]),
                pltpu.make_async_copy(x_ref.at[t], xb.at[xk], x_sem.at[xk]),
                pltpu.make_async_copy(w_ref.at[pl.ds(row0(tile), vt), :], wb.at[wk], w_sem.at[wk]),
                new_x, new_w,
            )

        def load(u):
            tile, t, xk, wk, new_x, new_w = _step_of(u)
            r0 = row0(tile)
            for i in range(n_stage):
                pltpu.make_async_copy(z_ref.at[t, i, pl.ds(r0, vt), :], zb.at[u % 2, i], z_sem.at[u % 2]).start()

            @pl.when(new_x)
            def _():
                for i in range(0, n_stage, 2):
                    part = pl.ds(i, 2)
                    pltpu.make_async_copy(x_ref.at[t, part], xb.at[xk, part], x_sem.at[xk]).start()

            @pl.when(new_w)
            def _():
                for i in range(2):
                    src, dst = pl.ds(r0 + i * vt // 2, vt // 2), pl.ds(i * vt // 2, vt // 2)
                    pltpu.make_async_copy(w_ref.at[src, :], wb.at[wk, dst, :], w_sem.at[wk]).start()

        def arrive(u):
            z_in, x_in, w_in, new_x, new_w = whole(u)
            z_in.wait()

            @pl.when(new_x)
            def _():
                x_in.wait()

            @pl.when(new_w)
            def _():
                w_in.wait()

        def tail_load(t):
            return pltpu.make_async_copy(z_ref.at[t, :, pl.ds(tail_row, n_tail), :], zt, zt_sem)

        load(jnp.int32(0))
        w_tail = pltpu.make_async_copy(w_ref.at[pl.ds(tail_row, n_tail), :], wt, wt_sem)
        w_tail.start()
        w_tail.wait()

        def step(u, carry):
            tile, t, xk, wk, _, _ = _step_of(u)
            arrive(u)

            @pl.when(u < N_STEP - 1)
            def _():
                load(u + 1)

            last = tile == 2 * n_own - 1

            @pl.when(last)
            def _():
                tail_load(t).start()

            exchanges(u)
            g_tile(zb.at[u % 2], g, t, row0(tile))
            x_t = xb[xk].reshape(n_stage * rows, d)
            for xx in range(n_x):
                gx = g[:, 2 * xx * rows:2 * (xx + 1) * rows]
                dxp = lax.dot_general(gx, wb[wk], (((0,), (0,)), ((), ())), preferred_element_type=F32)
                dxb[t, xx] = jnp.where(tile == 0, 0.0, dxb[t, xx]) + dxp.reshape(2, rows, d)
            dwb[tile] = jnp.where(t == 0, 0.0, dwb[tile]) + jnp.dot(g[...], x_t, preferred_element_type=F32)

            @pl.when(last)
            def _():
                tail_load(t).wait()
                g_tile(zt, gt, t, tail_row)
                x_t = xb[xk].reshape(n_stage * rows, d)
                dxp = lax.dot_general(gt[...], wt[...], (((0,), (0,)), ((), ())), preferred_element_type=F32)
                dxb[t] = dxb[t] + dxp.reshape(n_x, 2, rows, d)
                dwt[...] = jnp.where(t == 0, 0.0, dwt[...]) + jnp.dot(gt[...], x_t, preferred_element_type=F32)
                send_d(t).start()

            for j, end in enumerate(SENT):
                @pl.when(u == end)
                def _(j=j):
                    send_b(j).start()

            return carry

        lax.fori_loop(0, N_STEP, step, 0)

    n_lane = n_stage * rows
    pl.run_scoped(
        products,
        pltpu.VMEM((2, n_stage, vt, rows), F32),
        pltpu.VMEM((2, n_stage, rows, d), BF16),
        pltpu.VMEM((2, vt, d), BF16),
        pltpu.VMEM((n_stage, n_tail, rows), F32),
        pltpu.VMEM((n_tail, d), BF16),
        pltpu.VMEM((vt, n_lane), BF16),
        pltpu.VMEM((n_tail, n_lane), BF16),
    )

    def rows_of(hh, half, j, n=None):
        n = vt if n is None else n
        return gh_ref.at[pl.ds(pl.multiple_of(hh * first_row + (half * n_own + j) * vt, 16), n), :]

    def finish(stage, fin, fint, w1, w2, act, ub):
        send_tail = remote(dwt, tr, sb_sem.at[n_own], rb_sem.at[n_own], to_b)
        send_tail.start()

        def fin_copy(j, way):
            src, dst = fin.at[j], rows_of(h, yh, j)
            if way == 0:
                return remote(src, dst, sf_sem.at[j, 0], rf_sem.at[j, 0], to_a)
            return remote(src, dst, sf_sem.at[j, 1], rf_sem.at[j, 1], to_b)

        def fin_local(j):
            return pltpu.make_async_copy(fin.at[j], rows_of(h, yh, j), o_sem.at[j])

        def forward(j):
            ref = rows_of(1 - h, yh, j) if j == 0 else rows_of(h, 1 - yh, j)
            return remote(ref, ref, sf_sem.at[j, 2], rf_sem.at[j, 2], to_b if j == 0 else to_a)

        def arrived(j, way):
            ref = rows_of(1 - h, yh, j) if way == 0 else rows_of(h, 1 - yh, j) if way == 1 else rows_of(1 - h, 1 - yh, j)
            return remote(ref, ref, sf_sem.at[j, way], rf_sem.at[j, way], to_a)

        n_rows, ff = act.shape[1], w1_ref.shape[1]
        n_block, n_chunk = a_ref.shape[0] // n_rows, ff // MLP_CHUNK
        n_mlp = n_block * n_chunk
        per_group = n_x * 2 * rows // n_rows

        def act_in(m):
            r = pl.ds(pl.multiple_of((m % n_block) * n_rows, n_rows), n_rows)
            return pltpu.make_async_copy(a_ref.at[r, :], act.at[m % 2], ai_sem.at[m % 2])

        def act_out(m):
            r = pl.ds(pl.multiple_of((m % n_block) * n_rows, n_rows), n_rows)
            return pltpu.make_async_copy(act.at[m % 2], mo_ref.at[r, :], ao_sem.at[m % 2])

        def weights(chunk):
            part = pl.ds(pl.multiple_of(chunk * MLP_CHUNK, MLP_CHUNK), MLP_CHUNK)
            k = chunk % 2
            return (
                pltpu.make_async_copy(w1_ref.at[:, part], w1.at[k], mw_sem.at[k, 0]),
                pltpu.make_async_copy(w2_ref.at[part, :], w2.at[k], mw_sem.at[k, 1]),
            )

        def mlp_step(m):
            chunk, block = m // n_block, m % n_block
            k = m % 2

            @pl.when(block == 0)
            def _():
                for cp in weights(chunk):
                    cp.wait()

                @pl.when(chunk + 1 < n_chunk)
                def _():
                    for cp in weights(chunk + 1):
                        cp.start()

            act_in(m).wait()

            @pl.when(m + 1 < n_mlp)
            def _():
                @pl.when(m - 1 >= n_mlp - n_block)
                def _():
                    act_out(m - 1).wait()

                act_in(m + 1).start()

            hid = jnp.dot(act[k], w1[chunk % 2], preferred_element_type=F32)
            ub[...] = jax.nn.gelu(hid).astype(BF16)
            out = jnp.dot(ub[...], w2[chunk % 2], preferred_element_type=F32)
            group, part = block // per_group, block % per_group
            per = n_rows // (2 * rows)
            xs = pl.ds(part * per, per)
            total = jnp.where(chunk == 0, 0.0, dxb[group, xs]) + out.reshape(per, 2, rows, d)

            @pl.when(chunk < n_chunk - 1)
            def _():
                dxb[group, xs] = total

            @pl.when(chunk == n_chunk - 1)
            def _():
                act[k] = (act[k].astype(F32) + total.reshape(n_rows, d)).astype(BF16)
                act_out(m).start()

        for cp in weights(jnp.int32(0)):
            cp.start()
        act_in(jnp.int32(0)).start()

        def finish_tile(j):
            send_b(j).wait_recv()
            cp = pltpu.make_async_copy(rcv[j], stage, st_sem)
            cp.start()
            cp.wait()

            def add(i, carry):
                r = pl.ds(pl.multiple_of(i * piece, piece), piece)
                fin[j, r, :] = ((dwb[n_own + j, r, :] + stage[r, :]) * (1.0 / n_data)).astype(BF16)
                return carry

            lax.fori_loop(0, vt // piece, add, 0)
            fin_copy(j, 0).start()
            if j > 0:
                fin_copy(j, 1).start()
            fin_local(j).start()

        def tail_copy(hh, remote_copy):
            n = n_tail - over * (1 - hh)
            src, dst = fint.at[pl.ds(0, n), :], gh_ref.at[pl.ds(hh * first_row + tail_row, n), :]
            if remote_copy:
                return remote(src, dst, sf_sem.at[n_own, 0], rf_sem.at[n_own, 0], to_a)
            return pltpu.make_async_copy(src, dst, o_sem.at[n_own])

        def event(what, j):
            if what == "fin":
                finish_tile(j)
            elif what == "fb":
                fin_copy(j, 1).start()
            elif what == "d":
                exchange_d(j)
            elif what == "1":
                exchange_1(j)
            elif what == "2":
                exchange_2(j)
            elif what == "tail":
                send_tail.wait_recv()
                fint[...] = ((dwt[...] + tr[...]) * (1.0 / n_data)).astype(BF16)
                for hh in range(2):
                    @pl.when(h == hh)
                    def _(hh=hh):
                        tail_copy(hh, True).start()
                        tail_copy(hh, False).start()
            else:
                arrived(j, 0 if j == 0 else 1).wait_recv()
                forward(j).start()

        def after(u, carry):
            for at, what, j in EVENTS:
                @pl.when(u == at)
                def _(what=what, j=j):
                    event(what, j)

            for t in range(n_t // 2):
                @pl.when(u == MLP_FROM + t * per_group)
                def _(t=t):
                    send_d(t).wait_send()
                    send_1(t, 0).wait_send()
                    send_1(t, 1).wait_send()
                    send_2(t).wait_send()
                    send_a(t).wait_send()

            @pl.when(jnp.logical_and(u >= MLP_FROM, u < MLP_FROM + n_mlp))
            def _():
                mlp_step(u - MLP_FROM)

            return carry

        lax.fori_loop(N_STEP, max(MLP_FROM + n_mlp, EVENTS[-1][0] + 1), after, 0)
        act_out(jnp.int32(n_mlp - 2)).wait()
        act_out(jnp.int32(n_mlp - 1)).wait()

        for q in range(n_t // 2):
            send_a(q).wait_recv()
            gx_ref[q] = dxb[n_t // 2 + q, x, c] + ra[q]
        send_loss().wait()
        loss_ref[...] = (ls[...] + lr[...]) * (1.0 / n_data)
        for j in range(n_own):
            send_b(j).wait_send()
        send_tail.wait_send()
        for t in range(n_t // 2, n_t):
            send_d(t).wait_send()
            send_1(t, 0).wait_send()
            send_1(t, 1).wait_send()
            send_2(t).wait_send()
        for hh in range(2):
            @pl.when(h == hh)
            def _(hh=hh):
                tail_copy(hh, True).wait_send()
                tail_copy(hh, False).wait()
                tail_copy(1 - hh, True).wait_recv()
        for j in range(n_own):
            fin_local(j).wait()
            fin_copy(j, 0).wait_send()
            fin_copy(j, 1).wait_send()
            forward(j).wait_send()
            arrived(j, 1 if j == 0 else 0).wait_recv()
            arrived(j, 2).wait_recv()

    pl.run_scoped(
        finish,
        pltpu.VMEM((vt, d), F32),
        pltpu.VMEM((n_own, vt, d), BF16),
        pltpu.VMEM((n_tail, d), BF16),
        pltpu.VMEM((2, d, MLP_CHUNK), BF16),
        pltpu.VMEM((2, MLP_CHUNK, d), BF16),
        pltpu.VMEM((2, min(512, n_lane), d), BF16),
        pltpu.VMEM((min(512, n_lane), MLP_CHUNK), BF16),
    )


def grads(lab, coef, z, x, w, vt, shard, act, w1, w2):
    n_t, n_stage, rows, d = x.shape
    win = w.shape[0]
    n_tail = win - N_TILE * vt
    n = n_stage * rows
    vm = pl.BlockSpec(memory_space=pltpu.VMEM)
    hbm = pl.BlockSpec(memory_space=pl.ANY)
    dma = pltpu.SemaphoreType.DMA
    n_x = n_stage // 2
    n_own = N_TILE // 2
    return pl.pallas_call(
        functools.partial(_grads_body, n_stage=n_stage, first_row=shard - win, over=2 * win - shard),
        in_specs=[vm, vm] + [hbm] * 6,
        out_specs=[hbm] * 5 + [vm] * 2,
        out_shape=[jax.ShapeDtypeStruct((shard, d), BF16), jax.ShapeDtypeStruct(act.shape, BF16)] + [jax.ShapeDtypeStruct((vt, d), F32)] * n_own + [
            jax.ShapeDtypeStruct((n_t // 2, rows, d), F32),
            jax.ShapeDtypeStruct((8, 128), F32),
        ],
        scratch_shapes=[
            pltpu.VMEM((n_t, n_x, 2, rows, d), F32),
            pltpu.VMEM((N_TILE, vt, d), F32),
            pltpu.VMEM((n_tail, d), F32),
            pltpu.VMEM((n_tail, d), F32),
            pltpu.VMEM((2, n_x, rows, d), F32),
            pltpu.VMEM((SLOTS_1, 2, rows, d), F32),
            pltpu.VMEM((SLOTS_2, rows, d), F32),
            pltpu.VMEM((n_t // 2, rows, d), F32),
            pltpu.VMEM((8, 128), F32),
            pltpu.VMEM((8, 128), F32),
            dma((2,)), dma((2,)), dma((2,)), dma, dma, dma((4,)), dma((4,)), dma((4,)),
            dma((n_t,)), dma((n_t,)), dma((n_t, 2)), dma((n_t, 2)), dma((n_t,)), dma((n_t,)), dma((n_t // 2,)), dma((n_t // 2,)),
            dma((4, 3)), dma((4, 3)), dma, dma((2,)), dma((2,)), dma((2,)), dma((2, 2)),
        ],
        compiler_params=pltpu.CompilerParams(vmem_limit_bytes=67043328, collective_id=1, has_side_effects=True),
        cost_estimate=_cost(4 * n_t * n * d * win, 4 * n_t * n * win, n_t * n * win),
        name="grads",
    )(lab, coef, z, x, w, act, w1, w2)


def solution(mesh):
    n_data, n_stage = mesh.shape["data"], mesh.shape["stage"]
    tok_spec = P(("pod", "data", "stage"), None)
    rep_spec = P(("pod", "data"))
    vocab_spec = P("stage", None)
    layer_spec = P("stage", None, None)
    swap_a = [(i, i ^ 1) for i in range(n_data)]

    def local_step(x_rows, w_head, labels, loss_mask, w_embed, tok_ids, act_in, w_up, w_down):
        y, s = lax.axis_index("data"), lax.axis_index("stage")
        shard, d = w_head.shape
        yh = y >> 1
        h = (y ^ yh) & 1
        step_rows = 16 * N_TILE
        win = -(-shard // (2 * step_rows)) * step_rows
        vt = (win // N_TILE - 1) // 16 * 16
        first_row = shard - win
        over = 2 * win - shard

        def over_a(v):
            return lax.ppermute(v, "data", swap_a)

        lab_a = over_a(labels)

        def local(lab):
            lab = lab - (s * shard + h * first_row)
            return jnp.where(lab < win - over * (1 - h), lab, -1)

        n_tok = labels.shape[0]
        lab_two = jnp.stack([local(labels), local(lab_a)])
        local_ids = tok_ids - s * shard
        in_slice = (local_ids >= 0) & (local_ids < shard)
        rows_emb = w_embed.at[jnp.clip(local_ids, 0, shard - 1)].get(mode="promise_in_bounds").reshape(n_stage, -1, d)
        hit = jnp.broadcast_to(in_slice[:, None], (n_tok, 128)).astype(BF16).reshape(n_stage, -1, 128)
        z, x_all, w_win, emb_part, coef = head(
            x_rows, w_head, lab_two.reshape(2, 1, n_tok), loss_mask.reshape(1, -1), rows_emb, hit, n_stage, win, logits_tile(win)
        )
        emb_part = emb_part.reshape(n_tok, d)
        n_t, _, rows, _ = x_all.shape
        lab = lab_two[::-1].reshape(2, n_stage, n_t // 2, rows).transpose(0, 2, 1, 3).reshape(n_t, 1, n_stage * rows)
        grad_head, mlp_out, _, _, _, gx, loss = grads(lab, coef, z, x_all, w_win, vt, shard, act_in, w_up[0], w_down[0])
        grad_x = gx.reshape(x_rows.shape)
        mean_loss = loss[0, 0]

        embed_out = lax.psum_scatter(emb_part, "stage", scatter_dimension=0, tiled=True)

        return mean_loss.reshape(1), grad_x, grad_head, embed_out, mlp_out

    return jax.shard_map(
        local_step,
        mesh=mesh,
        in_specs=(tok_spec, vocab_spec, rep_spec, rep_spec, vocab_spec, rep_spec, tok_spec, layer_spec, layer_spec),
        out_specs=(P("pod"), tok_spec, P(("pod", "stage"), None), tok_spec, tok_spec),
        check_vma=False,
    )
```

```python
import functools

import jax
import jax.numpy as jnp
from jax import lax
from jax.experimental import pallas as pl
from jax.experimental.pallas import tpu as pltpu
from jax.sharding import PartitionSpec as P

MESH = pl.DeviceIdType.MESH
F32 = jnp.float32
BF16 = jnp.bfloat16
N_TILE = 6


def logits_tile(win):
    return next(v for v in range(352, 0, -16) if win % v == 0 and v <= 288)


LOW = -1e30


def _params(mib=60, **kw):
    return pltpu.CompilerParams(vmem_limit_bytes=mib * 2**20, **kw)


def _cost(flops, nbytes, trans=0):
    return pl.CostEstimate(flops=int(flops), bytes_accessed=int(nbytes), transcendentals=int(trans))


def _logits_block(z_ref, x, w_ref, lab, end, vt):
    tb = x.shape[0]
    lab8 = jnp.broadcast_to(lab, (8, tb))
    sub = lax.broadcasted_iota(jnp.int32, (vt // 8, 8, tb), 0) * 8 + lax.broadcasted_iota(jnp.int32, (vt // 8, 8, tb), 1)
    m8 = s8 = t8 = None
    n_v = w_ref.shape[0] // vt
    for v in range(n_v):
        vs = slice(v * vt, (v + 1) * vt)
        z = lax.dot_general(w_ref[vs, :], x, (((1,), (1,)), ((), ())), preferred_element_type=F32)
        if v == n_v - 1:
            z = jnp.where(lax.broadcasted_iota(jnp.int32, (vt, tb), 0) + v * vt < end, z, LOW)
        z_ref[vs, :] = z
        zr = z_ref[vs, :].reshape(vt // 8, 8, tb)
        tile_max = jnp.max(zr, axis=0)
        m_new = tile_max if v == 0 else jnp.maximum(m8, tile_max)
        e_sum = jnp.sum(jnp.exp(zr - m_new[None]), axis=0)
        hit = jnp.sum(jnp.where(sub + v * vt == lab8[None], zr, 0.0), axis=0)
        s8 = e_sum if v == 0 else s8 * jnp.exp(m8 - m_new) + e_sum
        t8 = hit if v == 0 else t8 + hit
        m8 = m_new
    m = jnp.max(m8, axis=0, keepdims=True)
    s = jnp.sum(s8 * jnp.exp(m8 - m), axis=0, keepdims=True)
    t = jnp.sum(t8, axis=0, keepdims=True)
    return jnp.concatenate([m, s, t, jnp.zeros((5, tb), F32)], axis=0)


def _head_body(
    x_ref, wh_ref, lab_ref, mask_ref, emb_ref, hit_ref, z_ref, xo_ref, wo_ref, eo_ref, coef_out,
    xbuf, wbuf, zbuf, st, got, mine, coef, ebuf,
    ei_sem, eo_sem, own_sem, w_sem, wo_sem, z_sem, xo_sem, xs_sem, xr_sem, send1, recv1, send2, recv2, *, n_stage, first_row, over, vt,
):
    y, s = lax.axis_index("data"), lax.axis_index("stage")
    h = lax.rem(y + y // 2, 2)
    n_x = n_stage // 2
    x, c = s // 2, lax.rem(s, 2)
    n_q, rows = xbuf.shape[1:3]
    win = wbuf.shape[0]
    n_blk = 2 * n_stage
    y_a = y + 1 - 2 * lax.rem(y, 2)
    sib = s + 1 - 2 * c

    def at(off, flip=0):
        return 2 * lax.rem(x + off, n_x) + lax.rem(c + flip, 2)

    left, right, far = at(n_x - 1), at(1), at(2)
    here = {"data": y, "stage": s}
    to_a = {"data": y_a, "stage": s}
    to_sib = {"data": y, "stage": sib}
    to_left = {"data": y, "stage": left}
    to_right = {"data": y, "stage": right}

    def slot(f, stage):
        return f * n_stage + stage

    sends = [
        (slot(0, s), slot(0, s), to_right, None),
        (slot(0, s), slot(0, s), to_left, None),
        (slot(0, s), slot(1, s), to_a, None),
        (slot(0, s), slot(0, s), to_sib, None),
        (slot(0, left), slot(0, left), to_right, 0),
        (slot(0, right), slot(0, right), to_left, 1),
        (slot(1, s), slot(1, s), to_right, None),
        (slot(1, s), slot(1, s), to_left, None),
        (slot(1, s), slot(1, s), to_sib, None),
        (slot(0, left), slot(0, left), to_sib, None),
        (slot(0, right), slot(0, right), to_sib, None),
        (slot(0, far), slot(1, far), to_a, None),
        (slot(0, far), slot(0, far), to_sib, None),
        (slot(1, left), slot(1, left), to_sib, None),
        (slot(1, right), slot(1, right), to_sib, None),
        (slot(1, far), slot(1, far), to_sib, None),
    ]

    def half(i, part):
        return xbuf.at[i, pl.ds(part * n_q // 2, n_q // 2)]

    def copy(k):
        src, dst, to, part = sends[k]
        return pltpu.make_async_remote_copy(
            src_ref=xbuf.at[src] if part is None else half(src, part),
            dst_ref=xbuf.at[dst] if part is None else half(dst, part),
            send_sem=xs_sem.at[k],
            recv_sem=xr_sem.at[n_blk if part == 1 else dst],
            device_id=to,
            device_id_type=MESH,
        )

    def arrival(ref, sem):
        return pltpu.make_async_remote_copy(
            src_ref=ref, dst_ref=ref, send_sem=xs_sem.at[0], recv_sem=sem, device_id=here, device_id_type=MESH
        )

    def got_block(f, stage):
        arrival(xbuf.at[slot(f, stage)], xr_sem.at[slot(f, stage)]).wait_recv()

    def got_half(part):
        i = slot(0, far)
        arrival(half(i, part), xr_sem.at[n_blk if part == 1 else i]).wait_recv()

    own = pltpu.make_async_copy(x_ref, xbuf.at[slot(0, s)], own_sem)
    own.start()
    w_load = pltpu.make_async_copy(wh_ref.at[pl.ds(pl.multiple_of(h * first_row, 16), win), :], wbuf, w_sem)
    w_load.start()

    def emb_in(e):
        return pltpu.make_async_copy(emb_ref.at[e], ebuf.at[e % 2], ei_sem.at[e % 2])

    def emb_out(e):
        return pltpu.make_async_copy(ebuf.at[e % 2], eo_ref.at[e], eo_sem.at[e % 2])

    def select(e, carry):
        emb_in(e).wait()
        hit = jnp.concatenate([hit_ref[e]] * (ebuf.shape[2] // hit_ref.shape[2]), axis=1)
        v = ebuf[e % 2]
        ebuf[e % 2] = jnp.where(hit != 0, v, jnp.zeros_like(v))
        emb_out(e).start()

        @pl.when(jnp.logical_and(e >= 1, e + 1 < n_stage))
        def _():
            emb_out(e - 1).wait()
            emb_in(e + 1).start()

        return carry

    emb_in(0).start()
    emb_in(1).start()

    peers = [(f, k) for f in range(2) for k in range(n_stage) if (f, k) != (0, 0)]

    def peer(f, k):
        return {"data": y if f == 0 else y_a, "stage": lax.rem(s + k, n_stage)}

    barrier = pltpu.get_barrier_semaphore()
    for f, k in peers:
        pl.semaphore_signal(barrier, inc=1, device_id=peer(f, k), device_id_type=MESH)
    pl.semaphore_wait(barrier, len(peers))

    own.wait()
    for k in range(4):
        copy(k).start()
    w_load.wait()
    w_out = pltpu.make_async_copy(wbuf, wo_ref, wo_sem)
    w_out.start()

    def quarter(stage):
        return pl.ds(pl.multiple_of(stage * rows, rows), rows)

    def z_copy(zs, b, f, stage):
        return pltpu.make_async_copy(
            zbuf.at[zs, :, pl.ds(b * rows, rows)],
            z_ref.at[n_q * (1 - f) + b, stage],
            z_sem.at[zs, b],
        )

    def x_copy(f, stage):
        i = slot(f, stage)
        return pltpu.make_async_copy(xbuf.at[i], xo_ref.at[pl.ds(n_q * (1 - f), n_q), stage], xo_sem.at[i])

    def step(i, carry):
        @pl.when(i == 1)
        def _():
            got_block(0, sib)

        @pl.when(i == 2)
        def _():
            lax.fori_loop(0, n_stage, select, 0)
            got_block(1, s)
            got_block(0, left)
            got_block(0, right)
            for k in range(4, 11):
                copy(k).start()

        @pl.when(i == 5)
        def _():
            got_half(0)
            got_half(1)
            copy(11).start()
            copy(12).start()
            got_block(1, sib)

        @pl.when(i == 6)
        def _():
            got_block(0, at(n_x - 1, 1))

        @pl.when(i == 7)
        def _():
            got_block(0, at(1, 1))

        @pl.when(i == 9)
        def _():
            got_block(0, at(2, 1))

        @pl.when(i == 10)
        def _():
            got_block(1, left)
            got_block(1, right)
            copy(13).start()
            copy(14).start()

        @pl.when(i == 12)
        def _():
            got_block(1, far)
            copy(15).start()
            got_block(1, at(n_x - 1, 1))

        @pl.when(i == 13)
        def _():
            got_block(1, at(1, 1))

        @pl.when(i == 15)
        def _():
            got_block(1, at(2, 1))

        def among(*ks):
            return functools.reduce(jnp.logical_or, [i == k for k in ks])

        f = jnp.where(jnp.logical_or(among(2, 5), i >= 10), 1, 0)
        flip = jnp.where(among(1, 5, 6, 7, 9, 12, 13, 15), 1, 0)
        off = jnp.where(among(3, 6, 10, 12), n_x - 1, jnp.where(among(4, 7, 11, 13), 1, jnp.where(among(8, 9, 14, 15), 2, 0)))
        stage = at(off, flip)
        blk = slot(f, stage)
        zs = lax.rem(i, 2)

        @pl.when(i >= 2)
        def _():
            for b in range(n_q):
                z_copy(zs, b, f, stage).wait()

        x_copy(f, stage).start()
        lab = lab_ref[f, :, pl.ds(pl.multiple_of(stage * n_q * rows, n_q * rows), n_q * rows)]
        res = _logits_block(zbuf.at[zs], xbuf[blk].reshape(n_q * rows, -1), wbuf, lab, win - over * (1 - h), vt)
        for b in range(n_q):
            st[n_q * (1 - f) + b, :, quarter(stage)] = res[:, b * rows:(b + 1) * rows]
            z_copy(zs, b, f, stage).start()
        return carry

    lax.fori_loop(0, n_blk, step, 0)

    first = []
    for f, k in peers:
        c1 = pltpu.make_async_remote_copy(
            src_ref=st.at[pl.ds(n_q * (1 - f), n_q), :, quarter(lax.rem(s + k, n_stage))],
            dst_ref=got.at[slot(f, k)],
            send_sem=send1.at[slot(f, k)],
            recv_sem=recv1.at[slot(f, k)],
            device_id=peer(f, k),
            device_id_type=MESH,
        )
        c1.start()
        first.append(c1)
    weight = mask_ref[...].astype(F32)
    denom = jnp.maximum(jnp.sum(weight), 1.0)
    mu = jnp.stack([mask_ref[:, pl.ds(pl.multiple_of((n_q * s + b) * rows, rows), rows)].astype(F32) for b in range(n_q)])
    scale = mu / denom
    for c1 in first:
        c1.wait_recv()
    parts = [st[n_q:2 * n_q, :, quarter(s)]] + [got[slot(f, k)] for f, k in peers]
    m = functools.reduce(jnp.maximum, [p[:, 0:1, :] for p in parts])
    z = sum(p[:, 1:2, :] * jnp.exp(p[:, 0:1, :] - m) for p in parts)
    t = sum(p[:, 2:3, :] for p in parts)
    loss = scale * (jnp.log(z) + m - t)
    res = jnp.concatenate([m, scale / z, scale, loss, jnp.zeros((n_q, 4, rows), F32)], axis=1)
    mine[...] = res
    second = []
    for f, k in peers:
        c2 = pltpu.make_async_remote_copy(
            src_ref=mine,
            dst_ref=coef.at[pl.ds(n_q * (1 - f), n_q), :, quarter(s)],
            send_sem=send2.at[slot(f, k)],
            recv_sem=recv2.at[slot(f, k)],
            device_id=peer(f, k),
            device_id_type=MESH,
        )
        c2.start()
        second.append(c2)
    coef[n_q:2 * n_q, :, quarter(s)] = res
    for zs in range(2):
        for b in range(n_q):
            z_copy(zs, b, 0, s).wait()
    for i in range(n_blk):
        x_copy(i // n_stage, i % n_stage).wait()
    w_out.wait()
    emb_out(n_stage - 2).wait()
    emb_out(n_stage - 1).wait()
    for k in range(len(sends)):
        copy(k).wait_send()
    for c1 in first:
        c1.wait_send()
    for c2 in second:
        c2.wait_recv()
    coef_out[...] = coef[...]
    for c2 in second:
        c2.wait_send()


def head(x_rows, w_head, lab, mask, emb, hit, n_stage, win, vt):
    rows, d = x_rows.shape
    n_q = 4
    hr = rows // n_q
    shard = w_head.shape[0]
    n = n_stage * hr
    n_blk = 2 * n_stage
    vm = pl.BlockSpec(memory_space=pltpu.VMEM)
    hbm = pl.BlockSpec(memory_space=pl.ANY)
    dma = pltpu.SemaphoreType.DMA
    x3 = x_rows.reshape(n_q, hr, d)
    total = n_blk * rows
    return pl.pallas_call(
        functools.partial(_head_body, n_stage=n_stage, first_row=shard - win, over=2 * win - shard, vt=vt),
        in_specs=[hbm, hbm, vm, vm, hbm, vm],
        out_specs=[hbm, hbm, hbm, hbm, vm],
        out_shape=[
            jax.ShapeDtypeStruct((2 * n_q, n_stage, win, hr), F32),
            jax.ShapeDtypeStruct((2 * n_q, n_stage, hr, d), BF16),
            jax.ShapeDtypeStruct((win, d), BF16),
            jax.ShapeDtypeStruct(emb.shape, BF16),
            jax.ShapeDtypeStruct((2 * n_q, 8, n), F32),
        ],
        scratch_shapes=[
            pltpu.VMEM((n_blk, n_q, hr, d), BF16),
            pltpu.VMEM((win, d), BF16),
            pltpu.VMEM((2, win, rows), F32),
            pltpu.VMEM((2 * n_q, 8, n), F32),
            pltpu.VMEM((n_blk, n_q, 8, hr), F32),
            pltpu.VMEM((n_q, 8, hr), F32),
            pltpu.VMEM((2 * n_q, 8, n), F32),
            pltpu.VMEM((2, *emb.shape[1:]), BF16),
            dma((2,)), dma((2,)), dma, dma, dma, dma((2, n_q)), dma((n_blk,)), dma((16,)), dma((n_blk + 1,)),
            dma((n_blk,)), dma((n_blk,)), dma((n_blk,)), dma((n_blk,)),
        ],
        compiler_params=_params(56, collective_id=0, has_side_effects=True),
        cost_estimate=_cost(2 * total * d * win, 4 * total * win, total * win),
        name="head",
    )(x3, w_head, lab, mask, emb, hit)


DONE = (12, 17, 27, 31, 35, 41, 44, 47)
SENT = (7, 23, 38)
N_STEP = 48
Z_SLOTS = 3
AFTER_D, AFTER_1, AFTER_2 = 3, 12, 18
SLOTS_1, SLOTS_2 = 6, 4


PHASES = ((0, 1, 0, 0), (8, 5, 1, 0), (18, 1, 1, 2), (24, 4, 2, 2), (36, 1, 2, 5), (39, 3, 3, 5))
EVENTS = (
    (48, "2", 3), (48, "fin", 0), (49, "d", 7), (49, "fin", 1), (53, "1", 5), (53, "fin", 2), (53, "fb", 0), (54, "2", 4), (56, "tail", 0),
    (60, "1", 6), (61, "2", 5), (62, "pass", 0), (65, "1", 7), (68, "2", 6), (70, "pass", 1), (72, "2", 7), (83, "pass", 2),
)
MLP_FROM = 50
MLP_CHUNK = 512


def _step_of(u):
    tile = group = xi = wi = jnp.int32(0)
    new_x = new_w = False
    x_base = w_base = 0
    ends = [p[0] for p in PHASES[1:]] + [N_STEP]
    for (start, n_tile, tile0, group0), end in zip(PHASES, ends):
        k = u - start
        on = u >= start
        turn = k if n_tile == 1 else sum(jnp.where(k >= i, 1, 0) for i in range(n_tile, end - start, n_tile))
        place = k - n_tile * turn
        tile = jnp.where(on, tile0 + place, tile)
        group = jnp.where(on, group0 + turn, group)
        xi = jnp.where(on, x_base + turn, xi)
        wi = jnp.where(on, w_base + (k if n_tile > 1 else 0), wi)
        new_x = jnp.where(on, place == 0, new_x)
        new_w = jnp.where(on, True if n_tile > 1 else k == 0, new_w)
        x_base += (end - start) // n_tile
        w_base += end - start if n_tile > 1 else 1
    return tile, group, xi % 2, wi % 2, new_x, new_w


def _grads_body(
    lab_ref, coef_ref, z_ref, x_ref, w_ref, a_ref, w1_ref, w2_ref, gh_ref, mo_ref, rcv0, rcv1, rcv2, gx_ref, loss_ref,
    dxb, dwb, dwt, tr, rd, r1, r2, ra, ls, lr,
    z_sem, x_sem, w_sem, zt_sem, wt_sem, o_sem, sb_sem, rb_sem, sd_sem, rd_sem, s1_sem, r1_sem, s2_sem, r2_sem, sa_sem, ra_sem,
    sf_sem, rf_sem, st_sem, l_sem, ai_sem, ao_sem, mw_sem,
    *, n_stage, first_row, over,
):
    y, s = lax.axis_index("data"), lax.axis_index("stage")
    n_x = n_stage // 2
    x, c = s // 2, lax.rem(s, 2)
    yh = y // 2
    y_a = y + 1 - 2 * lax.rem(y, 2)
    n_data = lax.axis_size("data")
    y_b = n_data - 1 - y
    h = lax.rem(y + yh, 2)
    x_1, x_3 = x + 1 - 2 * lax.rem(x, 2), n_x - 1 - x
    vt = dwb.shape[1]
    n_own = dwb.shape[0] // 2
    n_t, _, _, rows, d = dxb.shape
    n_tail = dwt.shape[0]
    piece = min(rows, vt)
    tail_row = 2 * n_own * vt
    rcv = (rcv0, rcv1, rcv2)
    to_sib = {"data": y, "stage": 2 * x + 1 - c}
    to_a = {"data": y_a, "stage": s}
    to_b = {"data": y_b, "stage": s}

    def stage_at(xx):
        return {"data": y, "stage": 2 * xx + c}

    def remote(src, dst, send, recv, to):
        return pltpu.make_async_remote_copy(
            src_ref=src, dst_ref=dst, send_sem=send, recv_sem=recv, device_id=to, device_id_type=MESH
        )

    def row0(tile):
        far = tile < n_own
        half = jnp.where(far, 1 - yh, yh)
        return pl.multiple_of((half * n_own + tile - jnp.where(far, 0, n_own)) * vt, vt)

    def send_loss():
        return remote(ls, lr, l_sem.at[0], l_sem.at[1], to_b)

    def meet():
        peers = (to_sib, to_a, to_b, stage_at(x_1), stage_at(x_3))
        barrier = pltpu.get_barrier_semaphore()
        for p in peers:
            pl.semaphore_signal(barrier, inc=1, device_id=p, device_id_type=MESH)
        pl.semaphore_wait(barrier, len(peers))

        loss_part = [jnp.sum(coef_ref[i * n_t // 2:(i + 1) * n_t // 2, 3:4, :]) for i in range(2)]
        loss_pair = loss_part[0] + loss_part[1]
        ls[...] = jnp.full(ls.shape, loss_pair, F32)

        send_loss().start()

    def send_d(t):
        return remote(dxb.at[t, :, 1 - c], rd.at[t % 2], sd_sem.at[t], rd_sem.at[t], to_sib)

    def order(t):
        even = t % 2 == 0
        return jnp.where(even, x_1, x_3), jnp.where(even, x_3, x_1)

    def send_1(t, k):
        p1, _ = order(t)
        mine = p1 if k == 0 else n_x - 1 - x_1
        return remote(dxb.at[t, mine, c], r1.at[t % SLOTS_1, k], s1_sem.at[t, k], r1_sem.at[t, k], stage_at(p1))

    def send_2(t):
        _, p2 = order(t)
        return remote(dxb.at[t, p2, c], r2.at[t % SLOTS_2], s2_sem.at[t], r2_sem.at[t], stage_at(p2))

    def send_a(t):
        return remote(dxb.at[t, x, c], ra.at[t], sa_sem.at[t], ra_sem.at[t], to_a)

    def exchange_d(t):
        send_d(t).wait_recv()

        def add(xx, carry):
            dxb[t, xx, c] = dxb[t, xx, c] + rd[t % 2, xx]
            return carry

        lax.fori_loop(0, n_x, add, 0)
        send_1(t, 0).start()
        send_1(t, 1).start()

    def exchange_1(t):
        _, p2 = order(t)
        send_1(t, 0).wait_recv()
        send_1(t, 1).wait_recv()
        dxb[t, p2, c] = dxb[t, p2, c] + r1[t % SLOTS_1, 1]
        send_2(t).start()
        dxb[t, x, c] = dxb[t, x, c] + r1[t % SLOTS_1, 0]

    def exchange_2(t):
        send_2(t).wait_recv()
        dxb[t, x, c] = dxb[t, x, c] + r2[t % SLOTS_2]

        @pl.when(t < n_t // 2)
        def _():
            send_a(t).start()

    def exchanges(u):
        for after, run in ((AFTER_2, exchange_2), (AFTER_1, exchange_1), (AFTER_D, exchange_d)):
            done = [d for d in DONE if d + after < N_STEP]
            t = sum(jnp.where(u == d + after, i, 0) for i, d in enumerate(done))

            @pl.when(functools.reduce(jnp.logical_or, [u == d + after for d in done]))
            def _(run=run, t=t):
                run(t)

    def g_tile(z, g_out, t, base):
        n_row = z.shape[1]
        sub = lax.broadcasted_iota(jnp.int32, (n_row // 8, 8, rows), 0) * 8 + lax.broadcasted_iota(jnp.int32, (n_row // 8, 8, rows), 1)
        for i in range(n_stage):
            cs = slice(i * rows, (i + 1) * rows)
            m8 = jnp.broadcast_to(coef_ref[t, 0:1, cs], (8, rows))
            c8 = jnp.broadcast_to(coef_ref[t, 1:2, cs], (8, rows))
            q8 = jnp.broadcast_to(coef_ref[t, 2:3, cs], (8, rows))
            lab8 = jnp.broadcast_to(lab_ref[t, :, cs], (8, rows)) - base
            zr = z[i].reshape(n_row // 8, 8, rows)
            e = jnp.exp(zr - m8[None]) * c8[None]
            gi = jnp.where(sub == lab8[None], e - q8[None], e)
            g_out[:, cs] = gi.reshape(n_row, rows).astype(BF16)

    def send_b(j):
        return remote(dwb.at[j], rcv[j], sb_sem.at[j], rb_sem.at[j], to_b)

    def products(zb, xb, wb, zt, wt, g, gt):
        def z_whole(u):
            tile, t = _step_of(u)[:2]
            return pltpu.make_async_copy(z_ref.at[t, :, pl.ds(row0(tile), vt), :], zb.at[u % Z_SLOTS], z_sem.at[u % Z_SLOTS])

        def z_load(u):
            tile, t = _step_of(u)[:2]
            for i in range(0, n_stage, 2):
                part = pl.ds(i, 2)
                pltpu.make_async_copy(z_ref.at[t, part, pl.ds(row0(tile), vt), :], zb.at[u % Z_SLOTS, part], z_sem.at[u % Z_SLOTS]).start()

        def whole(u):
            tile, t, xk, wk, new_x, new_w = _step_of(u)
            return (
                z_whole(u),
                pltpu.make_async_copy(x_ref.at[t], xb.at[xk], x_sem.at[xk]),
                pltpu.make_async_copy(w_ref.at[pl.ds(row0(tile), vt), :], wb.at[wk], w_sem.at[wk]),
                new_x, new_w,
            )

        def load(u):
            tile, t, xk, wk, new_x, new_w = _step_of(u)
            r0 = row0(tile)

            @pl.when(new_x)
            def _():
                for i in range(0, n_stage, 2):
                    part = pl.ds(i, 2)
                    pltpu.make_async_copy(x_ref.at[t, part], xb.at[xk, part], x_sem.at[xk]).start()

            @pl.when(new_w)
            def _():
                for i in range(2):
                    src, dst = pl.ds(r0 + i * vt // 2, vt // 2), pl.ds(i * vt // 2, vt // 2)
                    pltpu.make_async_copy(w_ref.at[src, :], wb.at[wk, dst, :], w_sem.at[wk]).start()

        def arrive(u):
            z_in, x_in, w_in, new_x, new_w = whole(u)
            z_in.wait()

            @pl.when(new_x)
            def _():
                x_in.wait()

            @pl.when(new_w)
            def _():
                w_in.wait()

        def tail_load(t):
            return pltpu.make_async_copy(z_ref.at[t, :, pl.ds(tail_row, n_tail), :], zt, zt_sem)

        z_load(jnp.int32(0))
        load(jnp.int32(0))
        z_load(jnp.int32(1))
        w_tail = pltpu.make_async_copy(w_ref.at[pl.ds(tail_row, n_tail), :], wt, wt_sem)
        w_tail.start()
        meet()
        w_tail.wait()

        def step(u, carry):
            tile, t, xk, wk, _, _ = _step_of(u)
            arrive(u)

            @pl.when(u < N_STEP - 1)
            def _():
                load(u + 1)

            @pl.when(u < N_STEP - 2)
            def _():
                z_load(u + 2)

            last = tile == 2 * n_own - 1

            @pl.when(last)
            def _():
                tail_load(t).start()

            exchanges(u)
            g_tile(zb.at[u % Z_SLOTS], g, t, row0(tile))
            x_t = xb[xk].reshape(n_stage * rows, d)
            for xx in range(n_x):
                gx = g[:, 2 * xx * rows:2 * (xx + 1) * rows]
                dxp = lax.dot_general(gx, wb[wk], (((0,), (0,)), ((), ())), preferred_element_type=F32)
                dxb[t, xx] = jnp.where(tile == 0, 0.0, dxb[t, xx]) + dxp.reshape(2, rows, d)
            dwb[tile] = jnp.where(t == 0, 0.0, dwb[tile]) + jnp.dot(g[...], x_t, preferred_element_type=F32)

            @pl.when(last)
            def _():
                tail_load(t).wait()
                g_tile(zt, gt, t, tail_row)
                x_t = xb[xk].reshape(n_stage * rows, d)
                for xx in range(n_x):
                    gx = gt[:, 2 * xx * rows:2 * (xx + 1) * rows]
                    dxp = lax.dot_general(gx, wt[...], (((0,), (0,)), ((), ())), preferred_element_type=F32)
                    dxb[t, xx] = dxb[t, xx] + dxp.reshape(2, rows, d)
                dwt[...] = jnp.where(t == 0, 0.0, dwt[...]) + jnp.dot(gt[...], x_t, preferred_element_type=F32)
                send_d(t).start()

            for j, end in enumerate(SENT):
                @pl.when(u == end)
                def _(j=j):
                    send_b(j).start()

            return carry

        lax.fori_loop(0, N_STEP, step, 0)

    n_lane = n_stage * rows
    pl.run_scoped(
        products,
        pltpu.VMEM((Z_SLOTS, n_stage, vt, rows), F32),
        pltpu.VMEM((2, n_stage, rows, d), BF16),
        pltpu.VMEM((2, vt, d), BF16),
        pltpu.VMEM((n_stage, n_tail, rows), F32),
        pltpu.VMEM((n_tail, d), BF16),
        pltpu.VMEM((vt, n_lane), BF16),
        pltpu.VMEM((n_tail, n_lane), BF16),
    )

    def rows_of(hh, half, j, n=None):
        n = vt if n is None else n
        return gh_ref.at[pl.ds(pl.multiple_of(hh * first_row + (half * n_own + j) * vt, 16), n), :]

    def finish(stage, fin, fint, w1, w2, act, ub):
        send_tail = remote(dwt, tr, sb_sem.at[n_own], rb_sem.at[n_own], to_b)
        send_tail.start()

        def fin_copy(j, way):
            src, dst = fin.at[j], rows_of(h, yh, j)
            if way == 0:
                return remote(src, dst, sf_sem.at[j, 0], rf_sem.at[j, 0], to_a)
            return remote(src, dst, sf_sem.at[j, 1], rf_sem.at[j, 1], to_b)

        def fin_local(j):
            return pltpu.make_async_copy(fin.at[j], rows_of(h, yh, j), o_sem.at[j])

        def forward(j):
            ref = rows_of(1 - h, yh, j) if j == 0 else rows_of(h, 1 - yh, j)
            return remote(ref, ref, sf_sem.at[j, 2], rf_sem.at[j, 2], to_b if j == 0 else to_a)

        def arrived(j, way):
            ref = rows_of(1 - h, yh, j) if way == 0 else rows_of(h, 1 - yh, j) if way == 1 else rows_of(1 - h, 1 - yh, j)
            return remote(ref, ref, sf_sem.at[j, way], rf_sem.at[j, way], to_a)

        n_rows, ff = act.shape[1], w1_ref.shape[1]
        n_block, n_chunk = a_ref.shape[0] // n_rows, ff // MLP_CHUNK
        n_mlp = n_block * n_chunk
        per_group = n_x * 2 * rows // n_rows

        def act_in(m):
            r = pl.ds(pl.multiple_of((m % n_block) * n_rows, n_rows), n_rows)
            return pltpu.make_async_copy(a_ref.at[r, :], act.at[m % 2], ai_sem.at[m % 2])

        def act_out(m):
            r = pl.ds(pl.multiple_of((m % n_block) * n_rows, n_rows), n_rows)
            return pltpu.make_async_copy(act.at[m % 2], mo_ref.at[r, :], ao_sem.at[m % 2])

        def weights(chunk):
            part = pl.ds(pl.multiple_of(chunk * MLP_CHUNK, MLP_CHUNK), MLP_CHUNK)
            k = chunk % 2
            return (
                pltpu.make_async_copy(w1_ref.at[:, part], w1.at[k], mw_sem.at[k, 0]),
                pltpu.make_async_copy(w2_ref.at[part, :], w2.at[k], mw_sem.at[k, 1]),
            )

        def mlp_step(m):
            chunk, block = m // n_block, m % n_block
            k = m % 2

            @pl.when(block == 0)
            def _():
                for cp in weights(chunk):
                    cp.wait()

                @pl.when(chunk + 1 < n_chunk)
                def _():
                    for cp in weights(chunk + 1):
                        cp.start()

            act_in(m).wait()

            @pl.when(m + 1 < n_mlp)
            def _():
                @pl.when(m - 1 >= n_mlp - n_block)
                def _():
                    act_out(m - 1).wait()

                act_in(m + 1).start()

            hid = jnp.dot(act[k], w1[chunk % 2], preferred_element_type=F32)
            ub[...] = jax.nn.gelu(hid).astype(BF16)
            out = jnp.dot(ub[...], w2[chunk % 2], preferred_element_type=F32)
            group, part = block // per_group, block % per_group
            per = n_rows // (2 * rows)
            xs = pl.ds(part * per, per)
            total = jnp.where(chunk == 0, 0.0, dxb[group, xs]) + out.reshape(per, 2, rows, d)

            @pl.when(chunk < n_chunk - 1)
            def _():
                dxb[group, xs] = total

            @pl.when(chunk == n_chunk - 1)
            def _():
                act[k] = (act[k].astype(F32) + total.reshape(n_rows, d)).astype(BF16)
                act_out(m).start()

        for cp in weights(jnp.int32(0)):
            cp.start()
        act_in(jnp.int32(0)).start()

        def finish_tile(j):
            send_b(j).wait_recv()
            cp = pltpu.make_async_copy(rcv[j], stage, st_sem)
            cp.start()
            cp.wait()

            def add(i, carry):
                r = pl.ds(pl.multiple_of(i * piece, piece), piece)
                fin[j, r, :] = ((dwb[n_own + j, r, :] + stage[r, :]) * (1.0 / n_data)).astype(BF16)
                return carry

            lax.fori_loop(0, vt // piece, add, 0)
            fin_copy(j, 0).start()
            if j > 0:
                fin_copy(j, 1).start()
            fin_local(j).start()

        def tail_copy(hh, remote_copy):
            n = n_tail - over * (1 - hh)
            src, dst = fint.at[pl.ds(0, n), :], gh_ref.at[pl.ds(hh * first_row + tail_row, n), :]
            if remote_copy:
                return remote(src, dst, sf_sem.at[n_own, 0], rf_sem.at[n_own, 0], to_a)
            return pltpu.make_async_copy(src, dst, o_sem.at[n_own])

        def event(what, j):
            if what == "fin":
                finish_tile(j)
            elif what == "fb":
                fin_copy(j, 1).start()
            elif what == "d":
                exchange_d(j)
            elif what == "1":
                exchange_1(j)
            elif what == "2":
                exchange_2(j)
            elif what == "tail":
                send_tail.wait_recv()
                fint[...] = ((dwt[...] + tr[...]) * (1.0 / n_data)).astype(BF16)
                for hh in range(2):
                    @pl.when(h == hh)
                    def _(hh=hh):
                        tail_copy(hh, True).start()
                        tail_copy(hh, False).start()
            else:
                arrived(j, 0 if j == 0 else 1).wait_recv()
                forward(j).start()

        def after(u, carry):
            for at, what, j in EVENTS:
                @pl.when(u == at)
                def _(what=what, j=j):
                    event(what, j)

            for t in range(n_t // 2):
                @pl.when(u == MLP_FROM + t * per_group)
                def _(t=t):
                    send_d(t).wait_send()
                    send_1(t, 0).wait_send()
                    send_1(t, 1).wait_send()
                    send_2(t).wait_send()
                    send_a(t).wait_send()

            @pl.when(jnp.logical_and(u >= MLP_FROM, u < MLP_FROM + n_mlp))
            def _():
                mlp_step(u - MLP_FROM)

            return carry

        lax.fori_loop(N_STEP, max(MLP_FROM + n_mlp, EVENTS[-1][0] + 1), after, 0)
        act_out(jnp.int32(n_mlp - 2)).wait()
        act_out(jnp.int32(n_mlp - 1)).wait()

        for q in range(n_t // 2):
            send_a(q).wait_recv()
            gx_ref[q] = dxb[n_t // 2 + q, x, c] + ra[q]
        send_loss().wait()
        loss_ref[...] = (ls[...] + lr[...]) * (1.0 / n_data)
        for j in range(n_own):
            send_b(j).wait_send()
        send_tail.wait_send()
        for t in range(n_t // 2, n_t):
            send_d(t).wait_send()
            send_1(t, 0).wait_send()
            send_1(t, 1).wait_send()
            send_2(t).wait_send()
        for hh in range(2):
            @pl.when(h == hh)
            def _(hh=hh):
                tail_copy(hh, True).wait_send()
                tail_copy(hh, False).wait()
                tail_copy(1 - hh, True).wait_recv()
        for j in range(n_own):
            fin_local(j).wait()
            fin_copy(j, 0).wait_send()
            fin_copy(j, 1).wait_send()
            forward(j).wait_send()
            arrived(j, 1 if j == 0 else 0).wait_recv()
            arrived(j, 2).wait_recv()

    pl.run_scoped(
        finish,
        pltpu.VMEM((vt, d), F32),
        pltpu.VMEM((n_own, vt, d), BF16),
        pltpu.VMEM((n_tail, d), BF16),
        pltpu.VMEM((2, d, MLP_CHUNK), BF16),
        pltpu.VMEM((2, MLP_CHUNK, d), BF16),
        pltpu.VMEM((2, min(512, n_lane), d), BF16),
        pltpu.VMEM((min(512, n_lane), MLP_CHUNK), BF16),
    )


def grads(lab, coef, z, x, w, vt, shard, act, w1, w2):
    n_t, n_stage, rows, d = x.shape
    win = w.shape[0]
    n_tail = win - N_TILE * vt
    n = n_stage * rows
    vm = pl.BlockSpec(memory_space=pltpu.VMEM)
    hbm = pl.BlockSpec(memory_space=pl.ANY)
    dma = pltpu.SemaphoreType.DMA
    n_x = n_stage // 2
    n_own = N_TILE // 2
    return pl.pallas_call(
        functools.partial(_grads_body, n_stage=n_stage, first_row=shard - win, over=2 * win - shard),
        in_specs=[vm, vm] + [hbm] * 6,
        out_specs=[hbm] * 5 + [vm] * 2,
        out_shape=[jax.ShapeDtypeStruct((shard, d), BF16), jax.ShapeDtypeStruct(act.shape, BF16)] + [jax.ShapeDtypeStruct((vt, d), F32)] * n_own + [
            jax.ShapeDtypeStruct((n_t // 2, rows, d), F32),
            jax.ShapeDtypeStruct((8, 128), F32),
        ],
        scratch_shapes=[
            pltpu.VMEM((n_t, n_x, 2, rows, d), F32),
            pltpu.VMEM((N_TILE, vt, d), F32),
            pltpu.VMEM((n_tail, d), F32),
            pltpu.VMEM((n_tail, d), F32),
            pltpu.VMEM((2, n_x, rows, d), F32),
            pltpu.VMEM((SLOTS_1, 2, rows, d), F32),
            pltpu.VMEM((SLOTS_2, rows, d), F32),
            pltpu.VMEM((n_t // 2, rows, d), F32),
            pltpu.VMEM((8, 128), F32),
            pltpu.VMEM((8, 128), F32),
            dma((Z_SLOTS,)), dma((2,)), dma((2,)), dma, dma, dma((4,)), dma((4,)), dma((4,)),
            dma((n_t,)), dma((n_t,)), dma((n_t, 2)), dma((n_t, 2)), dma((n_t,)), dma((n_t,)), dma((n_t // 2,)), dma((n_t // 2,)),
            dma((4, 3)), dma((4, 3)), dma, dma((2,)), dma((2,)), dma((2,)), dma((2, 2)),
        ],
        compiler_params=pltpu.CompilerParams(vmem_limit_bytes=67043328, collective_id=1, has_side_effects=True),
        cost_estimate=_cost(4 * n_t * n * d * win, 4 * n_t * n * win, n_t * n * win),
        name="grads",
    )(lab, coef, z, x, w, act, w1, w2)


def solution(mesh):
    n_data, n_stage = mesh.shape["data"], mesh.shape["stage"]
    tok_spec = P(("pod", "data", "stage"), None)
    rep_spec = P(("pod", "data"))
    vocab_spec = P("stage", None)
    layer_spec = P("stage", None, None)
    swap_a = [(i, i ^ 1) for i in range(n_data)]

    def local_step(x_rows, w_head, labels, loss_mask, w_embed, tok_ids, act_in, w_up, w_down):
        y, s = lax.axis_index("data"), lax.axis_index("stage")
        shard, d = w_head.shape
        yh = y >> 1
        h = (y ^ yh) & 1
        step_rows = 16 * N_TILE
        win = -(-shard // (2 * step_rows)) * step_rows
        vt = (win // N_TILE - 1) // 16 * 16
        first_row = shard - win
        over = 2 * win - shard

        def over_a(v):
            return lax.ppermute(v, "data", swap_a)

        lab_a = over_a(labels)

        def local(lab):
            lab = lab - (s * shard + h * first_row)
            return jnp.where(lab < win - over * (1 - h), lab, -1)

        n_tok = labels.shape[0]
        lab_two = jnp.stack([local(labels), local(lab_a)])
        local_ids = tok_ids - s * shard
        in_slice = (local_ids >= 0) & (local_ids < shard)
        rows_emb = w_embed.at[jnp.clip(local_ids, 0, shard - 1)].get(mode="promise_in_bounds").reshape(n_stage, -1, d)
        hit = jnp.broadcast_to(in_slice[:, None], (n_tok, 128)).astype(BF16).reshape(n_stage, -1, 128)
        z, x_all, w_win, emb_part, coef = head(
            x_rows, w_head, lab_two.reshape(2, 1, n_tok), loss_mask.reshape(1, -1), rows_emb, hit, n_stage, win, logits_tile(win)
        )
        emb_part = emb_part.reshape(n_tok, d)
        n_t, _, rows, _ = x_all.shape
        lab = lab_two[::-1].reshape(2, n_stage, n_t // 2, rows).transpose(0, 2, 1, 3).reshape(n_t, 1, n_stage * rows)
        grad_head, mlp_out, _, _, _, gx, loss = grads(lab, coef, z, x_all, w_win, vt, shard, act_in, w_up[0], w_down[0])
        grad_x = gx.reshape(x_rows.shape)
        mean_loss = loss[0, 0]

        embed_out = lax.psum_scatter(emb_part, "stage", scatter_dimension=0, tiled=True)

        return mean_loss.reshape(1), grad_x, grad_head, embed_out, mlp_out

    return jax.shard_map(
        local_step,
        mesh=mesh,
        in_specs=(tok_spec, vocab_spec, rep_spec, rep_spec, vocab_spec, rep_spec, tok_spec, layer_spec, layer_spec),
        out_specs=(P("pod"), tok_spec, P(("pod", "stage"), None), tok_spec, tok_spec),
        check_vma=False,
    )
```
